32 devices in a mesh: groups: 2 (over y), fibre: 4 (over z), seg: 2 (over x), rec: 2 (over core).
Axes of the slice: x: 2, y: 2, z: 4, core: 2. Of those that a mesh axis runs over, the one named last changes fastest.
Arguments:
- records: bfloat16 [2, 2048, 1024], P('rec', 'fibre', ('groups', 'seg')), parts along dimension 2, may hold values from -6 to 6
- pairs: int32 [16, 2], replicated, may hold values from 0 to 15
- observed: float32 [32, 32, 256], P(('groups', 'fibre', 'seg')), parts along dimension 0, may hold values from -6 to 6
- lag_mask: int32 [32, 256], P(('groups', 'fibre', 'seg')), parts along dimension 0, may hold values 0 or 1
Outputs:
- adjoint_sources: bfloat16 [2, 2048, 1024], P('rec', 'fibre', ('groups', 'seg')), parts along dimension 2
The draws below stay inside these ranges and needn't reach their ends.
There are 2 independent parts, one for each index of `groups`. The reference program is written for one: setup_inputs(seed, part) draws one part's arguments, and reference() takes and returns one part's arrays. A program takes and returns all parts, laid end to end along the dimension named above; an argument that names none is the same for every part. Nothing has to cross between parts.
All inputs are finite; a program needn't handle non-finite values. No bound on the sum of `lag_mask` on one device may be relied on, other than what follows from the above.
Results may differ from the reference program's by a relative error of at most 0.015.
Values may be sent and summed in bfloat16 or wider, within the bound.
A program may use at most 64 MiB of HBM per device.

```python
import jax
import jax.numpy as jnp

S = 2048
F = 1024
LAGS = 256
BLOCK = 32
CHANNELS = 512
NBLOCKS = 16
NPAIRS = 16


def set_ends(entries, own_key, least, largest):
    extent = entries.shape
    place = [jax.random.randint(jax.random.fold_in(own_key, axis), (), 0, extent[axis]) for axis in range(len(extent))]
    entries = entries.at[tuple(place)].set(least)
    longest = extent.index(max(extent))
    place[longest] = (place[longest] + 1) % extent[longest]
    return entries.at[tuple(place)].set(largest)


def steps_of(rng, shape, shards, low, top_value):
    loudness = 1.0
    for dim, shards_of in shards:
        steps = jax.random.uniform(jax.random.fold_in(jax.random.fold_in(rng, 6), dim), (shards_of,), jnp.float32, low / len(shards), top_value / len(shards))
        loudness = loudness * jnp.repeat(jnp.exp(steps), shape[dim] // shards_of).reshape((-1,) + (1,) * (len(shape) - 1 - dim))
    return loudness


def centred(stream_key, shape, deviation, limit, shards=(), kind=jnp.bfloat16):
    values = jax.random.normal(stream_key, shape, jnp.float32) * deviation
    if len(shards) > 0:
        values = steps_of(stream_key, shape, shards, -0.22, 0.18) * values
    return jnp.clip(values, min=-limit, max=limit).astype(kind)


def setup_inputs(seed: int = 0, part: int = 0) -> dict:
    streams_of = jax.random.split(jax.random.key(seed), 5)
    part_splits = jax.random.split(jax.random.fold_in(streams_of[4], part), 5)
    return {
        "records": centred(part_splits[0], (2, S, CHANNELS), 1.0, 6.0, ((0, 2), (1, 4), (2, 2))),
        "pairs": set_ends(jax.random.randint(streams_of[1], (NPAIRS, 2), 0, NBLOCKS), jax.random.fold_in(streams_of[1], 1), 0, NBLOCKS - 1).astype(jnp.int32),
        "observed": centred(part_splits[2], (NPAIRS, BLOCK, LAGS), 1.0, 6.0, ((0, 8),), jnp.float32),
        "lag_mask": set_ends((jax.random.randint(part_splits[3], (NPAIRS, LAGS), 0, 4) < 3).astype(jnp.int32), jax.random.fold_in(part_splits[3], 1), 0, 1),
    }


def forward_table():
    freq_index = jnp.arange(F, dtype=jnp.int32)
    time_index = jnp.arange(S, dtype=jnp.int32)
    phase = freq_index[:, None] * time_index[None, :] % S
    angles = phase.astype(jnp.float32) * (2.0 * jnp.pi / S)
    scale = 1.0 / jnp.sqrt(jnp.float32(S))
    return jnp.stack([(jnp.cos(angles) * scale).astype(jnp.bfloat16), (-jnp.sin(angles) * scale).astype(jnp.bfloat16)], axis=1)

def lag_table():
    freq_index = jnp.arange(F, dtype=jnp.int32)
    shifts = (jnp.arange(LAGS, dtype=jnp.int32) - LAGS // 2) % S
    phase = freq_index[:, None] * shifts[None, :] % S
    angles = phase.astype(jnp.float32) * (2.0 * jnp.pi / S)
    scale = 1.0 / jnp.sqrt(jnp.float32(F))
    return jnp.stack([(jnp.cos(angles) * scale).astype(jnp.bfloat16), (-jnp.sin(angles) * scale).astype(jnp.bfloat16)], axis=1)

def reference(records, pairs, observed, lag_mask):
    table = forward_table().astype(jnp.float32)
    lags = lag_table().astype(jnp.float32)
    spectra = jnp.einsum('wps,rsc->rwpc', table, records.astype(jnp.float32)).astype(jnp.bfloat16)
    blocks_grid = spectra.reshape(2, F, 2, NBLOCKS, BLOCK)
    first_side = jnp.take(blocks_grid, pairs[:, 0], axis=3).astype(jnp.float32)
    second_side = jnp.take(blocks_grid, pairs[:, 1], axis=3).astype(jnp.float32)
    first_re, first_im = (first_side[:, :, 0], first_side[:, :, 1])
    second_re, second_im = (second_side[:, :, 0], second_side[:, :, 1])
    cross_re = first_re * second_re + first_im * second_im
    cross_im = first_im * second_re - first_re * second_im
    cross_spec = jnp.stack([cross_re, cross_im], axis=2).astype(jnp.bfloat16)
    synthetic = jnp.einsum('rwpnk,wpl->nkl', cross_spec.astype(jnp.float32), lags)
    weights = lag_mask[:, None, :].astype(jnp.float32) * jnp.tanh(synthetic - observed)
    weights_low = weights.astype(jnp.bfloat16)
    adjoint_cross = jnp.einsum('nkl,wpl->wpnk', weights_low.astype(jnp.float32), lags).astype(jnp.bfloat16)
    adjoint_re = adjoint_cross[:, 0].astype(jnp.float32)[None]
    adjoint_im = adjoint_cross[:, 1].astype(jnp.float32)[None]
    grad_first = jnp.stack([adjoint_re * second_re - adjoint_im * second_im, adjoint_re * second_im + adjoint_im * second_re], axis=2)
    grad_second = jnp.stack([adjoint_re * first_re + adjoint_im * first_im, adjoint_re * first_im - adjoint_im * first_re], axis=2)
    contributions = jnp.concatenate([grad_first, grad_second], axis=3)
    endpoint_ids = jnp.concatenate([pairs[:, 0], pairs[:, 1]]).astype(jnp.int32)
    summed = jax.ops.segment_sum(jnp.moveaxis(contributions, 3, 0), endpoint_ids, num_segments=NBLOCKS)
    block_adjoint = jnp.moveaxis(summed, 0, 3).astype(jnp.bfloat16).reshape(2, F, 2, CHANNELS)
    adjoint_sources = jnp.einsum('rwpc,wps->rsc', block_adjoint.astype(jnp.float32), table)
    return adjoint_sources.astype(jnp.bfloat16)
```

```python
import functools

import jax
import jax.numpy as jnp
import numpy as np
from jax import lax
from jax.experimental import pallas as pl
from jax.experimental.pallas import tpu as pltpu
from jax.sharding import PartitionSpec as P

S = 2048
F = 1024
LAGS = 256
BLOCK = 32
CH_DEV = 64
VMEM_GRANT = 60899328


def forward_table():
    freq_index = jnp.arange(F, dtype=jnp.int32)
    time_index = jnp.arange(S, dtype=jnp.int32)
    phase = freq_index[:, None] * time_index[None, :] % S
    angles = phase.astype(jnp.float32) * (2.0 * jnp.pi / S)
    scale = 1.0 / jnp.sqrt(jnp.float32(S))
    return jnp.stack(
        [
            (jnp.cos(angles) * scale).astype(jnp.bfloat16),
            (-jnp.sin(angles) * scale).astype(jnp.bfloat16),
        ],
        axis=1,
    )


def lag_table():
    freq_index = jnp.arange(F, dtype=jnp.int32)
    shifts = (jnp.arange(LAGS, dtype=jnp.int32) - LAGS // 2) % S
    phase = freq_index[:, None] * shifts[None, :] % S
    angles = phase.astype(jnp.float32) * (2.0 * jnp.pi / S)
    scale = 1.0 / jnp.sqrt(jnp.float32(F))
    return jnp.stack(
        [
            (jnp.cos(angles) * scale).astype(jnp.bfloat16),
            (-jnp.sin(angles) * scale).astype(jnp.bfloat16),
        ],
        axis=1,
    )


def synthesize(incoming, table):
    count = incoming.shape[-1]
    flat = incoming.reshape(2 * F, count)
    result = jnp.einsum(
        "qn,qt->tn", flat, table.reshape(2 * F, S), preferred_element_type=jnp.float32
    )
    return result.astype(jnp.bfloat16)


def on_device(records, pairs, observed, lag_mask):
    fibre_count = lax.axis_size("fibre")
    seg_count = lax.axis_size("seg")
    spread_count = fibre_count * seg_count
    freq_dev = F // spread_count
    blocks_dev = CH_DEV // BLOCK
    block_count = CH_DEV * spread_count // BLOCK
    pair_total = pairs.shape[0]
    pairs_dev = pair_total // spread_count
    table = forward_table()
    lags = lag_table()
    spans = records.reshape(1, S // fibre_count, fibre_count, CH_DEV)
    incoming = lax.all_to_all(spans, "fibre", split_axis=2, concat_axis=1, tiled=True)
    count = incoming.shape[3]
    signal = incoming.reshape(S, count)
    result = jnp.einsum(
        "qs,sn->qn", table.reshape(2 * F, S), signal, preferred_element_type=jnp.float32
    )
    spectra = result.reshape(F, 2, count).astype(jnp.bfloat16)
    widened = lax.all_to_all(spectra, ("fibre", "seg"), split_axis=0, concat_axis=2, tiled=True)
    seg_blocks = fibre_count * blocks_dev
    slot_ids = (
        pairs % seg_blocks // blocks_dev * seg_count + pairs // seg_blocks
    ) * blocks_dev + pairs % blocks_dev
    blocks_grid = widened.reshape(freq_dev, 2, block_count, BLOCK)
    first_side = jnp.take(blocks_grid, slot_ids[:, 0], axis=2).astype(jnp.float32)
    second_side = jnp.take(blocks_grid, slot_ids[:, 1], axis=2).astype(jnp.float32)
    first_re, first_im = (first_side[:, 0], first_side[:, 1])
    second_re, second_im = (second_side[:, 0], second_side[:, 1])
    cross_re = first_re * second_re + first_im * second_im
    cross_im = first_im * second_re - first_re * second_im
    cross_spec = jnp.stack([cross_re, cross_im], axis=1).astype(jnp.bfloat16)
    cross_spec = cross_spec.reshape(freq_dev, 2, spread_count, pairs_dev * BLOCK)
    owned_spec = lax.all_to_all(
        cross_spec, ("fibre", "seg"), split_axis=2, concat_axis=0, tiled=True
    )
    owned_spec = owned_spec.reshape(F, 2, pairs_dev * BLOCK)
    partial_corr = jnp.einsum("wpx,wpl->xl", owned_spec, lags, preferred_element_type=jnp.float32)
    synthetic = (
        lax.psum(partial_corr.astype(jnp.bfloat16), "rec")
        .astype(jnp.float32)
        .reshape(pairs_dev, BLOCK, LAGS)
    )
    weights = lag_mask[:, None, :].astype(jnp.float32) * jnp.tanh(synthetic - observed)
    weights_low = weights.astype(jnp.bfloat16).reshape(pairs_dev * BLOCK, LAGS)
    adjoint_spec = jnp.einsum("xl,wpl->wpx", weights_low, lags, preferred_element_type=jnp.float32)
    adjoint_spec = adjoint_spec.astype(jnp.bfloat16).reshape(F, 2, 1, pairs_dev * BLOCK)
    returned = lax.all_to_all(
        adjoint_spec, ("fibre", "seg"), split_axis=0, concat_axis=2, tiled=True
    )
    returned = returned.reshape(freq_dev, 2, pair_total, BLOCK).astype(jnp.float32)
    adjoint_re, adjoint_im = (returned[:, 0], returned[:, 1])
    grad_first = jnp.stack(
        [
            adjoint_re * second_re - adjoint_im * second_im,
            adjoint_re * second_im + adjoint_im * second_re,
        ],
        axis=1,
    )
    grad_second = jnp.stack(
        [
            adjoint_re * first_re + adjoint_im * first_im,
            adjoint_re * first_im - adjoint_im * first_re,
        ],
        axis=1,
    )
    contributions = jnp.concatenate([grad_first, grad_second], axis=2)
    endpoint_ids = jnp.concatenate([slot_ids[:, 0], slot_ids[:, 1]])
    summed = jax.ops.segment_sum(
        jnp.moveaxis(contributions, 2, 0), endpoint_ids, num_segments=block_count
    )
    block_adjoint = jnp.moveaxis(summed, 0, 2).astype(jnp.bfloat16)
    outgoing = block_adjoint.reshape(freq_dev, 2, spread_count, CH_DEV)
    sources = synthesize(
        lax.all_to_all(outgoing, ("fibre", "seg"), split_axis=2, concat_axis=0, tiled=True), table
    )
    regrouped = lax.all_to_all(sources, "fibre", split_axis=0, concat_axis=1, tiled=True)
    return regrouped[None]


def window_tables(bands, segs):
    span, reach, n = S // bands, LAGS // 2, S // bands + LAGS
    half = n // 2

    def parts(freqs, times):
        angles = (freqs * times % n) * (2.0 * np.pi / n)
        return np.cos(angles), -np.sin(angles)

    freqs, places = np.arange(half), np.arange(n)
    shifts = np.arange(LAGS) - reach
    ends = np.where(freqs == 0, 1.0, 2.0) / (n * 2.0 * np.sqrt(F))

    def table(times, scale):
        real, imag = parts(freqs[None, :], times[:, None])
        imag[:, 0] = np.where(times % 2 == 0, 1.0, -1.0)
        return np.concatenate([real * scale, imag * scale], axis=1)

    whole = table(places, np.ones(half))
    core = whole[reach : reach + span]
    left, right = whole[:reach], whole[reach + span :]
    halo = np.stack([np.concatenate(p) for p in ((right, left), (left, right))])
    lags = table(shifts, ends).T
    taps = table(shifts, np.ones(half))
    back = table(places[reach : reach + span], ends)
    return [t.astype(np.float32).astype(jnp.bfloat16) for t in (core, halo, lags, taps, back)]


def dot(left, right, left_dim=1, right_dim=0):
    return lax.dot_general(
        left,
        right,
        (((left_dim,), (right_dim,)), ((), ())),
        preferred_element_type=jnp.float32,
    )


def spectral_product(p, q, sign):
    p0, p1 = p
    q0, q1 = q
    ends = lax.broadcasted_iota(jnp.int32, p0.shape, 1) == 0
    both = p1 * q1
    real = p0 * q0 + jnp.where(ends, 0.0, sign * both)
    imag = jnp.where(ends, both, p1 * q0 - sign * (p0 * q1))
    return real, imag


def fused_kernel(
    sizes, x_hbm, pairs, observed_hbm, mask_hbm, core_hbm, halo_hbm, lags_hbm, taps_hbm, back_hbm, out,
    core, halo, rest, observed, mask, core_table, halo_table, lags, taps, back,
    stage_sum, inbox_sum, partial_spec, core_spec, full_spec, select, cross,
    stage_core, inbox_core, stage3, inbox3, inbox4, grads, stage6,
    load_sem, send1, recv1, send2, recv2, core_sem, relay_send, relay_recv,
    send3, recv3, send4, recv4, send6, recv6,
):
    fibres, segs, recs = sizes
    bands = fibres * segs
    g, f, s, r = (lax.axis_index(name) for name in ("groups", "fibre", "seg", "rec"))
    o = 1 - s
    band = f * segs + s
    span, reach, width = S // bands, LAGS // 2, x_hbm.shape[1]
    n = span + LAGS
    half = n // 2
    blocks = width // BLOCK
    low, full = jnp.bfloat16, jnp.float32

    def at(fibre, seg, rec):
        return (g, fibre, seg, rec)

    def at_band(index):
        return at(index // segs, index % segs, r)

    def push(src, dst, send, recv, device):
        copy = pltpu.make_async_remote_copy(
            src_ref=src, dst_ref=dst, send_sem=send, recv_sem=recv,
            device_id=device, device_id_type=pl.DeviceIdType.MESH,
        )
        copy.start()
        return copy

    def arrived(dst, recv):
        pltpu.make_async_remote_copy(
            src_ref=dst, dst_ref=dst, send_sem=recv, recv_sem=recv,
            device_id=at(f, s, 1 - r), device_id_type=pl.DeviceIdType.MESH,
        ).wait_recv()

    def rows(start, count, unit):
        return pl.ds(pl.multiple_of(start, unit), count)

    def flipped(index, bits):
        result, bit = 0, 1
        while bit < bands:
            digit = index // bit % 2
            result += bit * (1 - digit if bits // bit % 2 else digit)
            bit *= 2
        return result

    partner = at(f, s, 1 - r)
    across = at(f, o, r)
    barrier = pltpu.get_barrier_semaphore()
    for d in range(1, bands):
        pl.semaphore_signal(
            barrier, inc=1, device_id=at_band(flipped(band, d)), device_id_type=pl.DeviceIdType.MESH
        )
    pl.semaphore_signal(barrier, inc=1, device_id=partner, device_id_type=pl.DeviceIdType.MESH)
    locals_ = [
        pltpu.make_async_copy(x_hbm.at[rows(span * s, span, reach)], core.at[s], load_sem.at[0]),
        pltpu.make_async_copy(
            x_hbm.at[rows(span - reach * s, reach, reach)], halo.at[s, pl.ds(0, reach)], load_sem.at[1]
        ),
        pltpu.make_async_copy(x_hbm.at[rows((2 * span - reach) * o, reach, reach)], rest, load_sem.at[2]),
    ]
    loads = [
        pltpu.make_async_copy(core_hbm, core_table, load_sem.at[3]),
        pltpu.make_async_copy(halo_hbm.at[s], halo_table, load_sem.at[4]),
        pltpu.make_async_copy(lags_hbm, lags, load_sem.at[5]),
        pltpu.make_async_copy(observed_hbm.at[r], observed, load_sem.at[6]),
        pltpu.make_async_copy(mask_hbm, mask, load_sem.at[7]),
        pltpu.make_async_copy(taps_hbm, taps, load_sem.at[8]),
        pltpu.make_async_copy(back_hbm, back, load_sem.at[9]),
    ]
    for load in locals_ + loads:
        load.start()
    pl.semaphore_wait(barrier, bands)
    tail = pl.ds(reach, reach)
    after, before = at((f + 1) % fibres, 0, r), at((f + fibres - 1) % fibres, 1, r)
    sends = [
        push(x_hbm.at[pl.ds(2 * span - reach, reach)], halo.at[s, tail], send1.at[2], recv1.at[2 + s], after),
        push(x_hbm.at[pl.ds(0, reach)], halo.at[s, tail], send1.at[3], recv1.at[2 + s], before),
        push(x_hbm.at[rows(span * o, span, reach)], core.at[s], send1.at[0], recv1.at[0], across),
        push(
            x_hbm.at[rows(span - reach * o, reach, reach)], halo.at[s, pl.ds(0, reach)],
            send1.at[1], recv1.at[1], across,
        ),
    ]
    for load in locals_:
        load.wait()
    folded = sum(
        part.astype(full).reshape(-1, 8, width).sum(axis=0)
        for part in (core[s], halo[s, pl.ds(0, reach)], rest[...])
    )
    odd = lax.broadcasted_iota(jnp.int32, folded.shape, 0) % 2 == 1
    stage_sum[...] = jnp.concatenate(
        [
            jnp.sum(folded, axis=0, keepdims=True),
            jnp.sum(jnp.where(odd, -folded, folded), axis=0, keepdims=True),
        ],
        axis=0,
    )
    for d in range(bands - 1, 0, -1):
        j = flipped(band, d)
        sends.append(push(stage_sum, inbox_sum.at[band], send2.at[d - 1], recv2.at[band], at_band(j)))
    inbox_sum[band] = stage_sum[...]

    count = pairs.shape[1] * BLOCK
    slots = [j * recs + h for h in range(recs) for j in range(bands)]
    lane = lax.broadcasted_iota(jnp.int32, (1, 2 * count), 1)
    target = lane
    for side in range(2):
        for place, pair in enumerate(slots):
            first = side * count + place * BLOCK
            inside = (lane >= first) & (lane < first + BLOCK)
            target = jnp.where(inside, lane + (pairs[side, pair] * BLOCK - first), target)
    row = lax.broadcasted_iota(jnp.int32, select.shape, 0)
    select[...] = jnp.where(row == target, 1.0, 0.0).astype(low)

    def core_part(seg):
        part = dot(core[seg], core_table[...], 0, 0)
        partial_spec[seg] = part
        core_spec[rows(seg * blocks, blocks, blocks)] = part.astype(low).reshape(blocks, BLOCK, n)

    loads[0].wait()
    core_part(s)
    arrived(core.at[o], recv1.at[0])
    core_part(o)
    for d in range(1, bands):
        k = (band + d) % bands
        arrived(inbox_sum.at[k], recv2.at[k])
    loads[1].wait()
    arrived(halo.at[s, tail], recv1.at[2 + s])
    arrived(halo.at[o, tail], recv1.at[2 + o])
    arrived(halo.at[o, pl.ds(0, reach)], recv1.at[1])
    for seg in range(segs):
        part = partial_spec[seg] + dot(halo[seg], halo_table[...], 0, 0)
        total = sum(inbox_sum[k * segs + seg] for k in range(fibres)) * (n / S)
        total = jnp.concatenate([total] * 4, axis=0).T
        head = lax.broadcasted_iota(jnp.int32, (1, 128), 1) == 0
        part = jnp.concatenate(
            [
                part[:, :128] + jnp.where(head, total[:, 0:1], 0.0),
                part[:, 128:half],
                part[:, half : half + 128] - jnp.where(head, total[:, 1:2], 0.0),
                part[:, half + 128 :],
            ],
            axis=1,
        )
        full_spec[pl.ds(seg * blocks, blocks)] = part.astype(low).reshape(blocks, BLOCK, n)

    def block(spec, index):
        value = spec[index].astype(full)
        return value[:, :half], value[:, half:]

    def correlate(place, h):
        for j in range(bands):
            pair = j * recs + h
            first = block(full_spec, pairs[0, pair])
            second = block(core_spec, pairs[1, pair])
            here = pl.ds(j * BLOCK, BLOCK)
            real, imag = spectral_product(first, second, 1.0)
            cross[place, here, pl.ds(0, half)] = real.astype(low)
            cross[place, here, pl.ds(half, half)] = imag.astype(low)
        return dot(cross[place], lags[...])

    loads[2].wait()
    stage_core[...] = correlate(0, 1 - r).astype(low)
    sends.append(push(stage_core, inbox_core, core_sem.at[0], core_sem.at[1], partner))
    partial = correlate(1, r)
    arrived(inbox_core, core_sem.at[1])
    partial = (partial + inbox_core[...].astype(full)).astype(low)
    stage3[...] = partial.reshape(stage3.shape)
    for d in range(bands - 1, 0, -1):
        j = flipped(band, d)
        sends.append(push(stage3.at[j], inbox3.at[band], send3.at[d - 1], recv3.at[band], at_band(j)))
    inbox3[band] = stage3[band]
    loads[3].wait()
    loads[4].wait()
    for d in range(1, bands):
        k = flipped(band, d)
        arrived(inbox3.at[k], recv3.at[k])
    synthetic = inbox3[0].astype(full)
    for k in range(1, bands):
        synthetic += inbox3[k].astype(full)
    window = mask[pl.ds(r, 1), :].astype(full)
    inbox4[r, band] = (window * jnp.tanh(synthetic - observed[...])).astype(low)
    own = inbox4.at[r, band]
    for d in range(bands - 1, 0, -1):
        j = flipped(band, d)
        sends.append(push(own, own, send4.at[d - 1], recv4.at[band], at_band(j)))
    sends.append(push(own, own, relay_send.at[0], relay_recv.at[band], partner))
    for d in range(1, bands):
        k = flipped(band, d)
        arrived(inbox4.at[r, k], recv4.at[k])
        got = inbox4.at[r, k]
        sends.append(push(got, got, relay_send.at[d], relay_recv.at[k], partner))
    for d in range(bands):
        k = flipped(band, d)
        arrived(inbox4.at[1 - r, k], relay_recv.at[k])
    loads[5].wait()
    for h in range(recs):
        spread = dot(inbox4[h].reshape(bands * BLOCK, LAGS), taps[...])
        for j in range(bands):
            pair = j * recs + h
            filters = spread[j * BLOCK : (j + 1) * BLOCK]
            filters = filters[:, :half], filters[:, half:]
            first = block(full_spec, pairs[0, pair])
            second = block(full_spec, pairs[1, pair])
            place = (h * bands + j) * BLOCK
            for base, parts in (
                (place, spectral_product(filters, second, -1.0)),
                (count + place, spectral_product(first, filters, 1.0)),
            ):
                for p in range(2):
                    grads[pl.ds(base, BLOCK), pl.ds(p * half, half)] = parts[p].astype(low)
    loads[6].wait()

    def source(seg):
        summed = dot(select[rows(seg * width, width, width), :], grads[...]).astype(low)
        return dot(back[...], summed, 1, 1).astype(low)

    here = rows(span * s, span, span)
    stage6[...] = source(o)
    sends.append(push(stage6, out.at[here, :], send6.at[0], recv6.at[0], across))
    out[here, :] = source(s)
    there = rows(span * o, span, span)
    arrived(out.at[there, :], recv6.at[0])
    for copy in sends:
        copy.wait_send()


def fused_on_device(mesh_shape, tables, records, pairs, observed, lag_mask):
    fibres, segs, recs = (mesh_shape[name] for name in ("fibre", "seg", "rec"))
    bands = fibres * segs
    _, extent, width = records.shape
    span, reach = S // bands, LAGS // 2
    n = span + LAGS
    count = pairs.shape[0] * BLOCK
    own = count // recs
    low, full = jnp.bfloat16, jnp.float32
    vmem = pl.BlockSpec(memory_space=pltpu.VMEM)
    hbm = pl.BlockSpec(memory_space=pltpu.HBM)
    corr = (BLOCK, LAGS)

    def sems(*sizes):
        return [pltpu.SemaphoreType.DMA((size,)) for size in sizes]

    result = pl.pallas_call(
        functools.partial(fused_kernel, (fibres, segs, recs)),
        out_shape=pltpu.VMEM((extent, width), low),
        in_specs=[hbm, pl.BlockSpec(memory_space=pltpu.SMEM)] + [hbm] * 7,
        out_specs=vmem,
        scratch_shapes=[
            pltpu.VMEM((segs, span, width), low),
            pltpu.VMEM((segs, 2 * reach, width), low),
            pltpu.VMEM((reach, width), low),
            pltpu.VMEM(corr, full),
            pltpu.VMEM(lag_mask.shape, jnp.int32),
            pltpu.VMEM((span, n), low),
            pltpu.VMEM((2 * reach, n), low),
            pltpu.VMEM((n, LAGS), low),
            pltpu.VMEM((LAGS, n), low),
            pltpu.VMEM((span, n), low),
            pltpu.VMEM((2, width), full),
            pltpu.VMEM((bands, 2, width), full),
            pltpu.VMEM((segs, width, n), full),
            pltpu.VMEM((segs * width // BLOCK, BLOCK, n), low),
            pltpu.VMEM((segs * width // BLOCK, BLOCK, n), low),
            pltpu.VMEM((segs * width, 2 * count), low),
            pltpu.VMEM((recs, own, n), low),
            pltpu.VMEM((own, LAGS), low),
            pltpu.VMEM((own, LAGS), low),
            pltpu.VMEM((bands,) + corr, low),
            pltpu.VMEM((bands,) + corr, low),
            pltpu.VMEM((recs, bands) + corr, low),
            pltpu.VMEM((2 * count, n), low),
            pltpu.VMEM((span, width), low),
            *sems(10, 4, 4, bands - 1, bands, 2, bands, bands),
            *sems(bands - 1, bands, bands - 1, bands, 1, 1),
        ],
        compiler_params=pltpu.CompilerParams(
            has_side_effects=True, collective_id=0, vmem_limit_bytes=VMEM_GRANT
        ),
        name="adjoint",
    )(records[0], pairs.T, observed, lag_mask, *tables)
    return result[None]


def fits_fused(shape, records, pairs):
    fibres, segs, recs = (shape[name] for name in ("fibre", "seg", "rec"))
    bands = fibres * segs
    width = records.shape[2] // (shape["groups"] * segs)
    return (
        fibres > 1
        and fibres & (fibres - 1) == 0
        and segs == 2
        and recs == 2
        and width % 128 == 0
        and width * segs <= 512
        and S // bands >= LAGS
        and pairs.shape[0] == bands * recs
    )


def solution(mesh):
    in_specs = (
        P("rec", "fibre", ("groups", "seg")),
        P(),
        P(("groups", "fibre", "seg"), None, None),
        P(("groups", "fibre", "seg"), None),
    )
    out_specs = P("rec", "fibre", ("groups", "seg"))
    shape = dict(mesh.shape)

    def run(records, pairs, observed, lag_mask):
        args = (records, pairs, observed, lag_mask)
        if not fits_fused(shape, records, pairs):
            return jax.shard_map(
                on_device, mesh=mesh, in_specs=in_specs, out_specs=out_specs, check_vma=False
            )(*args)
        tables = [jnp.asarray(t) for t in window_tables(shape["fibre"] * shape["seg"], shape["seg"])]

        def body(*blocks):
            return fused_on_device(shape, tables, *blocks)

        return jax.shard_map(
            body, mesh=mesh, in_specs=in_specs, out_specs=out_specs, check_vma=False
        )(*args)

    return run
```

```python
import functools

import jax
import jax.numpy as jnp
import numpy as np
from jax import lax
from jax.experimental import pallas as pl
from jax.experimental.pallas import tpu as pltpu
from jax.sharding import PartitionSpec as P

S = 2048
F = 1024
LAGS = 256
BLOCK = 32
CH_DEV = 64
VMEM_GRANT = 60899328


def forward_table():
    freq_index = jnp.arange(F, dtype=jnp.int32)
    time_index = jnp.arange(S, dtype=jnp.int32)
    phase = freq_index[:, None] * time_index[None, :] % S
    angles = phase.astype(jnp.float32) * (2.0 * jnp.pi / S)
    scale = 1.0 / jnp.sqrt(jnp.float32(S))
    return jnp.stack(
        [
            (jnp.cos(angles) * scale).astype(jnp.bfloat16),
            (-jnp.sin(angles) * scale).astype(jnp.bfloat16),
        ],
        axis=1,
    )


def lag_table():
    freq_index = jnp.arange(F, dtype=jnp.int32)
    shifts = (jnp.arange(LAGS, dtype=jnp.int32) - LAGS // 2) % S
    phase = freq_index[:, None] * shifts[None, :] % S
    angles = phase.astype(jnp.float32) * (2.0 * jnp.pi / S)
    scale = 1.0 / jnp.sqrt(jnp.float32(F))
    return jnp.stack(
        [
            (jnp.cos(angles) * scale).astype(jnp.bfloat16),
            (-jnp.sin(angles) * scale).astype(jnp.bfloat16),
        ],
        axis=1,
    )


def synthesize(incoming, table):
    count = incoming.shape[-1]
    flat = incoming.reshape(2 * F, count)
    result = jnp.einsum(
        "qn,qt->tn", flat, table.reshape(2 * F, S), preferred_element_type=jnp.float32
    )
    return result.astype(jnp.bfloat16)


def on_device(records, pairs, observed, lag_mask):
    fibre_count = lax.axis_size("fibre")
    seg_count = lax.axis_size("seg")
    spread_count = fibre_count * seg_count
    freq_dev = F // spread_count
    blocks_dev = CH_DEV // BLOCK
    block_count = CH_DEV * spread_count // BLOCK
    pair_total = pairs.shape[0]
    pairs_dev = pair_total // spread_count
    table = forward_table()
    lags = lag_table()
    spans = records.reshape(1, S // fibre_count, fibre_count, CH_DEV)
    incoming = lax.all_to_all(spans, "fibre", split_axis=2, concat_axis=1, tiled=True)
    count = incoming.shape[3]
    signal = incoming.reshape(S, count)
    result = jnp.einsum(
        "qs,sn->qn", table.reshape(2 * F, S), signal, preferred_element_type=jnp.float32
    )
    spectra = result.reshape(F, 2, count).astype(jnp.bfloat16)
    widened = lax.all_to_all(spectra, ("fibre", "seg"), split_axis=0, concat_axis=2, tiled=True)
    seg_blocks = fibre_count * blocks_dev
    slot_ids = (
        pairs % seg_blocks // blocks_dev * seg_count + pairs // seg_blocks
    ) * blocks_dev + pairs % blocks_dev
    blocks_grid = widened.reshape(freq_dev, 2, block_count, BLOCK)
    first_side = jnp.take(blocks_grid, slot_ids[:, 0], axis=2).astype(jnp.float32)
    second_side = jnp.take(blocks_grid, slot_ids[:, 1], axis=2).astype(jnp.float32)
    first_re, first_im = (first_side[:, 0], first_side[:, 1])
    second_re, second_im = (second_side[:, 0], second_side[:, 1])
    cross_re = first_re * second_re + first_im * second_im
    cross_im = first_im * second_re - first_re * second_im
    cross_spec = jnp.stack([cross_re, cross_im], axis=1).astype(jnp.bfloat16)
    cross_spec = cross_spec.reshape(freq_dev, 2, spread_count, pairs_dev * BLOCK)
    owned_spec = lax.all_to_all(
        cross_spec, ("fibre", "seg"), split_axis=2, concat_axis=0, tiled=True
    )
    owned_spec = owned_spec.reshape(F, 2, pairs_dev * BLOCK)
    partial_corr = jnp.einsum("wpx,wpl->xl", owned_spec, lags, preferred_element_type=jnp.float32)
    synthetic = (
        lax.psum(partial_corr.astype(jnp.bfloat16), "rec")
        .astype(jnp.float32)
        .reshape(pairs_dev, BLOCK, LAGS)
    )
    weights = lag_mask[:, None, :].astype(jnp.float32) * jnp.tanh(synthetic - observed)
    weights_low = weights.astype(jnp.bfloat16).reshape(pairs_dev * BLOCK, LAGS)
    adjoint_spec = jnp.einsum("xl,wpl->wpx", weights_low, lags, preferred_element_type=jnp.float32)
    adjoint_spec = adjoint_spec.astype(jnp.bfloat16).reshape(F, 2, 1, pairs_dev * BLOCK)
    returned = lax.all_to_all(
        adjoint_spec, ("fibre", "seg"), split_axis=0, concat_axis=2, tiled=True
    )
    returned = returned.reshape(freq_dev, 2, pair_total, BLOCK).astype(jnp.float32)
    adjoint_re, adjoint_im = (returned[:, 0], returned[:, 1])
    grad_first = jnp.stack(
        [
            adjoint_re * second_re - adjoint_im * second_im,
            adjoint_re * second_im + adjoint_im * second_re,
        ],
        axis=1,
    )
    grad_second = jnp.stack(
        [
            adjoint_re * first_re + adjoint_im * first_im,
            adjoint_re * first_im - adjoint_im * first_re,
        ],
        axis=1,
    )
    contributions = jnp.concatenate([grad_first, grad_second], axis=2)
    endpoint_ids = jnp.concatenate([slot_ids[:, 0], slot_ids[:, 1]])
    summed = jax.ops.segment_sum(
        jnp.moveaxis(contributions, 2, 0), endpoint_ids, num_segments=block_count
    )
    block_adjoint = jnp.moveaxis(summed, 0, 2).astype(jnp.bfloat16)
    outgoing = block_adjoint.reshape(freq_dev, 2, spread_count, CH_DEV)
    sources = synthesize(
        lax.all_to_all(outgoing, ("fibre", "seg"), split_axis=2, concat_axis=0, tiled=True), table
    )
    regrouped = lax.all_to_all(sources, "fibre", split_axis=0, concat_axis=1, tiled=True)
    return regrouped[None]


def window_tables(bands):
    span, reach, n = S // bands, LAGS // 2, S // bands + LAGS
    half = n // 2
    freqs, places = np.arange(half), np.arange(n)
    shifts = np.arange(LAGS) - reach
    ends = np.where(freqs == 0, 1.0, 2.0) / (n * 2.0 * np.sqrt(F))

    def table(times, scale):
        angles = (freqs[None, :] * times[:, None] % n) * (2.0 * np.pi / n)
        real, imag = np.cos(angles), -np.sin(angles)
        imag[:, 0] = np.where(times % 2 == 0, 1.0, -1.0)
        return np.concatenate([real * scale, imag * scale], axis=1)

    whole = table(places, np.ones(half))
    left, core, right = whole[:reach], whole[reach : reach + span], whole[reach + span :]
    signs = np.where(places % 2 == 0, 1.0, -1.0)[:, None]
    parts = (slice(reach, reach + span), slice(0, reach), slice(0, n), slice(0, 0))
    fixes = np.stack([row for p in parts for row in (whole[p].sum(0), -(signs * whole)[p].sum(0))]) / S
    lags = table(shifts, ends).T
    taps = table(shifts, np.ones(half))
    back = table(places[reach : reach + span], ends)
    halo = np.stack([left, right])
    return [t.astype(np.float32).astype(jnp.bfloat16) for t in (core, halo, lags, taps, back)] + [
        fixes.astype(np.float32)
    ]


def dot(left, right, left_dim=1, right_dim=0):
    return lax.dot_general(
        left,
        right,
        (((left_dim,), (right_dim,)), ((), ())),
        preferred_element_type=jnp.float32,
    )


def spectral_product(terms, sign):
    both = sum(p1 * q1 for (_, p1), (_, q1) in terms)
    real = sum(p0 * q0 for (p0, _), (q0, _) in terms)
    imag = sum(p1 * q0 - sign * (p0 * q1) for (p0, p1), (q0, q1) in terms)
    ends = lax.broadcasted_iota(jnp.int32, both.shape, 1) == 0
    return real + jnp.where(ends, 0.0, sign * both), jnp.where(ends, both, imag)


def fused_kernel(
    sizes, x_hbm, pairs_hbm, observed_hbm, mask_hbm, core_hbm, halo_hbm, lags_hbm, taps_hbm, back_hbm, fixes_hbm,
    out, pairs, core, halo, rest, observed, mask, core_table, halo_table, lags, taps, back, fixes,
    stage_sum, sum_across, stage_low, sum_low, sum_high, held_spec, core_spec, both_spec, first_core, first_left,
    full_spec, select, cross, stage_core, inbox_core, stage3, inbox3, inbox4, grads, stage6,
    high, load_sem, send1, recv1, send_sum, recv_sum, recv_high, core_send, core_recv, relay_send, relay_recv,
    send3, recv3, send4, recv4, send6, recv6,
):
    fibres, segs, recs = sizes
    bands = fibres * segs
    last = fibres - 1
    g, f, s, r = (lax.axis_index(name) for name in ("groups", "fibre", "seg", "rec"))
    o = 1 - s
    band = f * segs + s
    span, reach, width = S // bands, LAGS // 2, x_hbm.shape[1]
    n = span + LAGS
    half = n // 2
    blocks = width // BLOCK
    count = pairs.shape[1] * BLOCK
    own_count = count // recs
    low, full = jnp.bfloat16, jnp.float32

    def at(fibre, seg, rec):
        return (g, fibre, seg, rec)

    def at_band(index):
        return at(index // segs, index % segs, r)

    def remote(src, dst, send, recv, device):
        return pltpu.make_async_remote_copy(
            src_ref=src, dst_ref=dst, send_sem=send, recv_sem=recv,
            device_id=device, device_id_type=pl.DeviceIdType.MESH,
        )

    def push(src, dst, send, recv, device):
        copy = remote(src, dst, send, recv, device)
        copy.start()
        return copy

    def arrived(dst, recv):
        remote(dst, dst, recv, recv, at(f, s, 1 - r)).wait_recv()

    def signal(sem, device):
        pl.semaphore_signal(sem, inc=1, device_id=device, device_id_type=pl.DeviceIdType.MESH)

    def rows(start, size, unit):
        return pl.ds(pl.multiple_of(start, unit), size)

    def flipped(index, bits):
        result, bit = 0, 1
        while bit < bands:
            digit = index // bit % 2
            result += bit * (1 - digit if bits // bit % 2 else digit)
            bit *= 2
        return result

    partner = at(f, s, 1 - r)
    across = at(f, o, r)
    places = [(fi, si) for fi in range(fibres) for si in range(segs)]

    barrier = pltpu.get_barrier_semaphore()
    signal(barrier, partner)
    signal(barrier, across)
    for fi, si in places:

        @pl.when((fi >= f - 1) & (fi != f))
        def _():
            signal(barrier, at(fi, si, r))

    locals_ = [
        pltpu.make_async_copy(x_hbm.at[rows(span * s, span, reach)], core.at[s], load_sem.at[0]),
        pltpu.make_async_copy(x_hbm.at[rows(reach + reach * o, reach, reach)], halo.at[o, s], load_sem.at[1]),
        pltpu.make_async_copy(x_hbm.at[rows((2 * span - reach) * o, reach, reach)], rest, load_sem.at[2]),
    ]
    loads = [
        pltpu.make_async_copy(src, dst, load_sem.at[3 + i])
        for i, (src, dst) in enumerate(
            [
                (pairs_hbm, pairs), (core_hbm, core_table), (halo_hbm, halo_table), (fixes_hbm, fixes),
                (lags_hbm, lags), (observed_hbm.at[r], observed), (mask_hbm, mask), (taps_hbm, taps), (back_hbm, back),
            ]
        )
    ]
    for load in locals_ + loads:
        load.start()
    pl.semaphore_wait(barrier, segs * jnp.minimum(f + 2, fibres))
    after = push(
        x_hbm.at[pl.ds(2 * span - reach, reach)], halo.at[0, s], send1.at[0], recv1.at[2 + s],
        at((f + 1) % fibres, 0, r),
    )
    before = remote(
        x_hbm.at[pl.ds(0, reach)], halo.at[1, s], send1.at[1], recv1.at[4 + s], at((f + last) % fibres, 1, r)
    )
    core_cut = span // 2
    core_sends = [
        remote(
            x_hbm.at[rows(span * o + core_cut * i, core_cut, core_cut)], core.at[s, pl.ds(core_cut * i, core_cut)],
            send1.at[2 + i], recv1.at[6 + i], across,
        )
        for i in range(2)
    ]
    row = remote(
        x_hbm.at[rows(reach + reach * s, reach, reach)], halo.at[s, s], send1.at[4], recv1.at[1], across
    )

    @pl.when(s == 0)
    def _():
        core_sends[0].start()

    for fi, si in places:

        @pl.when(fi < f - 1)
        def _():
            signal(high, at(fi, si, r))

    for load in locals_:
        load.wait()
    folded = sum(
        part.astype(full).reshape(-1, 8, width).sum(axis=0) for part in (core[s], halo[o, s], rest[...])
    )
    odd = lax.broadcasted_iota(jnp.int32, folded.shape, 0) % 2 == 1
    sums = jnp.concatenate(
        [
            jnp.sum(folded, axis=0, keepdims=True),
            jnp.sum(jnp.where(odd, -folded, folded), axis=0, keepdims=True),
        ],
        axis=0,
    )
    stage_sum[...] = sums
    sends = [after, before, row] + core_sends
    sends.append(push(stage_sum, sum_across, send_sum.at[bands], recv_sum.at[0], across))
    sum_sends = [
        remote(stage_sum, sum_high.at[band], send_sum.at[fi * segs + si], recv_high.at[band], at(fi, si, r))
        for fi, si in places
    ]
    for (fi, si), copy in zip(places, sum_sends):

        @pl.when(fi < f)
        def _():
            copy.start()

    @pl.when(s == 1)
    def _():
        core_sends[0].start()

    core_sends[1].start()
    row.start()

    @pl.when(f > 0)
    def _():
        before.start()

    loads[0].wait()
    lane = lax.broadcasted_iota(jnp.int32, (1, 2 * own_count), 1)
    line = lax.broadcasted_iota(jnp.int32, select.shape[1:], 0)
    for h in range(recs):
        target = lane
        for side in range(2):
            for j in range(bands):
                first = side * own_count + j * BLOCK
                inside = (lane >= first) & (lane < first + BLOCK)
                target = jnp.where(inside, lane + (pairs[side, j * recs + h] * BLOCK - first), target)
        select[h] = jnp.where(line == target, 1.0, 0.0).astype(low)

    def put(spec, seg, value):
        spec[rows(seg * blocks, blocks, blocks)] = value.astype(low).reshape(blocks, BLOCK, n)

    def core_part(seg):
        part = dot(core[seg], core_table[...], 0, 0)
        held_spec[seg] = part
        put(core_spec, seg, part)

    loads[1].wait()
    core_part(s)
    arrived(sum_across, recv_sum.at[0])

    @pl.when(f > 0)
    def _():
        arrived(sum_low, recv_sum.at[1])

    stage_low[s] = stage_sum[...] + jnp.where(f > 0, sum_low[s], 0.0)
    stage_low[o] = sum_across[...] + jnp.where(f > 0, sum_low[o], 0.0)
    low_send = remote(stage_low, sum_low, send_sum.at[bands + 1], recv_sum.at[1], at((f + 1) % fibres, s, r))

    @pl.when(f < last)
    def _():
        low_send.start()

    for i in range(2):
        arrived(core.at[o, pl.ds(core_cut * i, core_cut)], recv1.at[6 + i])
    core_part(o)
    for fi, si in places:

        @pl.when(fi > f)
        def _():
            arrived(sum_high.at[fi * segs + si], recv_high.at[fi * segs + si])

    loads[2].wait()
    loads[3].wait()

    columns = []
    for seg in range(segs):
        total = stage_low[seg]
        for fi in range(1, fibres):
            total += jnp.where(fi > f, sum_high[fi * segs + seg], 0.0)
        columns.append(jnp.concatenate([total] * 4, axis=0).T)

    def fixed(value, seg, part):
        column = columns[seg]
        line = fixes[2 * part : 2 * part + 2, :]
        return value + (column[:, 0:1] * line[0:1] + column[:, 1:2] * line[1:2])

    for seg in range(segs):
        put(first_core, seg, fixed(held_spec[seg], seg, 0))

    @pl.when(s == 0)
    def _():
        for seg in range(segs):
            arrived(halo.at[0, seg], recv1.at[2 + seg])

    @pl.when(s == 1)
    def _():
        arrived(halo.at[0, 0], recv1.at[1])

    for seg in range(segs):
        part = dot(halo[0, seg], halo_table[0], 0, 0)
        put(first_left, seg, fixed(part, seg, 1))
        part += held_spec[seg]
        held_spec[seg] = part
        put(both_spec, seg, part)

    def block(spec, index):
        value = spec[index].astype(full)
        return value[:, :half], value[:, half:]

    cut = bands // 2

    def correlate(place, h, side):
        for i in range(cut):
            pair = (side * cut + i) * recs + h
            one, two = pairs[0, pair], pairs[1, pair]
            terms = [(block(first_core, one), block(both_spec, two)), (block(first_left, one), block(core_spec, two))]
            real, imag = spectral_product(terms, 1.0)
            here = pl.ds(i * BLOCK, BLOCK)
            cross[place, here, pl.ds(0, half)] = real.astype(low)
            cross[place, here, pl.ds(half, half)] = imag.astype(low)
        return dot(cross[place], lags[...])

    loads[4].wait()
    near = band // cut
    sides = (1 - near, near)
    for i, side in enumerate(sides):
        stage_core[i] = correlate(i, 1 - r, side).astype(low)
        sends.append(push(stage_core.at[i], inbox_core.at[i], core_send.at[i], core_recv.at[i], partner))

    @pl.when(f < last - 1)
    def _():
        pl.semaphore_wait(high, segs * (last - 1 - f))

    @pl.when(f == 0)
    def _():
        before.start()

    for i, side in enumerate(sides):
        partial = correlate(2 + i, r, side)
        arrived(inbox_core.at[i], core_recv.at[i])
        partial = (partial + inbox_core[i].astype(full)).astype(low)
        stage3[rows(side * cut, cut, cut)] = partial.reshape(cut, BLOCK, LAGS)
        for d in range(bands - 1 - i * cut, max(bands - 1 - (i + 1) * cut, 0), -1):
            j = flipped(band, d)
            sends.append(push(stage3.at[j], inbox3.at[band], send3.at[d - 1], recv3.at[band], at_band(j)))
    inbox3[band] = stage3[band]

    @pl.when(s == 0)
    def _():
        arrived(halo.at[1, 1], recv1.at[1])

    @pl.when(s == 1)
    def _():
        for seg in range(segs):
            arrived(halo.at[1, seg], recv1.at[4 + seg])

    for seg in range(segs):
        put(full_spec, seg, fixed(held_spec[seg] + dot(halo[1, seg], halo_table[1], 0, 0), seg, 2))
    loads[5].wait()
    loads[6].wait()
    for d in range(1, bands):
        k = flipped(band, d)
        arrived(inbox3.at[k], recv3.at[k])
    synthetic = inbox3[0].astype(full)
    for k in range(1, bands):
        synthetic += inbox3[k].astype(full)
    window = mask[pl.ds(r, 1), :].astype(full)
    inbox4[r, band] = (window * jnp.tanh(synthetic - observed[...])).astype(low)
    own = inbox4.at[r, band]
    for d in range(bands - 1, 0, -1):
        j = flipped(band, d)
        sends.append(push(own, own, send4.at[d - 1], recv4.at[band], at_band(j)))
    sends.append(push(own, own, relay_send.at[0], relay_recv.at[band], partner))
    for d in range(1, bands):
        k = flipped(band, d)
        arrived(inbox4.at[r, k], recv4.at[k])
        got = inbox4.at[r, k]
        sends.append(push(got, got, relay_send.at[d], relay_recv.at[k], partner))
    loads[7].wait()

    def gradients(h):
        spread = dot(inbox4[h].reshape(own_count, LAGS), taps[...])
        for j in range(bands):
            pair = j * recs + h
            filters = spread[j * BLOCK : (j + 1) * BLOCK]
            filters = filters[:, :half], filters[:, half:]
            first = block(full_spec, pairs[0, pair])
            second = block(full_spec, pairs[1, pair])
            for base, parts in (
                (j * BLOCK, spectral_product([(filters, second)], -1.0)),
                (own_count + j * BLOCK, spectral_product([(first, filters)], 1.0)),
            ):
                for p in range(2):
                    grads[pl.ds(base, BLOCK), pl.ds(p * half, half)] = parts[p].astype(low)

    def gathered(h, seg):
        return dot(select[h, rows(seg * width, width, width), :], grads[...])

    gradients(r)
    for seg in range(segs):
        held_spec[seg] = gathered(r, seg)
    for d in range(bands):
        k = flipped(band, d)
        arrived(inbox4.at[1 - r, k], relay_recv.at[k])
    gradients(1 - r)
    loads[8].wait()
    here = rows(span * s, span, span)
    there = rows(span * o, span, span)
    summed = (held_spec[o] + gathered(1 - r, o)).astype(low)
    for i in range(2):
        piece = pl.ds(i * core_cut, core_cut)
        stage6[piece, :] = dot(back[piece, :], summed, 1, 1).astype(low)
        dst = out.at[rows(span * s + i * core_cut, core_cut, core_cut), :]
        sends.append(push(stage6.at[piece], dst, send6.at[i], recv6.at[i], across))
    summed = (held_spec[s] + gathered(1 - r, s)).astype(low)
    out[here, :] = dot(back[...], summed, 1, 1).astype(low)
    for i in range(2):
        arrived(out.at[rows(span * o + i * core_cut, core_cut, core_cut), :], recv6.at[i])
    for copy in sends:
        copy.wait_send()
    for (fi, si), copy in zip(places, sum_sends):

        @pl.when(fi < f)
        def _():
            copy.wait_send()

    @pl.when(f < last)
    def _():
        low_send.wait_send()


def fused_on_device(mesh_shape, tables, records, pairs, observed, lag_mask):
    fibres, segs, recs = (mesh_shape[name] for name in ("fibre", "seg", "rec"))
    bands = fibres * segs
    _, extent, width = records.shape
    span, reach = S // bands, LAGS // 2
    n = span + LAGS
    count = pairs.shape[0] * BLOCK
    own = count // recs
    total = segs * width
    low, full = jnp.bfloat16, jnp.float32
    vmem = pl.BlockSpec(memory_space=pltpu.VMEM)
    hbm = pl.BlockSpec(memory_space=pltpu.HBM)
    corr = (BLOCK, LAGS)
    spec = pltpu.VMEM((total // BLOCK, BLOCK, n), low)

    def sems(*sizes):
        return [pltpu.SemaphoreType.DMA((size,)) for size in sizes]

    result = pl.pallas_call(
        functools.partial(fused_kernel, (fibres, segs, recs)),
        out_shape=pltpu.VMEM((extent, width), low),
        in_specs=[hbm] * 10,
        out_specs=vmem,
        scratch_shapes=[
            pltpu.SMEM((2, pairs.shape[0]), jnp.int32),
            pltpu.VMEM((segs, span, width), low),
            pltpu.VMEM((2, segs, reach, width), low),
            pltpu.VMEM((reach, width), low),
            pltpu.VMEM(corr, full),
            pltpu.VMEM(lag_mask.shape, jnp.int32),
            pltpu.VMEM((span, n), low),
            pltpu.VMEM((2, reach, n), low),
            pltpu.VMEM((n, LAGS), low),
            pltpu.VMEM((LAGS, n), low),
            pltpu.VMEM((span, n), low),
            pltpu.VMEM((8, n), full),
            pltpu.VMEM((2, width), full),
            pltpu.VMEM((2, width), full),
            pltpu.VMEM((segs, 2, width), full),
            pltpu.VMEM((segs, 2, width), full),
            pltpu.VMEM((bands, 2, width), full),
            pltpu.VMEM((segs, width, n), full),
            spec, spec, spec, spec, spec,
            pltpu.VMEM((recs, total, 2 * own), low),
            pltpu.VMEM((2 * recs, own // 2, n), low),
            pltpu.VMEM((2, own // 2, LAGS), low),
            pltpu.VMEM((2, own // 2, LAGS), low),
            pltpu.VMEM((bands,) + corr, low),
            pltpu.VMEM((bands,) + corr, low),
            pltpu.VMEM((recs, bands) + corr, low),
            pltpu.VMEM((2 * own, n), low),
            pltpu.VMEM((span, width), low),
            pltpu.SemaphoreType.REGULAR,
            *sems(12, 5, 8, bands + 2, 2, bands, 2, 2, bands, bands),
            *sems(bands - 1, bands, bands - 1, bands, 2, 2),
        ],
        compiler_params=pltpu.CompilerParams(
            has_side_effects=True, collective_id=0, vmem_limit_bytes=VMEM_GRANT
        ),
        name="adjoint",
    )(records[0], pairs.T, observed, lag_mask, *tables)
    return result[None]


def fits_fused(shape, records, pairs):
    fibres, segs, recs = (shape[name] for name in ("fibre", "seg", "rec"))
    bands = fibres * segs
    width = records.shape[2] // (shape["groups"] * segs)
    return (
        fibres > 1
        and fibres & (fibres - 1) == 0
        and segs == 2
        and recs == 2
        and width % 128 == 0
        and width * segs <= 512
        and S // bands >= LAGS
        and pairs.shape[0] == bands * recs
    )


def solution(mesh):
    in_specs = (
        P("rec", "fibre", ("groups", "seg")),
        P(),
        P(("groups", "fibre", "seg"), None, None),
        P(("groups", "fibre", "seg"), None),
    )
    out_specs = P("rec", "fibre", ("groups", "seg"))
    shape = dict(mesh.shape)

    def run(records, pairs, observed, lag_mask):
        args = (records, pairs, observed, lag_mask)
        if not fits_fused(shape, records, pairs):
            return jax.shard_map(
                on_device, mesh=mesh, in_specs=in_specs, out_specs=out_specs, check_vma=False
            )(*args)
        tables = [jnp.asarray(t) for t in window_tables(shape["fibre"] * shape["seg"])]

        def body(*blocks):
            return fused_on_device(shape, tables, *blocks)

        return jax.shard_map(
            body, mesh=mesh, in_specs=in_specs, out_specs=out_specs, check_vma=False
        )(*args)

    return run
```

```python
import functools

import jax
import jax.numpy as jnp
import numpy as np
from jax import lax
from jax.experimental import pallas as pl
from jax.experimental.pallas import tpu as pltpu
from jax.sharding import PartitionSpec as P

S = 2048
F = 1024
LAGS = 256
BLOCK = 32
CH_DEV = 64
PIECE = 32
VMEM_GRANT = 60899328


def forward_table():
    freq_index = jnp.arange(F, dtype=jnp.int32)
    time_index = jnp.arange(S, dtype=jnp.int32)
    phase = freq_index[:, None] * time_index[None, :] % S
    angles = phase.astype(jnp.float32) * (2.0 * jnp.pi / S)
    scale = 1.0 / jnp.sqrt(jnp.float32(S))
    return jnp.stack(
        [
            (jnp.cos(angles) * scale).astype(jnp.bfloat16),
            (-jnp.sin(angles) * scale).astype(jnp.bfloat16),
        ],
        axis=1,
    )


def lag_table():
    freq_index = jnp.arange(F, dtype=jnp.int32)
    shifts = (jnp.arange(LAGS, dtype=jnp.int32) - LAGS // 2) % S
    phase = freq_index[:, None] * shifts[None, :] % S
    angles = phase.astype(jnp.float32) * (2.0 * jnp.pi / S)
    scale = 1.0 / jnp.sqrt(jnp.float32(F))
    return jnp.stack(
        [
            (jnp.cos(angles) * scale).astype(jnp.bfloat16),
            (-jnp.sin(angles) * scale).astype(jnp.bfloat16),
        ],
        axis=1,
    )


def synthesize(incoming, table):
    count = incoming.shape[-1]
    flat = incoming.reshape(2 * F, count)
    result = jnp.einsum(
        "qn,qt->tn", flat, table.reshape(2 * F, S), preferred_element_type=jnp.float32
    )
    return result.astype(jnp.bfloat16)


def on_device(records, pairs, observed, lag_mask):
    fibre_count = lax.axis_size("fibre")
    seg_count = lax.axis_size("seg")
    spread_count = fibre_count * seg_count
    freq_dev = F // spread_count
    blocks_dev = CH_DEV // BLOCK
    block_count = CH_DEV * spread_count // BLOCK
    pair_total = pairs.shape[0]
    pairs_dev = pair_total // spread_count
    table = forward_table()
    lags = lag_table()
    spans = records.reshape(1, S // fibre_count, fibre_count, CH_DEV)
    incoming = lax.all_to_all(spans, "fibre", split_axis=2, concat_axis=1, tiled=True)
    count = incoming.shape[3]
    signal = incoming.reshape(S, count)
    result = jnp.einsum(
        "qs,sn->qn", table.reshape(2 * F, S), signal, preferred_element_type=jnp.float32
    )
    spectra = result.reshape(F, 2, count).astype(jnp.bfloat16)
    widened = lax.all_to_all(spectra, ("fibre", "seg"), split_axis=0, concat_axis=2, tiled=True)
    seg_blocks = fibre_count * blocks_dev
    slot_ids = (
        pairs % seg_blocks // blocks_dev * seg_count + pairs // seg_blocks
    ) * blocks_dev + pairs % blocks_dev
    blocks_grid = widened.reshape(freq_dev, 2, block_count, BLOCK)
    first_side = jnp.take(blocks_grid, slot_ids[:, 0], axis=2).astype(jnp.float32)
    second_side = jnp.take(blocks_grid, slot_ids[:, 1], axis=2).astype(jnp.float32)
    first_re, first_im = (first_side[:, 0], first_side[:, 1])
    second_re, second_im = (second_side[:, 0], second_side[:, 1])
    cross_re = first_re * second_re + first_im * second_im
    cross_im = first_im * second_re - first_re * second_im
    cross_spec = jnp.stack([cross_re, cross_im], axis=1).astype(jnp.bfloat16)
    cross_spec = cross_spec.reshape(freq_dev, 2, spread_count, pairs_dev * BLOCK)
    owned_spec = lax.all_to_all(
        cross_spec, ("fibre", "seg"), split_axis=2, concat_axis=0, tiled=True
    )
    owned_spec = owned_spec.reshape(F, 2, pairs_dev * BLOCK)
    partial_corr = jnp.einsum("wpx,wpl->xl", owned_spec, lags, preferred_element_type=jnp.float32)
    synthetic = (
        lax.psum(partial_corr.astype(jnp.bfloat16), "rec")
        .astype(jnp.float32)
        .reshape(pairs_dev, BLOCK, LAGS)
    )
    weights = lag_mask[:, None, :].astype(jnp.float32) * jnp.tanh(synthetic - observed)
    weights_low = weights.astype(jnp.bfloat16).reshape(pairs_dev * BLOCK, LAGS)
    adjoint_spec = jnp.einsum("xl,wpl->wpx", weights_low, lags, preferred_element_type=jnp.float32)
    adjoint_spec = adjoint_spec.astype(jnp.bfloat16).reshape(F, 2, 1, pairs_dev * BLOCK)
    returned = lax.all_to_all(
        adjoint_spec, ("fibre", "seg"), split_axis=0, concat_axis=2, tiled=True
    )
    returned = returned.reshape(freq_dev, 2, pair_total, BLOCK).astype(jnp.float32)
    adjoint_re, adjoint_im = (returned[:, 0], returned[:, 1])
    grad_first = jnp.stack(
        [
            adjoint_re * second_re - adjoint_im * second_im,
            adjoint_re * second_im + adjoint_im * second_re,
        ],
        axis=1,
    )
    grad_second = jnp.stack(
        [
            adjoint_re * first_re + adjoint_im * first_im,
            adjoint_re * first_im - adjoint_im * first_re,
        ],
        axis=1,
    )
    contributions = jnp.concatenate([grad_first, grad_second], axis=2)
    endpoint_ids = jnp.concatenate([slot_ids[:, 0], slot_ids[:, 1]])
    summed = jax.ops.segment_sum(
        jnp.moveaxis(contributions, 2, 0), endpoint_ids, num_segments=block_count
    )
    block_adjoint = jnp.moveaxis(summed, 0, 2).astype(jnp.bfloat16)
    outgoing = block_adjoint.reshape(freq_dev, 2, spread_count, CH_DEV)
    sources = synthesize(
        lax.all_to_all(outgoing, ("fibre", "seg"), split_axis=2, concat_axis=0, tiled=True), table
    )
    regrouped = lax.all_to_all(sources, "fibre", split_axis=0, concat_axis=1, tiled=True)
    return regrouped[None]


def window_tables(bands):
    span, reach, n = S // bands, LAGS // 2, S // bands + LAGS
    half = n // 2
    freqs, places = np.arange(half), np.arange(n)
    shifts = np.arange(LAGS) - reach
    ends = np.where(freqs == 0, 1.0, 2.0) / (n * 2.0 * np.sqrt(F))

    def table(times, scale):
        angles = (freqs[None, :] * times[:, None] % n) * (2.0 * np.pi / n)
        real, imag = np.cos(angles), -np.sin(angles)
        imag[:, 0] = np.where(times % 2 == 0, 1.0, -1.0)
        return np.concatenate([real * scale, imag * scale], axis=1)

    whole = table(places, np.ones(half))
    left, core, right = whole[:reach], whole[reach : reach + span], whole[reach + span :]
    lags = table(shifts, ends).T
    taps = table(shifts, np.ones(half))
    back = table(places[reach : reach + span], ends)
    halo = np.stack([left, right])
    return [t.astype(np.float32).astype(jnp.bfloat16) for t in (core, halo, lags, taps, back)]


def dot(left, right, left_dim=1, right_dim=0):
    return lax.dot_general(
        left,
        right,
        (((left_dim,), (right_dim,)), ((), ())),
        preferred_element_type=jnp.float32,
    )


def spectral_product(terms, sign):
    both = sum(p1 * q1 for (_, p1), (_, q1) in terms)
    real = sum(p0 * q0 for (p0, _), (q0, _) in terms)
    imag = sum(p1 * q0 - sign * (p0 * q1) for (p0, p1), (q0, q1) in terms)
    ends = lax.broadcasted_iota(jnp.int32, both.shape, 1) == 0
    return real + jnp.where(ends, 0.0, sign * both), jnp.where(ends, both, imag)


def fused_kernel(
    sizes, x_hbm, pairs_hbm, observed_hbm, mask_hbm, core_hbm, halo_hbm, lags_hbm, taps_hbm, back_hbm,
    out, pairs, core, halo, rest, observed, mask, core_table, halo_table, lags, taps, back,
    inbox_sum, stage_total, inbox_total, columns, held_spec, core_spec, both_spec, left_spec,
    full_spec, select, cross, stage_core, inbox_core, stage3, inbox3, inbox4, grads, stage6,
    high, load_sem, send1, recv1, send_sum, recv_sum, total_sem, core_send, core_recv, relay_send, relay_recv,
    send3, recv3, send4, recv4, send6, recv6,
):
    fibres, segs, recs = sizes
    bands = fibres * segs
    last = fibres - 1
    g, f, s, r = (lax.axis_index(name) for name in ("groups", "fibre", "seg", "rec"))
    o = 1 - s
    band = f * segs + s
    span, reach, width = S // bands, LAGS // 2, x_hbm.shape[1]
    n = span + LAGS
    half = n // 2
    blocks = width // BLOCK
    count = pairs.shape[1] * BLOCK
    own_count = count // recs
    low, full = jnp.bfloat16, jnp.float32

    def at(fibre, seg, rec):
        return (g, fibre, seg, rec)

    def at_band(index):
        return at(index // segs, index % segs, r)

    def remote(src, dst, send, recv, device):
        return pltpu.make_async_remote_copy(
            src_ref=src, dst_ref=dst, send_sem=send, recv_sem=recv,
            device_id=device, device_id_type=pl.DeviceIdType.MESH,
        )

    def push(src, dst, send, recv, device):
        copy = remote(src, dst, send, recv, device)
        copy.start()
        return copy

    def arrived(dst, recv):
        remote(dst, dst, recv, recv, at(f, s, 1 - r)).wait_recv()

    def signal(sem, device):
        pl.semaphore_signal(sem, inc=1, device_id=device, device_id_type=pl.DeviceIdType.MESH)

    def rows(start, size, unit):
        return pl.ds(pl.multiple_of(start, unit), size)

    def flipped(index, bits):
        result, bit = 0, 1
        while bit < bands:
            digit = index // bit % 2
            result += bit * (1 - digit if bits // bit % 2 else digit)
            bit *= 2
        return result

    class bulk:
        def __init__(self, first, size, dst, send, recv, device):
            self.whole = remote(x_hbm.at[rows(first, size, PIECE)], dst, send, recv, device)
            self.pieces = [
                remote(x_hbm.at[rows(first + i, PIECE, PIECE)], dst.at[pl.ds(i, PIECE)], send, recv, device)
                for i in range(0, size, PIECE)
            ]

        def start(self):
            for piece in self.pieces:
                piece.start()

        def wait_send(self):
            self.whole.wait_send()

    partner = at(f, s, 1 - r)
    across = at(f, o, r)
    places = [(fi, si) for fi in range(fibres) for si in range(segs)]

    barrier = pltpu.get_barrier_semaphore()
    signal(barrier, partner)
    signal(barrier, across)
    for fi, si in places:

        @pl.when((fi >= f - 1) & (fi != f))
        def _():
            signal(barrier, at(fi, si, r))

    locals_ = [
        pltpu.make_async_copy(x_hbm.at[rows(span * s, span, reach)], core.at[s], load_sem.at[0]),
        pltpu.make_async_copy(x_hbm.at[rows(reach + reach * o, reach, reach)], halo.at[o, s], load_sem.at[1]),
        pltpu.make_async_copy(x_hbm.at[rows((2 * span - reach) * o, reach, reach)], rest, load_sem.at[2]),
    ]
    loads = [
        pltpu.make_async_copy(src, dst, load_sem.at[3 + i])
        for i, (src, dst) in enumerate(
            [
                (pairs_hbm, pairs), (core_hbm, core_table), (halo_hbm, halo_table), (lags_hbm, lags), (observed_hbm.at[r], observed), (mask_hbm, mask), (taps_hbm, taps), (back_hbm, back),
            ]
        )
    ]
    for load in locals_ + loads:
        load.start()
    pl.semaphore_wait(barrier, segs * jnp.minimum(f + 2, fibres))
    after = bulk(
        2 * span - reach, reach, halo.at[0, s], send1.at[0], recv1.at[2 + s], at((f + 1) % fibres, 0, r)
    )
    before = bulk(0, reach, halo.at[1, s], send1.at[1], recv1.at[4 + s], at((f + last) % fibres, 1, r))
    core_cut = span // 2
    core_sends = bulk(span * o, span, core.at[s], send1.at[2], recv1.at[0], across)
    row = bulk(reach + reach * s, reach, halo.at[s, s], send1.at[4], recv1.at[1], across)

    @pl.when((f < last))
    def _():
        after.start()

    core_sends.start()

    @pl.when(s == 0)
    def _():
        row.start()

    @pl.when(f == last)
    def _():
        after.start()

    for fi, si in places:

        @pl.when(fi < f - 1)
        def _():
            signal(high, at(fi, si, r))

    for load in locals_:
        load.wait()
    folded = sum(
        part.astype(full).reshape(-1, 8, width).sum(axis=0) for part in (core[s], halo[o, s], rest[...])
    )
    odd = lax.broadcasted_iota(jnp.int32, folded.shape, 0) % 2 == 1
    inbox_sum[band] = jnp.concatenate(
        [
            jnp.sum(folded, axis=0, keepdims=True),
            jnp.sum(jnp.where(odd, -folded, folded), axis=0, keepdims=True),
        ],
        axis=0,
    )
    sends = [after, before, row, core_sends]
    own_sum = inbox_sum.at[band]
    sum_sends = [
        remote(own_sum, own_sum, send_sum.at[fi * segs + si], recv_sum.at[band], at(fi, si, r)) for fi, si in places
    ]
    across_sum = push(own_sum, own_sum, send_sum.at[bands], recv_sum.at[band], across)
    sends.append(across_sum)
    for (fi, si), copy in zip(places, sum_sends):

        @pl.when(fi < f)
        def _():
            copy.start()

    loads[0].wait()
    lane = lax.broadcasted_iota(jnp.int32, (1, 2 * own_count), 1)
    line = lax.broadcasted_iota(jnp.int32, select.shape[1:], 0)
    for h in range(recs):
        target = lane
        for side in range(2):
            for j in range(bands):
                first = side * own_count + j * BLOCK
                inside = (lane >= first) & (lane < first + BLOCK)
                target = jnp.where(inside, lane + (pairs[side, j * recs + h] * BLOCK - first), target)
        select[h] = jnp.where(line == target, 1.0, 0.0).astype(low)

    def put(spec, seg, value):
        spec[rows(seg * blocks, blocks, blocks)] = value.astype(low).reshape(blocks, BLOCK, n)

    def core_part(seg):
        part = dot(core[seg], core_table[...], 0, 0)
        held_spec[seg] = part
        put(core_spec, seg, part)

    loads[1].wait()
    core_part(s)
    arrived(core.at[o], recv1.at[0])
    core_part(o)
    loads[2].wait()

    @pl.when(s == 0)
    def _():
        for seg in range(segs):
            arrived(halo.at[0, seg], recv1.at[2 + seg])

    @pl.when(s == 1)
    def _():
        arrived(halo.at[0, 0], recv1.at[1])

    for seg in range(segs):
        part = dot(halo[0, seg], halo_table[0], 0, 0)
        put(left_spec, seg, part)
        part += held_spec[seg]
        held_spec[seg] = part
        put(both_spec, seg, part)

    def block(spec, index):
        value = spec[index].astype(full)
        return value[:, :half], value[:, half:]

    cut = bands // 2

    def correlate(place, h, side):
        for i in range(cut):
            pair = (side * cut + i) * recs + h
            one, two = pairs[0, pair], pairs[1, pair]
            terms = [(block(core_spec, one), block(both_spec, two)), (block(left_spec, one), block(core_spec, two))]
            real, imag = spectral_product(terms, 1.0)
            here = pl.ds(i * BLOCK, BLOCK)
            cross[place, here, pl.ds(0, half)] = real.astype(low)
            cross[place, here, pl.ds(half, half)] = imag.astype(low)
        return dot(cross[place], lags[...])

    loads[3].wait()
    near = band // cut
    sides = (1 - near, near)
    for i, side in enumerate(sides):
        stage_core[i] = correlate(i, 1 - r, side).astype(low)
        sends.append(push(stage_core.at[i], inbox_core.at[i], core_send.at[i], core_recv.at[i], partner))

    @pl.when(f < last - 1)
    def _():
        pl.semaphore_wait(high, segs * (last - 1 - f))

    for (fi, si), copy in zip(places, sum_sends):

        @pl.when(fi > f)
        def _():
            copy.start()

    for i, side in enumerate(sides):
        partial = correlate(2 + i, r, side)
        arrived(inbox_core.at[i], core_recv.at[i])
        partial = (partial + inbox_core[i].astype(full)).astype(low)
        stage3[rows(side * cut, cut, cut)] = partial.reshape(cut, BLOCK, LAGS)
        for d in range(bands - 1 - i * cut, max(bands - 1 - (i + 1) * cut, 0), -1):
            j = flipped(band, d)
            sends.append(push(stage3.at[j], inbox3.at[band], send3.at[d - 1], recv3.at[band], at_band(j)))
    inbox3[band] = stage3[band]

    @pl.when(s == 1)
    def _():
        row.start()

    before.start()

    @pl.when(s == 0)
    def _():
        arrived(halo.at[1, 1], recv1.at[1])

    @pl.when(s == 1)
    def _():
        for seg in range(segs):
            arrived(halo.at[1, seg], recv1.at[4 + seg])

    for d in range(1, bands):
        k = flipped(band, d)
        arrived(inbox_sum.at[k], recv_sum.at[k])
    for seg in range(segs):
        stage_total[seg] = sum(inbox_sum[fi * segs + seg] for fi in range(fibres))
    sends.append(push(stage_total, inbox_total, total_sem.at[0], total_sem.at[1], partner))
    head = lax.broadcasted_iota(jnp.int32, (1, half), 1) == 0
    for seg in range(segs):
        total = jnp.concatenate([stage_total[seg]] * 4, axis=0).T * (n / S)
        value = held_spec[seg] + dot(halo[1, seg], halo_table[1], 0, 0)
        value = jnp.concatenate(
            [
                value[:, :half] + jnp.where(head, total[:, 0:1], 0.0),
                value[:, half:] - jnp.where(head, total[:, 1:2], 0.0),
            ],
            axis=1,
        )
        put(full_spec, seg, value)
    arrived(inbox_total, total_sem.at[1])
    for seg in range(segs):
        total = jnp.concatenate([stage_total[seg], inbox_total[seg]] * 2, axis=0)
        columns[pl.ds(seg * blocks, blocks)] = total.T.reshape(blocks, BLOCK, 8)
    loads[4].wait()
    loads[5].wait()
    ends = columns[pairs[0, band * recs + r]] * columns[pairs[1, band * recs + r]]
    flat = ends[:, 0:1] + ends[:, 2:3]
    alternating = ends[:, 1:2] + ends[:, 3:4]
    even = lax.broadcasted_iota(jnp.int32, (BLOCK, LAGS), 1) % 2 == reach % 2
    offset = (flat + jnp.where(even, -alternating, alternating)) * (1.0 / (2.0 * S * F**0.5))
    for d in range(1, bands):
        k = flipped(band, d)
        arrived(inbox3.at[k], recv3.at[k])
    synthetic = offset + inbox3[0].astype(full)
    for k in range(1, bands):
        synthetic += inbox3[k].astype(full)
    window = mask[pl.ds(r, 1), :].astype(full)
    inbox4[r, band] = (window * jnp.tanh(synthetic - observed[...])).astype(low)
    own = inbox4.at[r, band]
    for d in range(bands - 1, 0, -1):
        j = flipped(band, d)
        sends.append(push(own, own, send4.at[d - 1], recv4.at[band], at_band(j)))
    sends.append(push(own, own, relay_send.at[0], relay_recv.at[band], partner))
    for d in range(1, bands):
        k = flipped(band, d)
        arrived(inbox4.at[r, k], recv4.at[k])
        got = inbox4.at[r, k]
        sends.append(push(got, got, relay_send.at[d], relay_recv.at[k], partner))
    loads[6].wait()

    def gradients(h):
        spread = dot(inbox4[h].reshape(own_count, LAGS), taps[...])
        for j in range(bands):
            pair = j * recs + h
            filters = spread[j * BLOCK : (j + 1) * BLOCK]
            filters = filters[:, :half], filters[:, half:]
            first = block(full_spec, pairs[0, pair])
            second = block(full_spec, pairs[1, pair])
            for base, parts in (
                (j * BLOCK, spectral_product([(filters, second)], -1.0)),
                (own_count + j * BLOCK, spectral_product([(first, filters)], 1.0)),
            ):
                for p in range(2):
                    grads[pl.ds(base, BLOCK), pl.ds(p * half, half)] = parts[p].astype(low)

    def gathered(h, seg):
        return dot(select[h, rows(seg * width, width, width), :], grads[...])

    gradients(r)
    for seg in range(segs):
        held_spec[seg] = gathered(r, seg)
    for d in range(bands):
        k = flipped(band, d)
        arrived(inbox4.at[1 - r, k], relay_recv.at[k])
    gradients(1 - r)
    loads[7].wait()
    here = rows(span * s, span, span)
    there = rows(span * o, span, span)
    summed = (held_spec[o] + gathered(1 - r, o)).astype(low)
    for i in range(2):
        piece = pl.ds(i * core_cut, core_cut)
        stage6[piece, :] = dot(back[piece, :], summed, 1, 1).astype(low)
        dst = out.at[rows(span * s + i * core_cut, core_cut, core_cut), :]
        sends.append(push(stage6.at[piece], dst, send6.at[i], recv6.at[i], across))
    summed = (held_spec[s] + gathered(1 - r, s)).astype(low)
    out[here, :] = dot(back[...], summed, 1, 1).astype(low)
    for i in range(2):
        arrived(out.at[rows(span * o + i * core_cut, core_cut, core_cut), :], recv6.at[i])
    for copy in sends:
        copy.wait_send()
    for (fi, si), copy in zip(places, sum_sends):

        @pl.when(fi != f)
        def _():
            copy.wait_send()


def fused_on_device(mesh_shape, tables, records, pairs, observed, lag_mask):
    fibres, segs, recs = (mesh_shape[name] for name in ("fibre", "seg", "rec"))
    bands = fibres * segs
    _, extent, width = records.shape
    span, reach = S // bands, LAGS // 2
    n = span + LAGS
    count = pairs.shape[0] * BLOCK
    own = count // recs
    total = segs * width
    low, full = jnp.bfloat16, jnp.float32
    vmem = pl.BlockSpec(memory_space=pltpu.VMEM)
    hbm = pl.BlockSpec(memory_space=pltpu.HBM)
    corr = (BLOCK, LAGS)
    spec = pltpu.VMEM((total // BLOCK, BLOCK, n), low)

    def sems(*sizes):
        return [pltpu.SemaphoreType.DMA((size,)) for size in sizes]

    result = pl.pallas_call(
        functools.partial(fused_kernel, (fibres, segs, recs)),
        out_shape=pltpu.VMEM((extent, width), low),
        in_specs=[hbm] * 9,
        out_specs=vmem,
        scratch_shapes=[
            pltpu.SMEM((2, pairs.shape[0]), jnp.int32),
            pltpu.VMEM((segs, span, width), low),
            pltpu.VMEM((2, segs, reach, width), low),
            pltpu.VMEM((reach, width), low),
            pltpu.VMEM(corr, full),
            pltpu.VMEM(lag_mask.shape, jnp.int32),
            pltpu.VMEM((span, n), low),
            pltpu.VMEM((2, reach, n), low),
            pltpu.VMEM((n, LAGS), low),
            pltpu.VMEM((LAGS, n), low),
            pltpu.VMEM((span, n), low),
            pltpu.VMEM((bands, 2, width), full),
            pltpu.VMEM((segs, 2, width), full),
            pltpu.VMEM((segs, 2, width), full),
            pltpu.VMEM((total // BLOCK, BLOCK, 8), full),
            pltpu.VMEM((segs, width, n), full),
            spec, spec, spec, spec,
            pltpu.VMEM((recs, total, 2 * own), low),
            pltpu.VMEM((2 * recs, own // 2, n), low),
            pltpu.VMEM((2, own // 2, LAGS), low),
            pltpu.VMEM((2, own // 2, LAGS), low),
            pltpu.VMEM((bands,) + corr, low),
            pltpu.VMEM((bands,) + corr, low),
            pltpu.VMEM((recs, bands) + corr, low),
            pltpu.VMEM((2 * own, n), low),
            pltpu.VMEM((span, width), low),
            pltpu.SemaphoreType.REGULAR,
            *sems(11, 5, 8, bands + 1, bands, 2, 2, 2, bands, bands),
            *sems(bands - 1, bands, bands - 1, bands, 2, 2),
        ],
        compiler_params=pltpu.CompilerParams(
            has_side_effects=True, collective_id=0, vmem_limit_bytes=VMEM_GRANT
        ),
        name="adjoint",
    )(records[0], pairs.T, observed, lag_mask, *tables)
    return result[None]


def fits_fused(shape, records, pairs):
    fibres, segs, recs = (shape[name] for name in ("fibre", "seg", "rec"))
    bands = fibres * segs
    width = records.shape[2] // (shape["groups"] * segs)
    return (
        fibres > 1
        and fibres & (fibres - 1) == 0
        and segs == 2
        and recs == 2
        and width % 128 == 0
        and width * segs <= 512
        and S // bands >= LAGS
        and pairs.shape[0] == bands * recs
    )


def solution(mesh):
    in_specs = (
        P("rec", "fibre", ("groups", "seg")),
        P(),
        P(("groups", "fibre", "seg"), None, None),
        P(("groups", "fibre", "seg"), None),
    )
    out_specs = P("rec", "fibre", ("groups", "seg"))
    shape = dict(mesh.shape)

    def run(records, pairs, observed, lag_mask):
        args = (records, pairs, observed, lag_mask)
        if not fits_fused(shape, records, pairs):
            return jax.shard_map(
                on_device, mesh=mesh, in_specs=in_specs, out_specs=out_specs, check_vma=False
            )(*args)
        tables = [jnp.asarray(t) for t in window_tables(shape["fibre"] * shape["seg"])]

        def body(*blocks):
            return fused_on_device(shape, tables, *blocks)

        return jax.shard_map(
            body, mesh=mesh, in_specs=in_specs, out_specs=out_specs, check_vma=False
        )(*args)

    return run
```

```python
import functools

import jax
import jax.numpy as jnp
import numpy as np
from jax import lax
from jax.experimental import pallas as pl
from jax.experimental.pallas import tpu as pltpu
from jax.sharding import PartitionSpec as P

S = 2048
F = 1024
LAGS = 256
BLOCK = 32
CH_DEV = 64
PIECE = 32
VMEM_GRANT = 60899328


def forward_table():
    freq_index = jnp.arange(F, dtype=jnp.int32)
    time_index = jnp.arange(S, dtype=jnp.int32)
    phase = freq_index[:, None] * time_index[None, :] % S
    angles = phase.astype(jnp.float32) * (2.0 * jnp.pi / S)
    scale = 1.0 / jnp.sqrt(jnp.float32(S))
    return jnp.stack(
        [
            (jnp.cos(angles) * scale).astype(jnp.bfloat16),
            (-jnp.sin(angles) * scale).astype(jnp.bfloat16),
        ],
        axis=1,
    )


def lag_table():
    freq_index = jnp.arange(F, dtype=jnp.int32)
    shifts = (jnp.arange(LAGS, dtype=jnp.int32) - LAGS // 2) % S
    phase = freq_index[:, None] * shifts[None, :] % S
    angles = phase.astype(jnp.float32) * (2.0 * jnp.pi / S)
    scale = 1.0 / jnp.sqrt(jnp.float32(F))
    return jnp.stack(
        [
            (jnp.cos(angles) * scale).astype(jnp.bfloat16),
            (-jnp.sin(angles) * scale).astype(jnp.bfloat16),
        ],
        axis=1,
    )


def synthesize(incoming, table):
    count = incoming.shape[-1]
    flat = incoming.reshape(2 * F, count)
    result = jnp.einsum(
        "qn,qt->tn", flat, table.reshape(2 * F, S), preferred_element_type=jnp.float32
    )
    return result.astype(jnp.bfloat16)


def on_device(records, pairs, observed, lag_mask):
    fibre_count = lax.axis_size("fibre")
    seg_count = lax.axis_size("seg")
    spread_count = fibre_count * seg_count
    freq_dev = F // spread_count
    blocks_dev = CH_DEV // BLOCK
    block_count = CH_DEV * spread_count // BLOCK
    pair_total = pairs.shape[0]
    pairs_dev = pair_total // spread_count
    table = forward_table()
    lags = lag_table()
    spans = records.reshape(1, S // fibre_count, fibre_count, CH_DEV)
    incoming = lax.all_to_all(spans, "fibre", split_axis=2, concat_axis=1, tiled=True)
    count = incoming.shape[3]
    signal = incoming.reshape(S, count)
    result = jnp.einsum(
        "qs,sn->qn", table.reshape(2 * F, S), signal, preferred_element_type=jnp.float32
    )
    spectra = result.reshape(F, 2, count).astype(jnp.bfloat16)
    widened = lax.all_to_all(spectra, ("fibre", "seg"), split_axis=0, concat_axis=2, tiled=True)
    seg_blocks = fibre_count * blocks_dev
    slot_ids = (
        pairs % seg_blocks // blocks_dev * seg_count + pairs // seg_blocks
    ) * blocks_dev + pairs % blocks_dev
    blocks_grid = widened.reshape(freq_dev, 2, block_count, BLOCK)
    first_side = jnp.take(blocks_grid, slot_ids[:, 0], axis=2).astype(jnp.float32)
    second_side = jnp.take(blocks_grid, slot_ids[:, 1], axis=2).astype(jnp.float32)
    first_re, first_im = (first_side[:, 0], first_side[:, 1])
    second_re, second_im = (second_side[:, 0], second_side[:, 1])
    cross_re = first_re * second_re + first_im * second_im
    cross_im = first_im * second_re - first_re * second_im
    cross_spec = jnp.stack([cross_re, cross_im], axis=1).astype(jnp.bfloat16)
    cross_spec = cross_spec.reshape(freq_dev, 2, spread_count, pairs_dev * BLOCK)
    owned_spec = lax.all_to_all(
        cross_spec, ("fibre", "seg"), split_axis=2, concat_axis=0, tiled=True
    )
    owned_spec = owned_spec.reshape(F, 2, pairs_dev * BLOCK)
    partial_corr = jnp.einsum("wpx,wpl->xl", owned_spec, lags, preferred_element_type=jnp.float32)
    synthetic = (
        lax.psum(partial_corr.astype(jnp.bfloat16), "rec")
        .astype(jnp.float32)
        .reshape(pairs_dev, BLOCK, LAGS)
    )
    weights = lag_mask[:, None, :].astype(jnp.float32) * jnp.tanh(synthetic - observed)
    weights_low = weights.astype(jnp.bfloat16).reshape(pairs_dev * BLOCK, LAGS)
    adjoint_spec = jnp.einsum("xl,wpl->wpx", weights_low, lags, preferred_element_type=jnp.float32)
    adjoint_spec = adjoint_spec.astype(jnp.bfloat16).reshape(F, 2, 1, pairs_dev * BLOCK)
    returned = lax.all_to_all(
        adjoint_spec, ("fibre", "seg"), split_axis=0, concat_axis=2, tiled=True
    )
    returned = returned.reshape(freq_dev, 2, pair_total, BLOCK).astype(jnp.float32)
    adjoint_re, adjoint_im = (returned[:, 0], returned[:, 1])
    grad_first = jnp.stack(
        [
            adjoint_re * second_re - adjoint_im * second_im,
            adjoint_re * second_im + adjoint_im * second_re,
        ],
        axis=1,
    )
    grad_second = jnp.stack(
        [
            adjoint_re * first_re + adjoint_im * first_im,
            adjoint_re * first_im - adjoint_im * first_re,
        ],
        axis=1,
    )
    contributions = jnp.concatenate([grad_first, grad_second], axis=2)
    endpoint_ids = jnp.concatenate([slot_ids[:, 0], slot_ids[:, 1]])
    summed = jax.ops.segment_sum(
        jnp.moveaxis(contributions, 2, 0), endpoint_ids, num_segments=block_count
    )
    block_adjoint = jnp.moveaxis(summed, 0, 2).astype(jnp.bfloat16)
    outgoing = block_adjoint.reshape(freq_dev, 2, spread_count, CH_DEV)
    sources = synthesize(
        lax.all_to_all(outgoing, ("fibre", "seg"), split_axis=2, concat_axis=0, tiled=True), table
    )
    regrouped = lax.all_to_all(sources, "fibre", split_axis=0, concat_axis=1, tiled=True)
    return regrouped[None]


def window_tables(bands):
    span, reach, n = S // bands, LAGS // 2, S // bands + LAGS
    half = n // 2
    freqs, places = np.arange(half), np.arange(n)
    shifts = np.arange(LAGS) - reach
    ends = np.where(freqs == 0, 1.0, 2.0) / (n * 2.0 * np.sqrt(F))

    def table(times, scale):
        angles = (freqs[None, :] * times[:, None] % n) * (2.0 * np.pi / n)
        real, imag = np.cos(angles), -np.sin(angles)
        imag[:, 0] = np.where(times % 2 == 0, 1.0, -1.0)
        return np.concatenate([real * scale, imag * scale], axis=1)

    whole = table(places, np.ones(half))
    left, core, right = whole[:reach], whole[reach : reach + span], whole[reach + span :]
    lags = table(shifts, ends).T
    taps = table(shifts, np.ones(half))
    back = table(places[reach : reach + span], ends)
    halo = np.stack([left, right])
    return [t.astype(np.float32).astype(jnp.bfloat16) for t in (core, halo, lags, taps, back)]


def dot(left, right, left_dim=1, right_dim=0):
    return lax.dot_general(
        left,
        right,
        (((left_dim,), (right_dim,)), ((), ())),
        preferred_element_type=jnp.float32,
    )


def spectral_product(terms, sign):
    both = sum(p1 * q1 for (_, p1), (_, q1) in terms)
    real = sum(p0 * q0 for (p0, _), (q0, _) in terms)
    imag = sum(p1 * q0 - sign * (p0 * q1) for (p0, p1), (q0, q1) in terms)
    ends = lax.broadcasted_iota(jnp.int32, both.shape, 1) == 0
    return real + jnp.where(ends, 0.0, sign * both), jnp.where(ends, both, imag)


def fused_kernel(
    sizes, x_hbm, pairs_hbm, observed_hbm, mask_hbm, core_hbm, halo_hbm, lags_hbm, taps_hbm, back_hbm,
    out, pairs, core, halo, rest, observed, mask, core_table, halo_table, lags, taps, back,
    inbox_sum, stage_total, inbox_total, columns, held_spec, core_spec, both_spec, left_spec,
    full_spec, select, cross, stage_core, inbox_core, stage3, inbox3, inbox4, grads, stage6,
    following, high, load_sem, send1, recv1, send_sum, recv_sum, total_sem, core_send, core_recv, relay_send, relay_recv,
    send3, recv3, send4, recv4, send6, recv6,
):
    fibres, segs, recs = sizes
    bands = fibres * segs
    last = fibres - 1
    g, f, s, r = (lax.axis_index(name) for name in ("groups", "fibre", "seg", "rec"))
    o = 1 - s
    band = f * segs + s
    span, reach, width = S // bands, LAGS // 2, x_hbm.shape[1]
    n = span + LAGS
    half = n // 2
    blocks = width // BLOCK
    count = pairs.shape[1] * BLOCK
    low, full = jnp.bfloat16, jnp.float32

    def at(fibre, seg, rec):
        return (g, fibre, seg, rec)

    def at_band(index):
        return at(index // segs, index % segs, r)

    def remote(src, dst, send, recv, device):
        return pltpu.make_async_remote_copy(
            src_ref=src, dst_ref=dst, send_sem=send, recv_sem=recv,
            device_id=device, device_id_type=pl.DeviceIdType.MESH,
        )

    def push(src, dst, send, recv, device):
        copy = remote(src, dst, send, recv, device)
        copy.start()
        return copy

    def arrived(dst, recv):
        remote(dst, dst, recv, recv, at(f, s, 1 - r)).wait_recv()

    def signal(sem, device):
        pl.semaphore_signal(sem, inc=1, device_id=device, device_id_type=pl.DeviceIdType.MESH)

    def rows(start, size, unit):
        return pl.ds(pl.multiple_of(start, unit), size)

    def flipped(index, bits):
        result, bit = 0, 1
        while bit < bands:
            digit = index // bit % 2
            result += bit * (1 - digit if bits // bit % 2 else digit)
            bit *= 2
        return result

    class bulk:
        def __init__(self, first, size, dst, send, recv, device):
            self.whole = remote(x_hbm.at[rows(first, size, PIECE)], dst, send, recv, device)
            self.pieces = [
                remote(x_hbm.at[rows(first + i, PIECE, PIECE)], dst.at[pl.ds(i, PIECE)], send, recv, device)
                for i in range(0, size, PIECE)
            ]

        def start(self):
            for piece in self.pieces:
                piece.start()

        def wait_send(self):
            self.whole.wait_send()

    partner = at(f, s, 1 - r)
    across = at(f, o, r)
    places = [(fi, si) for fi in range(fibres) for si in range(segs)]

    barrier = pltpu.get_barrier_semaphore()
    signal(barrier, partner)
    signal(barrier, across)
    for fi, si in places:

        @pl.when(fi > f)
        def _():
            signal(barrier, at(fi, si, r))

    locals_ = [
        pltpu.make_async_copy(x_hbm.at[rows(span * s, span, reach)], core.at[s], load_sem.at[0]),
        pltpu.make_async_copy(x_hbm.at[rows(reach + reach * o, reach, reach)], halo.at[o, s], load_sem.at[1]),
        pltpu.make_async_copy(x_hbm.at[rows((2 * span - reach) * o, reach, reach)], rest, load_sem.at[2]),
    ]
    loads = [
        pltpu.make_async_copy(src, dst, load_sem.at[3 + i])
        for i, (src, dst) in enumerate(
            [
                (pairs_hbm, pairs), (core_hbm, core_table), (halo_hbm, halo_table), (lags_hbm, lags), (observed_hbm.at[r], observed), (mask_hbm, mask), (taps_hbm, taps), (back_hbm, back),
            ]
        )
    ]
    for load in locals_ + loads:
        load.start()
    pl.semaphore_wait(barrier, segs * (f + 1))
    after = bulk(
        2 * span - reach, reach, halo.at[0, s], send1.at[0], recv1.at[2 + s], at((f + 1) % fibres, 0, r)
    )
    before = bulk(0, reach, halo.at[1, s], send1.at[1], recv1.at[4 + s], at((f + last) % fibres, 1, r))
    core_cut = span // 2
    core_sends = bulk(span * o, span, core.at[s], send1.at[2], recv1.at[0], across)
    row = bulk(reach + reach * s, reach, halo.at[s, s], send1.at[4], recv1.at[1], across)

    core_sends.start()

    @pl.when(s == 0)
    def _():
        row.start()

    for fi, si in places:

        @pl.when(fi == f - 1)
        def _():
            signal(following, at(fi, si, r))

        @pl.when(fi < f - 1)
        def _():
            signal(high, at(fi, si, r))

    for load in locals_:
        load.wait()
    folded = sum(
        part.astype(full).reshape(-1, 8, width).sum(axis=0) for part in (core[s], halo[o, s], rest[...])
    )
    odd = lax.broadcasted_iota(jnp.int32, folded.shape, 0) % 2 == 1
    inbox_sum[band] = jnp.concatenate(
        [
            jnp.sum(folded, axis=0, keepdims=True),
            jnp.sum(jnp.where(odd, -folded, folded), axis=0, keepdims=True),
        ],
        axis=0,
    )
    sends = [after, before, row, core_sends]
    own_sum = inbox_sum.at[band]
    sum_sends = [
        remote(own_sum, own_sum, send_sum.at[fi * segs + si], recv_sum.at[band], at(fi, si, r)) for fi, si in places
    ]
    across_sum = push(own_sum, own_sum, send_sum.at[bands], recv_sum.at[band], across)
    sends.append(across_sum)
    for (fi, si), copy in zip(places, sum_sends):

        @pl.when(fi < f)
        def _():
            copy.start()

    loads[0].wait()
    cut = bands // 2
    near = band // cut
    groups = [(r, near), (r, 1 - near), (1 - r, near), (1 - r, 1 - near)]
    group = 2 * cut * BLOCK
    lane = lax.broadcasted_iota(jnp.int32, (1, 2 * count), 1)
    target = lane
    for p, (h, side) in enumerate(groups):
        for end in range(2):
            for i in range(cut):
                first = p * group + (end * cut + i) * BLOCK
                inside = (lane >= first) & (lane < first + BLOCK)
                target = jnp.where(inside, lane + (pairs[end, (side * cut + i) * recs + h] * BLOCK - first), target)
    line = lax.broadcasted_iota(jnp.int32, select.shape, 0)
    select[...] = jnp.where(line == target, 1.0, 0.0).astype(low)

    def put(spec, seg, value):
        spec[rows(seg * blocks, blocks, blocks)] = value.astype(low).reshape(blocks, BLOCK, n)

    def core_part(seg):
        part = dot(core[seg], core_table[...], 0, 0)
        held_spec[seg] = part
        put(core_spec, seg, part)

    loads[1].wait()
    core_part(s)

    @pl.when(f < last)
    def _():
        pl.semaphore_wait(following, segs)

    after.start()
    arrived(core.at[o], recv1.at[0])
    core_part(o)

    @pl.when(f < last - 1)
    def _():
        pl.semaphore_wait(high, segs * (last - 1 - f))

    for (fi, si), copy in zip(places, sum_sends):

        @pl.when(fi > f)
        def _():
            copy.start()

    @pl.when(f == 0)
    def _():
        before.start()

    loads[2].wait()

    def left_part(seg):
        part = dot(halo[0, seg], halo_table[0], 0, 0)
        put(left_spec, seg, part)
        part += held_spec[seg]
        held_spec[seg] = part
        put(both_spec, seg, part)

    @pl.when(s == 0)
    def _():
        arrived(halo.at[0, 0], recv1.at[2])

    left_part(s)

    @pl.when(s == 0)
    def _():
        arrived(halo.at[0, 1], recv1.at[3])

    @pl.when(s == 1)
    def _():
        arrived(halo.at[0, 0], recv1.at[1])
        row.start()

    @pl.when(f > 0)
    def _():
        before.start()

    left_part(o)

    def block(spec, index):
        value = spec[index].astype(full)
        return value[:, :half], value[:, half:]

    def correlate(place, h, side):
        for i in range(cut):
            pair = (side * cut + i) * recs + h
            one, two = pairs[0, pair], pairs[1, pair]
            terms = [(block(core_spec, one), block(both_spec, two)), (block(left_spec, one), block(core_spec, two))]
            real, imag = spectral_product(terms, 1.0)
            here = pl.ds(i * BLOCK, BLOCK)
            cross[place, here, pl.ds(0, half)] = real.astype(low)
            cross[place, here, pl.ds(half, half)] = imag.astype(low)
        return dot(cross[place], lags[...])

    loads[3].wait()
    sides = (1, 0)
    for i, side in enumerate(sides):
        stage_core[i] = correlate(i, 1 - r, side).astype(low)
        sends.append(push(stage_core.at[i], inbox_core.at[i], core_send.at[i], core_recv.at[i], partner))

    spread3 = [
        remote(stage3.at[j], inbox3.at[band], send3.at[j], recv3.at[band], at(j // segs, j % segs, r))
        for j in range(bands)
    ]
    for i, side in enumerate(sides):
        partial = correlate(2 + i, r, side)
        arrived(inbox_core.at[i], core_recv.at[i])
        partial = (partial + inbox_core[i].astype(full)).astype(low)
        stage3[rows(side * cut, cut, cut)] = partial.reshape(cut, BLOCK, LAGS)
        for j in range((side + 1) * cut - 1, side * cut - 1, -1):

            @pl.when(band != j)
            def _():
                spread3[j].start()

    inbox3[band] = stage3[band]

    for d in range(1, bands):
        k = flipped(band, d)
        arrived(inbox_sum.at[k], recv_sum.at[k])
    for seg in range(segs):
        stage_total[seg] = sum(inbox_sum[fi * segs + seg] for fi in range(fibres))
    sends.append(push(stage_total, inbox_total, total_sem.at[0], total_sem.at[1], partner))
    arrived(inbox_total, total_sem.at[1])
    for seg in range(segs):
        total = jnp.concatenate([stage_total[seg], inbox_total[seg]] * 2, axis=0)
        columns[pl.ds(seg * blocks, blocks)] = total.T.reshape(blocks, BLOCK, 8)
    loads[4].wait()
    loads[5].wait()
    ends = columns[pairs[0, band * recs + r]] * columns[pairs[1, band * recs + r]]
    flat = ends[:, 0:1] + ends[:, 2:3]
    alternating = ends[:, 1:2] + ends[:, 3:4]
    even = lax.broadcasted_iota(jnp.int32, (BLOCK, LAGS), 1) % 2 == reach % 2
    offset = (flat + jnp.where(even, -alternating, alternating)) * (1.0 / (2.0 * S * F**0.5))
    for d in range(1, bands):
        k = flipped(band, d)
        arrived(inbox3.at[k], recv3.at[k])
    synthetic = offset + inbox3[0].astype(full)
    for k in range(1, bands):
        synthetic += inbox3[k].astype(full)
    window = mask[pl.ds(r, 1), :].astype(full)
    inbox4[r, band] = (window * jnp.tanh(synthetic - observed[...])).astype(low)
    own = inbox4.at[r, band]
    spread4 = [
        remote(own, own, send4.at[j], recv4.at[band], at(j // segs, j % segs, r)) for j in range(bands)
    ]
    for j in range(bands):

        @pl.when(band != j)
        def _():
            spread4[j].start()

    sends.append(push(own, own, relay_send.at[0], relay_recv.at[band], partner))

    @pl.when(s == 0)
    def _():
        arrived(halo.at[1, 1], recv1.at[1])

    @pl.when(s == 1)
    def _():
        for seg in range(segs):
            arrived(halo.at[1, seg], recv1.at[4 + seg])

    head = lax.broadcasted_iota(jnp.int32, (1, half), 1) == 0
    for seg in range(segs):
        total = jnp.concatenate([stage_total[seg]] * 4, axis=0).T * (n / S)
        value = held_spec[seg] + dot(halo[1, seg], halo_table[1], 0, 0)
        value = jnp.concatenate(
            [
                value[:, :half] + jnp.where(head, total[:, 0:1], 0.0),
                value[:, half:] - jnp.where(head, total[:, 1:2], 0.0),
            ],
            axis=1,
        )
        put(full_spec, seg, value)
    loads[6].wait()

    def gradients(p):
        h, side = groups[p]
        spread = dot(inbox4[h, pl.ds(side * cut, cut)].reshape(cut * BLOCK, LAGS), taps[...])
        for i in range(cut):
            pair = (side * cut + i) * recs + h
            filters = spread[i * BLOCK : (i + 1) * BLOCK]
            filters = filters[:, :half], filters[:, half:]
            first = block(full_spec, pairs[0, pair])
            second = block(full_spec, pairs[1, pair])
            base = p * group + i * BLOCK
            for start, parts in (
                (base, spectral_product([(filters, second)], -1.0)),
                (base + cut * BLOCK, spectral_product([(first, filters)], 1.0)),
            ):
                for q in range(2):
                    grads[pl.ds(start, BLOCK), pl.ds(q * half, half)] = parts[q].astype(low)

    for d in range(1, bands):
        k = flipped(band, d)
        arrived(inbox4.at[r, k], recv4.at[k])
        got = inbox4.at[r, k]
        sends.append(push(got, got, relay_send.at[d], relay_recv.at[k], partner))
    for p, (first, stop) in enumerate(((0, 0), (0, 0), (0, cut), (cut, bands))):
        for d in range(first, stop):
            k = flipped(band, d)
            arrived(inbox4.at[1 - r, k], relay_recv.at[k])
        gradients(p)
    loads[7].wait()

    def summed(seg):
        return dot(select[rows(seg * width, width, width), :], grads[...]).astype(low)

    stage6[...] = dot(back[...], summed(o), 1, 1).astype(low)
    here = rows(span * s, span, span)
    sends.append(push(stage6, out.at[here, :], send6.at[0], recv6.at[0], across))
    out[here, :] = dot(back[...], summed(s), 1, 1).astype(low)
    arrived(out.at[rows(span * o, span, span), :], recv6.at[0])
    for copy in sends:
        copy.wait_send()
    for j in range(bands):

        @pl.when(band != j)
        def _():
            spread3[j].wait_send()
            spread4[j].wait_send()

    for (fi, si), copy in zip(places, sum_sends):

        @pl.when(fi != f)
        def _():
            copy.wait_send()


def fused_on_device(mesh_shape, tables, records, pairs, observed, lag_mask):
    fibres, segs, recs = (mesh_shape[name] for name in ("fibre", "seg", "rec"))
    bands = fibres * segs
    _, extent, width = records.shape
    span, reach = S // bands, LAGS // 2
    n = span + LAGS
    count = pairs.shape[0] * BLOCK
    own = count // recs
    total = segs * width
    low, full = jnp.bfloat16, jnp.float32
    vmem = pl.BlockSpec(memory_space=pltpu.VMEM)
    hbm = pl.BlockSpec(memory_space=pltpu.HBM)
    corr = (BLOCK, LAGS)
    spec = pltpu.VMEM((total // BLOCK, BLOCK, n), low)

    def sems(*sizes):
        return [pltpu.SemaphoreType.DMA((size,)) for size in sizes]

    result = pl.pallas_call(
        functools.partial(fused_kernel, (fibres, segs, recs)),
        out_shape=pltpu.VMEM((extent, width), low),
        in_specs=[hbm] * 9,
        out_specs=vmem,
        scratch_shapes=[
            pltpu.SMEM((2, pairs.shape[0]), jnp.int32),
            pltpu.VMEM((segs, span, width), low),
            pltpu.VMEM((2, segs, reach, width), low),
            pltpu.VMEM((reach, width), low),
            pltpu.VMEM(corr, full),
            pltpu.VMEM(lag_mask.shape, jnp.int32),
            pltpu.VMEM((span, n), low),
            pltpu.VMEM((2, reach, n), low),
            pltpu.VMEM((n, LAGS), low),
            pltpu.VMEM((LAGS, n), low),
            pltpu.VMEM((span, n), low),
            pltpu.VMEM((bands, 2, width), full),
            pltpu.VMEM((segs, 2, width), full),
            pltpu.VMEM((segs, 2, width), full),
            pltpu.VMEM((total // BLOCK, BLOCK, 8), full),
            pltpu.VMEM((segs, width, n), full),
            spec, spec, spec, spec,
            pltpu.VMEM((total, 2 * count), low),
            pltpu.VMEM((2 * recs, own // 2, n), low),
            pltpu.VMEM((2, own // 2, LAGS), low),
            pltpu.VMEM((2, own // 2, LAGS), low),
            pltpu.VMEM((bands,) + corr, low),
            pltpu.VMEM((bands,) + corr, low),
            pltpu.VMEM((recs, bands) + corr, low),
            pltpu.VMEM((2 * count, n), low),
            pltpu.VMEM((span, width), low),
            pltpu.SemaphoreType.REGULAR,
            pltpu.SemaphoreType.REGULAR,
            *sems(11, 5, 8, bands + 1, bands, 2, 2, 2, bands, bands),
            *sems(bands, bands, bands, bands, 2, 2),
        ],
        compiler_params=pltpu.CompilerParams(
            has_side_effects=True, collective_id=0, vmem_limit_bytes=VMEM_GRANT
        ),
        name="adjoint",
    )(records[0], pairs.T, observed, lag_mask, *tables)
    return result[None]


def fits_fused(shape, records, pairs):
    fibres, segs, recs = (shape[name] for name in ("fibre", "seg", "rec"))
    bands = fibres * segs
    width = records.shape[2] // (shape["groups"] * segs)
    return (
        fibres > 1
        and fibres & (fibres - 1) == 0
        and segs == 2
        and recs == 2
        and width % 128 == 0
        and width * segs <= 512
        and S // bands >= LAGS
        and pairs.shape[0] == bands * recs
    )


def solution(mesh):
    in_specs = (
        P("rec", "fibre", ("groups", "seg")),
        P(),
        P(("groups", "fibre", "seg"), None, None),
        P(("groups", "fibre", "seg"), None),
    )
    out_specs = P("rec", "fibre", ("groups", "seg"))
    shape = dict(mesh.shape)

    def run(records, pairs, observed, lag_mask):
        args = (records, pairs, observed, lag_mask)
        if not fits_fused(shape, records, pairs):
            return jax.shard_map(
                on_device, mesh=mesh, in_specs=in_specs, out_specs=out_specs, check_vma=False
            )(*args)
        tables = [jnp.asarray(t) for t in window_tables(shape["fibre"] * shape["seg"])]

        def body(*blocks):
            return fused_on_device(shape, tables, *blocks)

        return jax.shard_map(
            body, mesh=mesh, in_specs=in_specs, out_specs=out_specs, check_vma=False
        )(*args)

    return run
```

```python
import functools

import jax
import jax.numpy as jnp
import numpy as np
from jax import lax
from jax.experimental import pallas as pl
from jax.experimental.pallas import tpu as pltpu
from jax.sharding import PartitionSpec as P

S = 2048
F = 1024
LAGS = 256
BLOCK = 32
CH_DEV = 64
VMEM_GRANT = 60899328


def forward_table():
    freq_index = jnp.arange(F, dtype=jnp.int32)
    time_index = jnp.arange(S, dtype=jnp.int32)
    phase = freq_index[:, None] * time_index[None, :] % S
    angles = phase.astype(jnp.float32) * (2.0 * jnp.pi / S)
    scale = 1.0 / jnp.sqrt(jnp.float32(S))
    return jnp.stack(
        [
            (jnp.cos(angles) * scale).astype(jnp.bfloat16),
            (-jnp.sin(angles) * scale).astype(jnp.bfloat16),
        ],
        axis=1,
    )


def lag_table():
    freq_index = jnp.arange(F, dtype=jnp.int32)
    shifts = (jnp.arange(LAGS, dtype=jnp.int32) - LAGS // 2) % S
    phase = freq_index[:, None] * shifts[None, :] % S
    angles = phase.astype(jnp.float32) * (2.0 * jnp.pi / S)
    scale = 1.0 / jnp.sqrt(jnp.float32(F))
    return jnp.stack(
        [
            (jnp.cos(angles) * scale).astype(jnp.bfloat16),
            (-jnp.sin(angles) * scale).astype(jnp.bfloat16),
        ],
        axis=1,
    )


def synthesize(incoming, table):
    count = incoming.shape[-1]
    flat = incoming.reshape(2 * F, count)
    result = jnp.einsum(
        "qn,qt->tn", flat, table.reshape(2 * F, S), preferred_element_type=jnp.float32
    )
    return result.astype(jnp.bfloat16)


def on_device(records, pairs, observed, lag_mask):
    fibre_count = lax.axis_size("fibre")
    seg_count = lax.axis_size("seg")
    spread_count = fibre_count * seg_count
    freq_dev = F // spread_count
    blocks_dev = CH_DEV // BLOCK
    block_count = CH_DEV * spread_count // BLOCK
    pair_total = pairs.shape[0]
    pairs_dev = pair_total // spread_count
    table = forward_table()
    lags = lag_table()
    spans = records.reshape(1, S // fibre_count, fibre_count, CH_DEV)
    incoming = lax.all_to_all(spans, "fibre", split_axis=2, concat_axis=1, tiled=True)
    count = incoming.shape[3]
    signal = incoming.reshape(S, count)
    result = jnp.einsum(
        "qs,sn->qn", table.reshape(2 * F, S), signal, preferred_element_type=jnp.float32
    )
    spectra = result.reshape(F, 2, count).astype(jnp.bfloat16)
    widened = lax.all_to_all(spectra, ("fibre", "seg"), split_axis=0, concat_axis=2, tiled=True)
    seg_blocks = fibre_count * blocks_dev
    slot_ids = (
        pairs % seg_blocks // blocks_dev * seg_count + pairs // seg_blocks
    ) * blocks_dev + pairs % blocks_dev
    blocks_grid = widened.reshape(freq_dev, 2, block_count, BLOCK)
    first_side = jnp.take(blocks_grid, slot_ids[:, 0], axis=2).astype(jnp.float32)
    second_side = jnp.take(blocks_grid, slot_ids[:, 1], axis=2).astype(jnp.float32)
    first_re, first_im = (first_side[:, 0], first_side[:, 1])
    second_re, second_im = (second_side[:, 0], second_side[:, 1])
    cross_re = first_re * second_re + first_im * second_im
    cross_im = first_im * second_re - first_re * second_im
    cross_spec = jnp.stack([cross_re, cross_im], axis=1).astype(jnp.bfloat16)
    cross_spec = cross_spec.reshape(freq_dev, 2, spread_count, pairs_dev * BLOCK)
    owned_spec = lax.all_to_all(
        cross_spec, ("fibre", "seg"), split_axis=2, concat_axis=0, tiled=True
    )
    owned_spec = owned_spec.reshape(F, 2, pairs_dev * BLOCK)
    partial_corr = jnp.einsum("wpx,wpl->xl", owned_spec, lags, preferred_element_type=jnp.float32)
    synthetic = (
        lax.psum(partial_corr.astype(jnp.bfloat16), "rec")
        .astype(jnp.float32)
        .reshape(pairs_dev, BLOCK, LAGS)
    )
    weights = lag_mask[:, None, :].astype(jnp.float32) * jnp.tanh(synthetic - observed)
    weights_low = weights.astype(jnp.bfloat16).reshape(pairs_dev * BLOCK, LAGS)
    adjoint_spec = jnp.einsum("xl,wpl->wpx", weights_low, lags, preferred_element_type=jnp.float32)
    adjoint_spec = adjoint_spec.astype(jnp.bfloat16).reshape(F, 2, 1, pairs_dev * BLOCK)
    returned = lax.all_to_all(
        adjoint_spec, ("fibre", "seg"), split_axis=0, concat_axis=2, tiled=True
    )
    returned = returned.reshape(freq_dev, 2, pair_total, BLOCK).astype(jnp.float32)
    adjoint_re, adjoint_im = (returned[:, 0], returned[:, 1])
    grad_first = jnp.stack(
        [
            adjoint_re * second_re - adjoint_im * second_im,
            adjoint_re * second_im + adjoint_im * second_re,
        ],
        axis=1,
    )
    grad_second = jnp.stack(
        [
            adjoint_re * first_re + adjoint_im * first_im,
            adjoint_re * first_im - adjoint_im * first_re,
        ],
        axis=1,
    )
    contributions = jnp.concatenate([grad_first, grad_second], axis=2)
    endpoint_ids = jnp.concatenate([slot_ids[:, 0], slot_ids[:, 1]])
    summed = jax.ops.segment_sum(
        jnp.moveaxis(contributions, 2, 0), endpoint_ids, num_segments=block_count
    )
    block_adjoint = jnp.moveaxis(summed, 0, 2).astype(jnp.bfloat16)
    outgoing = block_adjoint.reshape(freq_dev, 2, spread_count, CH_DEV)
    sources = synthesize(
        lax.all_to_all(outgoing, ("fibre", "seg"), split_axis=2, concat_axis=0, tiled=True), table
    )
    regrouped = lax.all_to_all(sources, "fibre", split_axis=0, concat_axis=1, tiled=True)
    return regrouped[None]


def window_tables(bands):
    span, reach, n = S // bands, LAGS // 2, S // bands + LAGS
    half = n // 2
    freqs, places = np.arange(half), np.arange(n)
    shifts = np.arange(LAGS) - reach
    ends = np.where(freqs == 0, 1.0, 2.0) / (n * 2.0 * np.sqrt(F))

    def table(times, scale):
        angles = (freqs[None, :] * times[:, None] % n) * (2.0 * np.pi / n)
        real, imag = np.cos(angles), -np.sin(angles)
        imag[:, 0] = np.where(times % 2 == 0, 1.0, -1.0)
        return np.concatenate([real * scale, imag * scale], axis=1)

    whole = table(places, np.ones(half))
    lags = table(shifts, ends).T
    taps = table(shifts, np.ones(half))
    back = table(places[reach : reach + span], ends)
    return [t.astype(np.float32).astype(jnp.bfloat16) for t in (whole, lags, taps, back)]


def dot(left, right, left_dim=1, right_dim=0):
    return lax.dot_general(
        left,
        right,
        (((left_dim,), (right_dim,)), ((), ())),
        preferred_element_type=jnp.float32,
    )


def spectral_product(terms, sign):
    both = sum(p1 * q1 for (_, p1), (_, q1) in terms)
    real = sum(p0 * q0 for (p0, _), (q0, _) in terms)
    imag = sum(p1 * q0 - sign * (p0 * q1) for (p0, p1), (q0, q1) in terms)
    ends = lax.broadcasted_iota(jnp.int32, both.shape, 1) == 0
    return real + jnp.where(ends, 0.0, sign * both), jnp.where(ends, both, imag)


def fused_kernel(
    sizes, x_hbm, pairs_hbm, observed_hbm, mask_hbm, whole_hbm, lags_hbm, taps_hbm, back_hbm,
    out, pairs, ext, observed, mask, whole, lags, taps, back,
    inbox_sum, stage_total, inbox_total, columns, held_spec, core_spec, both_spec, left_spec,
    full_spec, select, cross, stage_core, inbox_core, stage3, inbox3, inbox4, grads,
    following, high, load_sem, send1, recv1, send_sum, recv_sum, total_sem, core_send, core_recv,
    relay_send, relay_recv, send3, recv3, send4, recv4,
):
    fibres, segs, recs = sizes
    bands = fibres * segs
    last = fibres - 1
    g, f, s, r = (lax.axis_index(name) for name in ("groups", "fibre", "seg", "rec"))
    o = 1 - s
    band = f * segs + s
    span, reach, width = S // bands, LAGS // 2, x_hbm.shape[1]
    n = span + LAGS
    half = n // 2
    blocks = width // BLOCK
    count = pairs.shape[1] * BLOCK
    low, full = jnp.bfloat16, jnp.float32

    def at(fibre, seg, rec):
        return (g, fibre, seg, rec)

    def at_band(index):
        return at(index // segs, index % segs, r)

    def remote(src, dst, send, recv, device):
        return pltpu.make_async_remote_copy(
            src_ref=src, dst_ref=dst, send_sem=send, recv_sem=recv,
            device_id=device, device_id_type=pl.DeviceIdType.MESH,
        )

    def push(src, dst, send, recv, device):
        copy = remote(src, dst, send, recv, device)
        copy.start()
        return copy

    def arrived(dst, recv):
        remote(dst, dst, recv, recv, at(f, s, 1 - r)).wait_recv()

    def signal(sem, device):
        pl.semaphore_signal(sem, inc=1, device_id=device, device_id_type=pl.DeviceIdType.MESH)

    def rows(start, size, unit):
        return pl.ds(pl.multiple_of(start, unit), size)

    def flipped(index, bits):
        result, bit = 0, 1
        while bit < bands:
            digit = index // bit % 2
            result += bit * (1 - digit if bits // bit % 2 else digit)
            bit *= 2
        return result

    partner = at(f, s, 1 - r)
    across = at(f, o, r)
    places = [(fi, si) for fi in range(fibres) for si in range(segs)]

    barrier = pltpu.get_barrier_semaphore()
    signal(barrier, partner)
    signal(barrier, across)
    for fi, si in places:

        @pl.when(fi > f)
        def _():
            signal(barrier, at(fi, si, r))

    loads = [
        pltpu.make_async_copy(src, dst, load_sem.at[i])
        for i, (src, dst) in enumerate(
            [
                (x_hbm, ext.at[s, pl.ds(reach, 2 * span)]), (pairs_hbm, pairs), (whole_hbm, whole), (lags_hbm, lags),
                (observed_hbm.at[r], observed), (mask_hbm, mask), (taps_hbm, taps), (back_hbm, back),
            ]
        )
    ]
    for load in loads:
        load.start()

    def give(first, size, place, send, recv, device):
        return remote(
            x_hbm.at[pl.ds(first, size)], ext.at[s, pl.ds(place, size)], send1.at[send], recv1.at[recv], device
        )

    needed = [
        [give(span, span, span + reach, 0, 0, across), give(reach, reach, 2 * reach, 1, 1, across)],
        [give(0, span, reach, 0, 0, across)],
    ]
    later = [give(0, reach, reach, 2, 2, across), give(span, span, reach + span, 2, 2, across)]
    upper, lower = (f + 1) % fibres, (f + last) % fibres
    up = give(2 * span - reach, reach, 0, 3, 3, at(upper, s, r))
    up_across = give(2 * span - reach, reach, 0, 4, 4, at(upper, 0, r))
    down = give(0, reach, reach + 2 * span, 5, 5, at(lower, s, r))
    edges = [pl.ds(0, reach), pl.ds(reach + 2 * span, reach)]
    passed = [
        remote(ext.at[s, edge], ext.at[s, edge], send1.at[6 + i], recv1.at[6 + i], across)
        for i, edge in enumerate(edges)
    ]

    def send_up():
        up.start()

        @pl.when(s == 1)
        def _():
            up_across.start()

    pl.semaphore_wait(barrier, segs * (f + 1))
    for si in range(segs):

        @pl.when(s == si)
        def _():
            for copy in needed[si]:
                copy.start()

    @pl.when(f > 0)
    def _():
        down.start()

    @pl.when(f == last)
    def _():
        send_up()

    for fi, si in places:

        @pl.when(fi == f - 1)
        def _():
            signal(following, at(fi, si, r))

        @pl.when(fi < f - 1)
        def _():
            signal(high, at(fi, si, r))

    loads[0].wait()
    folded = ext[s, pl.ds(reach, 2 * span)].astype(full).reshape(-1, 8, width).sum(axis=0)
    odd = lax.broadcasted_iota(jnp.int32, folded.shape, 0) % 2 == 1
    inbox_sum[band] = jnp.concatenate(
        [
            jnp.sum(folded, axis=0, keepdims=True),
            jnp.sum(jnp.where(odd, -folded, folded), axis=0, keepdims=True),
        ],
        axis=0,
    )
    sends = [up, down]
    own_sum = inbox_sum.at[band]
    sum_sends = [
        remote(own_sum, own_sum, send_sum.at[fi * segs + si], recv_sum.at[band], at(fi, si, r)) for fi, si in places
    ]
    across_sum = push(own_sum, own_sum, send_sum.at[bands], recv_sum.at[band], across)
    sends.append(across_sum)
    for (fi, si), copy in zip(places, sum_sends):

        @pl.when(fi < f)
        def _():
            copy.start()

    loads[1].wait()
    cut = bands // 2
    near = band // cut
    groups = [(r, near), (r, 1 - near), (1 - r, near), (1 - r, 1 - near)]
    group = 2 * cut * BLOCK
    lane = lax.broadcasted_iota(jnp.int32, (1, 2 * count), 1)
    target = lane
    for p, (h, side) in enumerate(groups):
        for end in range(2):
            for i in range(cut):
                first = p * group + (end * cut + i) * BLOCK
                inside = (lane >= first) & (lane < first + BLOCK)
                target = jnp.where(inside, lane + (pairs[end, (side * cut + i) * recs + h] * BLOCK - first), target)
    line = lax.broadcasted_iota(jnp.int32, select.shape, 0) + s * width
    select[...] = jnp.where(line == target, 1.0, 0.0).astype(low)

    def put(spec, seg, value):
        spec[rows(seg * blocks, blocks, blocks)] = value.astype(low).reshape(blocks, BLOCK, n)

    def core_part(seg):
        part = dot(ext[seg, rows(reach + span * s, span, reach)], whole[reach : reach + span], 0, 0)
        held_spec[seg] = part
        put(core_spec, seg, part)

    def left_part(seg):
        part = dot(ext[seg, rows(span * s, reach, reach)], whole[:reach], 0, 0)
        put(left_spec, seg, part)
        put(both_spec, seg, part + held_spec[seg])

    loads[2].wait()
    core_part(s)

    @pl.when(f < last)
    def _():
        pl.semaphore_wait(following, segs)
        send_up()

    for si in range(segs):

        @pl.when(s == 1 - si)
        def _():
            arrived(ext.at[si, pl.ds(reach + span * (1 - si), span)], recv1.at[0])

    core_part(o)

    @pl.when(f < last - 1)
    def _():
        pl.semaphore_wait(high, segs * (last - 1 - f))

    for (fi, si), copy in zip(places, sum_sends):

        @pl.when(fi > f)
        def _():
            copy.start()

    @pl.when(f == 0)
    def _():
        down.start()

    @pl.when(s == 0)
    def _():
        arrived(ext.at[0, edges[0]], recv1.at[3])

    left_part(s)

    @pl.when(s == 0)
    def _():
        arrived(ext.at[1, edges[0]], recv1.at[4])

    @pl.when(s == 1)
    def _():
        arrived(ext.at[0, pl.ds(2 * reach, reach)], recv1.at[1])

    left_part(o)

    def block(spec, index):
        value = spec[index].astype(full)
        return value[:, :half], value[:, half:]

    def correlate(place, h, side):
        for i in range(cut):
            pair = (side * cut + i) * recs + h
            one, two = pairs[0, pair], pairs[1, pair]
            terms = [(block(core_spec, one), block(both_spec, two)), (block(left_spec, one), block(core_spec, two))]
            real, imag = spectral_product(terms, 1.0)
            here = pl.ds(i * BLOCK, BLOCK)
            cross[place, here, pl.ds(0, half)] = real.astype(low)
            cross[place, here, pl.ds(half, half)] = imag.astype(low)
        return dot(cross[place], lags[...])

    loads[3].wait()
    sides = (1, 0)
    for i, side in enumerate(sides):
        stage_core[i] = correlate(i, 1 - r, side).astype(low)
        sends.append(push(stage_core.at[i], inbox_core.at[i], core_send.at[i], core_recv.at[i], partner))

    spread3 = [
        remote(stage3.at[j], inbox3.at[band], send3.at[j], recv3.at[band], at(j // segs, j % segs, r))
        for j in range(bands)
    ]
    for i, side in enumerate(sides):
        partial = correlate(2 + i, r, side)
        arrived(inbox_core.at[i], core_recv.at[i])
        partial = (partial + inbox_core[i].astype(full)).astype(low)
        stage3[rows(side * cut, cut, cut)] = partial.reshape(cut, BLOCK, LAGS)
        for j in range((side + 1) * cut - 1, side * cut - 1, -1):

            @pl.when(band != j)
            def _():
                spread3[j].start()

    inbox3[band] = stage3[band]

    @pl.when(s == 0)
    def _():
        later[0].start()
        passed[0].start()

    @pl.when(s == 1)
    def _():
        later[1].start()
        arrived(ext.at[1, edges[0]], recv1.at[3])

    arrived(ext.at[s, edges[1]], recv1.at[5])
    passed[1].start()

    for d in range(1, bands):
        k = flipped(band, d)
        arrived(inbox_sum.at[k], recv_sum.at[k])
    for seg in range(segs):
        stage_total[seg] = sum(inbox_sum[fi * segs + seg] for fi in range(fibres))
    sends.append(push(stage_total, inbox_total, total_sem.at[0], total_sem.at[1], partner))
    arrived(inbox_total, total_sem.at[1])
    for seg in range(segs):
        total = jnp.concatenate([stage_total[seg], inbox_total[seg]] * 2, axis=0)
        columns[pl.ds(seg * blocks, blocks)] = total.T.reshape(blocks, BLOCK, 8)
    loads[4].wait()
    loads[5].wait()
    ends = columns[pairs[0, band * recs + r]] * columns[pairs[1, band * recs + r]]
    flat = ends[:, 0:1] + ends[:, 2:3]
    alternating = ends[:, 1:2] + ends[:, 3:4]
    even = lax.broadcasted_iota(jnp.int32, (BLOCK, LAGS), 1) % 2 == reach % 2
    offset = (flat + jnp.where(even, -alternating, alternating)) * (1.0 / (2.0 * S * F**0.5))
    for d in range(1, bands):
        k = flipped(band, d)
        arrived(inbox3.at[k], recv3.at[k])
    synthetic = offset + inbox3[0].astype(full)
    for k in range(1, bands):
        synthetic += inbox3[k].astype(full)
    window = mask[pl.ds(r, 1), :].astype(full)
    inbox4[r, band] = (window * jnp.tanh(synthetic - observed[...])).astype(low)
    own = inbox4.at[r, band]
    spread4 = [
        remote(own, own, send4.at[j], recv4.at[band], at(j // segs, j % segs, r)) for j in range(bands)
    ]
    for j in range(bands):

        @pl.when(band != j)
        def _():
            spread4[j].start()

    sends.append(push(own, own, relay_send.at[0], relay_recv.at[band], partner))

    for si in range(segs):

        @pl.when(s == 1 - si)
        def _():
            arrived(ext.at[si, pl.ds(reach + span * si, reach + (span - reach) * si)], recv1.at[2])

    @pl.when(s == 1)
    def _():
        arrived(ext.at[0, edges[0]], recv1.at[6])

    arrived(ext.at[o, edges[1]], recv1.at[7])
    head = lax.broadcasted_iota(jnp.int32, (1, half), 1) == 0
    for seg in range(segs):
        total = jnp.concatenate([stage_total[seg]] * 4, axis=0).T * (n / S)
        for w in range(segs):
            value = dot(ext[seg, pl.ds(span * w, n)], whole[...], 0, 0)
            value = jnp.concatenate(
                [
                    value[:, :half] + jnp.where(head, total[:, 0:1], 0.0),
                    value[:, half:] - jnp.where(head, total[:, 1:2], 0.0),
                ],
                axis=1,
            )
            put(full_spec.at[w], seg, value)
    loads[6].wait()

    def gradients(p):
        h, side = groups[p]
        spread = dot(inbox4[h, pl.ds(side * cut, cut)].reshape(cut * BLOCK, LAGS), taps[...])
        for i in range(cut):
            pair = (side * cut + i) * recs + h
            filters = spread[i * BLOCK : (i + 1) * BLOCK]
            filters = filters[:, :half], filters[:, half:]
            base = p * group + i * BLOCK
            for w in range(segs):
                first = block(full_spec.at[w], pairs[0, pair])
                second = block(full_spec.at[w], pairs[1, pair])
                for start, parts in (
                    (base, spectral_product([(filters, second)], -1.0)),
                    (base + cut * BLOCK, spectral_product([(first, filters)], 1.0)),
                ):
                    for q in range(2):
                        grads[w, pl.ds(start, BLOCK), pl.ds(q * half, half)] = parts[q].astype(low)

    for d in range(1, bands):
        k = flipped(band, d)
        arrived(inbox4.at[r, k], recv4.at[k])
        got = inbox4.at[r, k]
        sends.append(push(got, got, relay_send.at[d], relay_recv.at[k], partner))
    for p, (first, stop) in enumerate(((0, 0), (0, 0), (0, cut), (cut, bands))):
        for d in range(first, stop):
            k = flipped(band, d)
            arrived(inbox4.at[1 - r, k], relay_recv.at[k])
        gradients(p)
    loads[7].wait()

    for w in range(segs):
        summed = dot(select[...], grads[w]).astype(low)
        out[pl.ds(span * w, span), :] = dot(back[...], summed, 1, 1).astype(low)
    for si in range(segs):

        @pl.when(s == si)
        def _():
            for copy in needed[si] + [later[si]] + passed[si:]:
                copy.wait_send()

    @pl.when(s == 1)
    def _():
        up_across.wait_send()

    for copy in sends:
        copy.wait_send()
    for j in range(bands):

        @pl.when(band != j)
        def _():
            spread3[j].wait_send()
            spread4[j].wait_send()

    for (fi, si), copy in zip(places, sum_sends):

        @pl.when(fi != f)
        def _():
            copy.wait_send()


def fused_on_device(mesh_shape, tables, records, pairs, observed, lag_mask):
    fibres, segs, recs = (mesh_shape[name] for name in ("fibre", "seg", "rec"))
    bands = fibres * segs
    _, extent, width = records.shape
    span, reach = S // bands, LAGS // 2
    n = span + LAGS
    count = pairs.shape[0] * BLOCK
    own = count // recs
    total = segs * width
    low, full = jnp.bfloat16, jnp.float32
    vmem = pl.BlockSpec(memory_space=pltpu.VMEM)
    hbm = pl.BlockSpec(memory_space=pltpu.HBM)
    corr = (BLOCK, LAGS)
    spec = (total // BLOCK, BLOCK, n)

    def sems(*sizes):
        return [pltpu.SemaphoreType.DMA((size,)) for size in sizes]

    result = pl.pallas_call(
        functools.partial(fused_kernel, (fibres, segs, recs)),
        out_shape=pltpu.VMEM((extent, width), low),
        in_specs=[hbm] * 8,
        out_specs=vmem,
        scratch_shapes=[
            pltpu.SMEM((2, pairs.shape[0]), jnp.int32),
            pltpu.VMEM((segs, 2 * span + 2 * reach, width), low),
            pltpu.VMEM(corr, full),
            pltpu.VMEM(lag_mask.shape, jnp.int32),
            pltpu.VMEM((n, n), low),
            pltpu.VMEM((n, LAGS), low),
            pltpu.VMEM((LAGS, n), low),
            pltpu.VMEM((span, n), low),
            pltpu.VMEM((bands, 2, width), full),
            pltpu.VMEM((segs, 2, width), full),
            pltpu.VMEM((segs, 2, width), full),
            pltpu.VMEM((total // BLOCK, BLOCK, 8), full),
            pltpu.VMEM((segs, width, n), full),
            pltpu.VMEM(spec, low),
            pltpu.VMEM(spec, low),
            pltpu.VMEM(spec, low),
            pltpu.VMEM((segs,) + spec, low),
            pltpu.VMEM((width, 2 * count), low),
            pltpu.VMEM((2 * recs, own // 2, n), low),
            pltpu.VMEM((2, own // 2, LAGS), low),
            pltpu.VMEM((2, own // 2, LAGS), low),
            pltpu.VMEM((bands,) + corr, low),
            pltpu.VMEM((bands,) + corr, low),
            pltpu.VMEM((recs, bands) + corr, low),
            pltpu.VMEM((segs, 2 * count, n), low),
            pltpu.SemaphoreType.REGULAR,
            pltpu.SemaphoreType.REGULAR,
            *sems(8, 8, 8, bands + 1, bands, 2, 2, 2, bands, bands, bands, bands, bands, bands),
        ],
        compiler_params=pltpu.CompilerParams(
            has_side_effects=True, collective_id=0, vmem_limit_bytes=VMEM_GRANT
        ),
        name="adjoint",
    )(records[0], pairs.T, observed, lag_mask, *tables)
    return result[None]


def fits_fused(shape, records, pairs):
    fibres, segs, recs = (shape[name] for name in ("fibre", "seg", "rec"))
    bands = fibres * segs
    width = records.shape[2] // (shape["groups"] * segs)
    return (
        fibres > 1
        and fibres & (fibres - 1) == 0
        and segs == 2
        and recs == 2
        and width % 128 == 0
        and width * segs <= 512
        and S // bands >= LAGS
        and pairs.shape[0] == bands * recs
    )


def solution(mesh):
    in_specs = (
        P("rec", "fibre", ("groups", "seg")),
        P(),
        P(("groups", "fibre", "seg"), None, None),
        P(("groups", "fibre", "seg"), None),
    )
    out_specs = P("rec", "fibre", ("groups", "seg"))
    shape = dict(mesh.shape)

    def run(records, pairs, observed, lag_mask):
        args = (records, pairs, observed, lag_mask)
        if not fits_fused(shape, records, pairs):
            return jax.shard_map(
                on_device, mesh=mesh, in_specs=in_specs, out_specs=out_specs, check_vma=False
            )(*args)
        tables = [jnp.asarray(t) for t in window_tables(shape["fibre"] * shape["seg"])]

        def body(*blocks):
            return fused_on_device(shape, tables, *blocks)

        return jax.shard_map(
            body, mesh=mesh, in_specs=in_specs, out_specs=out_specs, check_vma=False
        )(*args)

    return run
```

```python
import functools

import jax
import jax.numpy as jnp
import numpy as np
from jax import lax
from jax.experimental import pallas as pl
from jax.experimental.pallas import tpu as pltpu
from jax.sharding import PartitionSpec as P

S = 2048
F = 1024
LAGS = 256
BLOCK = 32
CH_DEV = 64
VMEM_GRANT = 60899328


def forward_table():
    freq_index = jnp.arange(F, dtype=jnp.int32)
    time_index = jnp.arange(S, dtype=jnp.int32)
    phase = freq_index[:, None] * time_index[None, :] % S
    angles = phase.astype(jnp.float32) * (2.0 * jnp.pi / S)
    scale = 1.0 / jnp.sqrt(jnp.float32(S))
    return jnp.stack(
        [
            (jnp.cos(angles) * scale).astype(jnp.bfloat16),
            (-jnp.sin(angles) * scale).astype(jnp.bfloat16),
        ],
        axis=1,
    )


def lag_table():
    freq_index = jnp.arange(F, dtype=jnp.int32)
    shifts = (jnp.arange(LAGS, dtype=jnp.int32) - LAGS // 2) % S
    phase = freq_index[:, None] * shifts[None, :] % S
    angles = phase.astype(jnp.float32) * (2.0 * jnp.pi / S)
    scale = 1.0 / jnp.sqrt(jnp.float32(F))
    return jnp.stack(
        [
            (jnp.cos(angles) * scale).astype(jnp.bfloat16),
            (-jnp.sin(angles) * scale).astype(jnp.bfloat16),
        ],
        axis=1,
    )


def synthesize(incoming, table):
    count = incoming.shape[-1]
    flat = incoming.reshape(2 * F, count)
    result = jnp.einsum(
        "qn,qt->tn", flat, table.reshape(2 * F, S), preferred_element_type=jnp.float32
    )
    return result.astype(jnp.bfloat16)


def on_device(records, pairs, observed, lag_mask):
    fibre_count = lax.axis_size("fibre")
    seg_count = lax.axis_size("seg")
    spread_count = fibre_count * seg_count
    freq_dev = F // spread_count
    blocks_dev = CH_DEV // BLOCK
    block_count = CH_DEV * spread_count // BLOCK
    pair_total = pairs.shape[0]
    pairs_dev = pair_total // spread_count
    table = forward_table()
    lags = lag_table()
    spans = records.reshape(1, S // fibre_count, fibre_count, CH_DEV)
    incoming = lax.all_to_all(spans, "fibre", split_axis=2, concat_axis=1, tiled=True)
    count = incoming.shape[3]
    signal = incoming.reshape(S, count)
    result = jnp.einsum(
        "qs,sn->qn", table.reshape(2 * F, S), signal, preferred_element_type=jnp.float32
    )
    spectra = result.reshape(F, 2, count).astype(jnp.bfloat16)
    widened = lax.all_to_all(spectra, ("fibre", "seg"), split_axis=0, concat_axis=2, tiled=True)
    seg_blocks = fibre_count * blocks_dev
    slot_ids = (
        pairs % seg_blocks // blocks_dev * seg_count + pairs // seg_blocks
    ) * blocks_dev + pairs % blocks_dev
    blocks_grid = widened.reshape(freq_dev, 2, block_count, BLOCK)
    first_side = jnp.take(blocks_grid, slot_ids[:, 0], axis=2).astype(jnp.float32)
    second_side = jnp.take(blocks_grid, slot_ids[:, 1], axis=2).astype(jnp.float32)
    first_re, first_im = (first_side[:, 0], first_side[:, 1])
    second_re, second_im = (second_side[:, 0], second_side[:, 1])
    cross_re = first_re * second_re + first_im * second_im
    cross_im = first_im * second_re - first_re * second_im
    cross_spec = jnp.stack([cross_re, cross_im], axis=1).astype(jnp.bfloat16)
    cross_spec = cross_spec.reshape(freq_dev, 2, spread_count, pairs_dev * BLOCK)
    owned_spec = lax.all_to_all(
        cross_spec, ("fibre", "seg"), split_axis=2, concat_axis=0, tiled=True
    )
    owned_spec = owned_spec.reshape(F, 2, pairs_dev * BLOCK)
    partial_corr = jnp.einsum("wpx,wpl->xl", owned_spec, lags, preferred_element_type=jnp.float32)
    synthetic = (
        lax.psum(partial_corr.astype(jnp.bfloat16), "rec")
        .astype(jnp.float32)
        .reshape(pairs_dev, BLOCK, LAGS)
    )
    weights = lag_mask[:, None, :].astype(jnp.float32) * jnp.tanh(synthetic - observed)
    weights_low = weights.astype(jnp.bfloat16).reshape(pairs_dev * BLOCK, LAGS)
    adjoint_spec = jnp.einsum("xl,wpl->wpx", weights_low, lags, preferred_element_type=jnp.float32)
    adjoint_spec = adjoint_spec.astype(jnp.bfloat16).reshape(F, 2, 1, pairs_dev * BLOCK)
    returned = lax.all_to_all(
        adjoint_spec, ("fibre", "seg"), split_axis=0, concat_axis=2, tiled=True
    )
    returned = returned.reshape(freq_dev, 2, pair_total, BLOCK).astype(jnp.float32)
    adjoint_re, adjoint_im = (returned[:, 0], returned[:, 1])
    grad_first = jnp.stack(
        [
            adjoint_re * second_re - adjoint_im * second_im,
            adjoint_re * second_im + adjoint_im * second_re,
        ],
        axis=1,
    )
    grad_second = jnp.stack(
        [
            adjoint_re * first_re + adjoint_im * first_im,
            adjoint_re * first_im - adjoint_im * first_re,
        ],
        axis=1,
    )
    contributions = jnp.concatenate([grad_first, grad_second], axis=2)
    endpoint_ids = jnp.concatenate([slot_ids[:, 0], slot_ids[:, 1]])
    summed = jax.ops.segment_sum(
        jnp.moveaxis(contributions, 2, 0), endpoint_ids, num_segments=block_count
    )
    block_adjoint = jnp.moveaxis(summed, 0, 2).astype(jnp.bfloat16)
    outgoing = block_adjoint.reshape(freq_dev, 2, spread_count, CH_DEV)
    sources = synthesize(
        lax.all_to_all(outgoing, ("fibre", "seg"), split_axis=2, concat_axis=0, tiled=True), table
    )
    regrouped = lax.all_to_all(sources, "fibre", split_axis=0, concat_axis=1, tiled=True)
    return regrouped[None]


def window_tables(bands):
    span, reach, n = S // bands, LAGS // 2, S // bands + LAGS
    half = n // 2
    freqs, places = np.arange(half), np.arange(n)
    shifts = np.arange(LAGS) - reach
    ends = np.where(freqs == 0, 1.0, 2.0) / (n * 2.0 * np.sqrt(F))

    def table(times, scale):
        angles = (freqs[None, :] * times[:, None] % n) * (2.0 * np.pi / n)
        real, imag = np.cos(angles), -np.sin(angles)
        imag[:, 0] = np.where(times % 2 == 0, 1.0, -1.0)
        return np.concatenate([real * scale, imag * scale], axis=1)

    whole = table(places, np.ones(half))
    lags = table(shifts, ends).T
    taps = table(shifts, np.ones(half))
    back = table(places[reach : reach + span], ends)
    return [t.astype(np.float32).astype(jnp.bfloat16) for t in (whole, lags, taps, back)]


def dot(left, right, left_dim=1, right_dim=0):
    return lax.dot_general(
        left,
        right,
        (((left_dim,), (right_dim,)), ((), ())),
        preferred_element_type=jnp.float32,
    )


def spectral_product(terms, sign):
    both = sum(p1 * q1 for (_, p1), (_, q1) in terms)
    real = sum(p0 * q0 for (p0, _), (q0, _) in terms)
    imag = sum(p1 * q0 - sign * (p0 * q1) for (p0, p1), (q0, q1) in terms)
    whole = real + sign * both
    ends = lax.broadcasted_iota(jnp.int32, (both.shape[0], 128), 1) == 0
    return tuple(
        jnp.concatenate([jnp.where(ends, end[:, :128], value[:, :128]), value[:, 128:]], axis=1)
        for end, value in ((real, whole), (both, imag))
    )


def fused_kernel(
    sizes, x_hbm, pairs_hbm, observed_hbm, mask_hbm, whole_hbm, lags_hbm, taps_hbm, back_hbm,
    out, pairs, ext, observed, mask, whole, lags, taps, back,
    inbox_sum, stage_total, inbox_total, columns, held_spec, core_spec, both_spec, left_spec,
    full_spec, select, cross, stage_core, inbox_core, stage3, inbox3, inbox4, grads,
    following, high, load_sem, send1, recv1, send_sum, recv_sum, total_sem, core_send, core_recv,
    relay_send, relay_recv, send3, recv3, send4, recv4,
):
    fibres, segs, recs = sizes
    bands = fibres * segs
    last = fibres - 1
    g, f, s, r = (lax.axis_index(name) for name in ("groups", "fibre", "seg", "rec"))
    o = 1 - s
    band = f * segs + s
    span, reach, width = S // bands, LAGS // 2, x_hbm.shape[1]
    n = span + LAGS
    half = n // 2
    blocks = width // BLOCK
    count = pairs.shape[1] * BLOCK
    low, full = jnp.bfloat16, jnp.float32

    def at(fibre, seg, rec):
        return (g, fibre, seg, rec)

    def at_band(index):
        return at(index // segs, index % segs, r)

    def remote(src, dst, send, recv, device):
        return pltpu.make_async_remote_copy(
            src_ref=src, dst_ref=dst, send_sem=send, recv_sem=recv,
            device_id=device, device_id_type=pl.DeviceIdType.MESH,
        )

    def push(src, dst, send, recv, device):
        copy = remote(src, dst, send, recv, device)
        copy.start()
        return copy

    def arrived(dst, recv):
        remote(dst, dst, recv, recv, at(f, s, 1 - r)).wait_recv()

    def signal(sem, device):
        pl.semaphore_signal(sem, inc=1, device_id=device, device_id_type=pl.DeviceIdType.MESH)

    def rows(start, size, unit):
        return pl.ds(pl.multiple_of(start, unit), size)

    def flipped(index, bits):
        result, bit = 0, 1
        while bit < bands:
            digit = index // bit % 2
            result += bit * (1 - digit if bits // bit % 2 else digit)
            bit *= 2
        return result

    partner = at(f, s, 1 - r)
    across = at(f, o, r)
    places = [(fi, si) for fi in range(fibres) for si in range(segs)]

    barrier = pltpu.get_barrier_semaphore()
    signal(barrier, partner)
    signal(barrier, across)
    for fi, si in places:

        @pl.when(fi > f)
        def _():
            signal(barrier, at(fi, si, r))

    loads = [
        pltpu.make_async_copy(src, dst, load_sem.at[i])
        for i, (src, dst) in enumerate(
            [
                (x_hbm, ext.at[s, pl.ds(reach, 2 * span)]), (pairs_hbm, pairs), (whole_hbm, whole), (lags_hbm, lags),
                (observed_hbm.at[r], observed), (mask_hbm, mask), (taps_hbm, taps), (back_hbm, back),
            ]
        )
    ]
    for load in loads:
        load.start()

    def give(first, size, place, send, recv, device):
        return remote(
            x_hbm.at[pl.ds(first, size)], ext.at[s, pl.ds(place, size)], send1.at[send], recv1.at[recv], device
        )

    needed = [
        [give(span, span, span + reach, 0, 0, across), give(reach, reach, 2 * reach, 1, 1, across)],
        [give(0, span, reach, 0, 0, across)],
    ]
    later = [give(0, reach, reach, 2, 2, across), give(span, span, reach + span, 2, 2, across)]
    upper, lower = (f + 1) % fibres, (f + last) % fibres
    up = give(2 * span - reach, reach, 0, 3, 3, at(upper, s, r))
    up_across = give(2 * span - reach, reach, 0, 4, 4, at(upper, 0, r))
    down = give(0, reach, reach + 2 * span, 5, 5, at(lower, s, r))
    edges = [pl.ds(0, reach), pl.ds(reach + 2 * span, reach)]
    passed = [
        remote(ext.at[s, edge], ext.at[s, edge], send1.at[6 + i], recv1.at[6 + i], across)
        for i, edge in enumerate(edges)
    ]

    def send_up():
        @pl.when(s == 0)
        def _():
            up.start()

        @pl.when(s == 1)
        def _():
            up_across.start()

    pl.semaphore_wait(barrier, segs * (f + 1))
    for si in range(segs):

        @pl.when(s == si)
        def _():
            for copy in needed[si]:
                copy.start()

    @pl.when(f == last)
    def _():
        send_up()

    for fi, si in places:

        @pl.when(fi == f - 1)
        def _():
            signal(following, at(fi, si, r))

        @pl.when(fi < f - 1)
        def _():
            signal(high, at(fi, si, r))

    loads[0].wait()
    folded = ext[s, pl.ds(reach, 2 * span)].astype(full).reshape(-1, 8, width).sum(axis=0)
    odd = lax.broadcasted_iota(jnp.int32, folded.shape, 0) % 2 == 1
    inbox_sum[band] = jnp.concatenate(
        [
            jnp.sum(folded, axis=0, keepdims=True),
            jnp.sum(jnp.where(odd, -folded, folded), axis=0, keepdims=True),
        ],
        axis=0,
    )
    sends = [up, down]
    own_sum = inbox_sum.at[band]
    sum_sends = [
        remote(own_sum, own_sum, send_sum.at[fi * segs + si], recv_sum.at[band], at(fi, si, r)) for fi, si in places
    ]
    across_sum = push(own_sum, own_sum, send_sum.at[bands], recv_sum.at[band], across)
    sends.append(across_sum)
    for (fi, si), copy in zip(places, sum_sends):

        @pl.when(fi < f)
        def _():
            copy.start()

    loads[1].wait()
    cut = bands // 2
    near = band // cut
    groups = [(r, near), (r, 1 - near), (1 - r, near), (1 - r, 1 - near)]
    group = 2 * cut * BLOCK
    lane = lax.broadcasted_iota(jnp.int32, (1, 2 * count), 1)
    target = lane
    for p, (h, side) in enumerate(groups):
        for end in range(2):
            for i in range(cut):
                first = p * group + (end * cut + i) * BLOCK
                inside = (lane >= first) & (lane < first + BLOCK)
                target = jnp.where(inside, lane + (pairs[end, (side * cut + i) * recs + h] * BLOCK - first), target)
    line = lax.broadcasted_iota(jnp.int32, select.shape, 0) + s * width
    select[...] = jnp.where(line == target, 1.0, 0.0).astype(low)

    def put(spec, seg, value):
        spec[rows(seg * blocks, blocks, blocks)] = value.astype(low).reshape(blocks, BLOCK, n)

    def core_part(seg):
        part = dot(ext[seg, rows(reach + span * s, span, reach)], whole[reach : reach + span], 0, 0)
        held_spec[seg] = part
        put(core_spec, seg, part)

    def left_part(seg):
        part = dot(ext[seg, rows(span * s, reach, reach)], whole[:reach], 0, 0)
        put(left_spec, seg, part)
        put(both_spec, seg, part + held_spec[seg])

    loads[2].wait()
    core_part(s)

    @pl.when(f < last)
    def _():
        pl.semaphore_wait(following, segs)
        send_up()

    for si in range(segs):

        @pl.when(s == 1 - si)
        def _():
            arrived(ext.at[si, pl.ds(reach + span * (1 - si), span)], recv1.at[0])

    core_part(o)

    @pl.when(f < last - 1)
    def _():
        pl.semaphore_wait(high, segs * (last - 1 - f))

    for (fi, si), copy in zip(places, sum_sends):

        @pl.when(fi > f)
        def _():
            copy.start()

    @pl.when(s == 1)
    def _():
        up.start()

    down.start()

    def send_later():
        for si in range(segs):

            @pl.when(s == si)
            def _():
                later[si].start()

    pl.when(f == 0)(send_later)

    @pl.when(s == 0)
    def _():
        arrived(ext.at[0, edges[0]], recv1.at[3])

    left_part(s)

    @pl.when(s == 0)
    def _():
        arrived(ext.at[1, edges[0]], recv1.at[4])

    @pl.when(s == 1)
    def _():
        arrived(ext.at[0, pl.ds(2 * reach, reach)], recv1.at[1])

    pl.when(f > 0)(send_later)
    left_part(o)

    def block(spec, index):
        value = spec[index].astype(full)
        return value[:, :half], value[:, half:]

    ordered = sorted(range(bands), key=lambda j: (-abs(2 * (j // segs) - last), -j))
    chunks = ordered[:cut], ordered[cut:]

    def correlate(place, h, chunk):
        for i, j in enumerate(chunk):
            pair = j * recs + h
            one, two = pairs[0, pair], pairs[1, pair]
            terms = [(block(core_spec, one), block(both_spec, two)), (block(left_spec, one), block(core_spec, two))]
            real, imag = spectral_product(terms, 1.0)
            here = pl.ds(i * BLOCK, BLOCK)
            cross[place, here, pl.ds(0, half)] = real.astype(low)
            cross[place, here, pl.ds(half, half)] = imag.astype(low)
        return dot(cross[place], lags[...])

    loads[3].wait()
    for i, chunk in enumerate(chunks):
        stage_core[i] = correlate(i, 1 - r, chunk).astype(low)
        sends.append(push(stage_core.at[i], inbox_core.at[i], core_send.at[i], core_recv.at[i], partner))

    spread3 = [
        remote(stage3.at[j], inbox3.at[band], send3.at[j], recv3.at[band], at(j // segs, j % segs, r))
        for j in range(bands)
    ]
    for i, chunk in enumerate(chunks):
        partial = correlate(2 + i, r, chunk)
        arrived(inbox_core.at[i], core_recv.at[i])
        partial = (partial + inbox_core[i].astype(full)).astype(low)
        for place, j in enumerate(chunk):
            stage3[j] = partial[place * BLOCK : (place + 1) * BLOCK]

            @pl.when(band != j)
            def _():
                spread3[j].start()

    inbox3[band] = stage3[band]

    @pl.when(s == 0)
    def _():
        passed[0].start()

    @pl.when(s == 1)
    def _():
        arrived(ext.at[1, edges[0]], recv1.at[3])

    arrived(ext.at[s, edges[1]], recv1.at[5])
    passed[1].start()

    for d in range(1, bands):
        k = flipped(band, d)
        arrived(inbox_sum.at[k], recv_sum.at[k])
    for seg in range(segs):
        stage_total[seg] = sum(inbox_sum[fi * segs + seg] for fi in range(fibres))
    sends.append(push(stage_total, inbox_total, total_sem.at[0], total_sem.at[1], partner))
    arrived(inbox_total, total_sem.at[1])
    for seg in range(segs):
        total = jnp.concatenate([stage_total[seg], inbox_total[seg]] * 2, axis=0)
        columns[pl.ds(seg * blocks, blocks)] = total.T.reshape(blocks, BLOCK, 8)
    loads[4].wait()
    loads[5].wait()
    ends = columns[pairs[0, band * recs + r]] * columns[pairs[1, band * recs + r]]
    flat = ends[:, 0:1] + ends[:, 2:3]
    alternating = ends[:, 1:2] + ends[:, 3:4]
    even = lax.broadcasted_iota(jnp.int32, (BLOCK, LAGS), 1) % 2 == reach % 2
    offset = (flat + jnp.where(even, -alternating, alternating)) * (1.0 / (2.0 * S * F**0.5))
    for d in range(1, bands):
        k = flipped(band, d)
        arrived(inbox3.at[k], recv3.at[k])
    synthetic = offset + inbox3[0].astype(full)
    for k in range(1, bands):
        synthetic += inbox3[k].astype(full)
    window = mask[pl.ds(r, 1), :].astype(full)
    inbox4[r, band] = (window * jnp.tanh(synthetic - observed[...])).astype(low)
    own = inbox4.at[r, band]
    spread4 = [
        remote(own, own, send4.at[j], recv4.at[band], at(j // segs, j % segs, r)) for j in range(bands)
    ]
    for j in range(bands):

        @pl.when(band != j)
        def _():
            spread4[j].start()

    sends.append(push(own, own, relay_send.at[0], relay_recv.at[band], partner))

    for si in range(segs):

        @pl.when(s == 1 - si)
        def _():
            arrived(ext.at[si, pl.ds(reach + span * si, reach + (span - reach) * si)], recv1.at[2])

    @pl.when(s == 1)
    def _():
        arrived(ext.at[0, edges[0]], recv1.at[6])

    arrived(ext.at[o, edges[1]], recv1.at[7])
    head = lax.broadcasted_iota(jnp.int32, (1, half), 1) == 0
    for seg in range(segs):
        total = jnp.concatenate([stage_total[seg]] * 4, axis=0).T * (n / S)
        for w in range(segs):
            value = dot(ext[seg, pl.ds(span * w, n)], whole[...], 0, 0)
            value = jnp.concatenate(
                [
                    value[:, :half] + jnp.where(head, total[:, 0:1], 0.0),
                    value[:, half:] - jnp.where(head, total[:, 1:2], 0.0),
                ],
                axis=1,
            )
            put(full_spec.at[w], seg, value)
    loads[6].wait()

    def gradients(p):
        h, side = groups[p]
        spread = dot(inbox4[h, pl.ds(side * cut, cut)].reshape(cut * BLOCK, LAGS), taps[...])
        for i in range(cut):
            pair = (side * cut + i) * recs + h
            filters = spread[i * BLOCK : (i + 1) * BLOCK]
            filters = filters[:, :half], filters[:, half:]
            base = p * group + i * BLOCK
            for w in range(segs):
                first = block(full_spec.at[w], pairs[0, pair])
                second = block(full_spec.at[w], pairs[1, pair])
                for start, parts in (
                    (base, spectral_product([(filters, second)], -1.0)),
                    (base + cut * BLOCK, spectral_product([(first, filters)], 1.0)),
                ):
                    for q in range(2):
                        grads[w, pl.ds(start, BLOCK), pl.ds(q * half, half)] = parts[q].astype(low)

    for d in range(1, bands):
        k = flipped(band, d)
        arrived(inbox4.at[r, k], recv4.at[k])
        got = inbox4.at[r, k]
        sends.append(push(got, got, relay_send.at[d], relay_recv.at[k], partner))
    for p, (first, stop) in enumerate(((0, 0), (0, 0), (0, cut), (cut, bands))):
        for d in range(first, stop):
            k = flipped(band, d)
            arrived(inbox4.at[1 - r, k], relay_recv.at[k])
        gradients(p)
    loads[7].wait()

    for w in range(segs):
        summed = dot(select[...], grads[w]).astype(low)
        out[pl.ds(span * w, span), :] = dot(back[...], summed, 1, 1).astype(low)
    for si in range(segs):

        @pl.when(s == si)
        def _():
            for copy in needed[si] + [later[si]] + passed[si:]:
                copy.wait_send()

    @pl.when(s == 1)
    def _():
        up_across.wait_send()

    for copy in sends:
        copy.wait_send()
    for j in range(bands):

        @pl.when(band != j)
        def _():
            spread3[j].wait_send()
            spread4[j].wait_send()

    for (fi, si), copy in zip(places, sum_sends):

        @pl.when(fi != f)
        def _():
            copy.wait_send()


def fused_on_device(mesh_shape, tables, records, pairs, observed, lag_mask):
    fibres, segs, recs = (mesh_shape[name] for name in ("fibre", "seg", "rec"))
    bands = fibres * segs
    _, extent, width = records.shape
    span, reach = S // bands, LAGS // 2
    n = span + LAGS
    count = pairs.shape[0] * BLOCK
    own = count // recs
    total = segs * width
    low, full = jnp.bfloat16, jnp.float32
    vmem = pl.BlockSpec(memory_space=pltpu.VMEM)
    hbm = pl.BlockSpec(memory_space=pltpu.HBM)
    corr = (BLOCK, LAGS)
    spec = (total // BLOCK, BLOCK, n)

    def sems(*sizes):
        return [pltpu.SemaphoreType.DMA((size,)) for size in sizes]

    result = pl.pallas_call(
        functools.partial(fused_kernel, (fibres, segs, recs)),
        out_shape=pltpu.VMEM((extent, width), low),
        in_specs=[hbm] * 8,
        out_specs=vmem,
        scratch_shapes=[
            pltpu.SMEM((2, pairs.shape[0]), jnp.int32),
            pltpu.VMEM((segs, 2 * span + 2 * reach, width), low),
            pltpu.VMEM(corr, full),
            pltpu.VMEM(lag_mask.shape, jnp.int32),
            pltpu.VMEM((n, n), low),
            pltpu.VMEM((n, LAGS), low),
            pltpu.VMEM((LAGS, n), low),
            pltpu.VMEM((span, n), low),
            pltpu.VMEM((bands, 2, width), full),
            pltpu.VMEM((segs, 2, width), full),
            pltpu.VMEM((segs, 2, width), full),
            pltpu.VMEM((total // BLOCK, BLOCK, 8), full),
            pltpu.VMEM((segs, width, n), full),
            pltpu.VMEM(spec, low),
            pltpu.VMEM(spec, low),
            pltpu.VMEM(spec, low),
            pltpu.VMEM((segs,) + spec, low),
            pltpu.VMEM((width, 2 * count), low),
            pltpu.VMEM((2 * recs, own // 2, n), low),
            pltpu.VMEM((2, own // 2, LAGS), low),
            pltpu.VMEM((2, own // 2, LAGS), low),
            pltpu.VMEM((bands,) + corr, low),
            pltpu.VMEM((bands,) + corr, low),
            pltpu.VMEM((recs, bands) + corr, low),
            pltpu.VMEM((segs, 2 * count, n), low),
            pltpu.SemaphoreType.REGULAR,
            pltpu.SemaphoreType.REGULAR,
            *sems(8, 8, 8, bands + 1, bands, 2, 2, 2, bands, bands, bands, bands, bands, bands),
        ],
        compiler_params=pltpu.CompilerParams(
            has_side_effects=True, collective_id=0, vmem_limit_bytes=VMEM_GRANT
        ),
        name="adjoint",
    )(records[0], pairs.T, observed, lag_mask, *tables)
    return result[None]


def fits_fused(shape, records, pairs):
    fibres, segs, recs = (shape[name] for name in ("fibre", "seg", "rec"))
    bands = fibres * segs
    width = records.shape[2] // (shape["groups"] * segs)
    return (
        fibres > 1
        and fibres & (fibres - 1) == 0
        and segs == 2
        and recs == 2
        and width % 128 == 0
        and width * segs <= 512
        and S // bands >= LAGS
        and pairs.shape[0] == bands * recs
    )


def solution(mesh):
    in_specs = (
        P("rec", "fibre", ("groups", "seg")),
        P(),
        P(("groups", "fibre", "seg"), None, None),
        P(("groups", "fibre", "seg"), None),
    )
    out_specs = P("rec", "fibre", ("groups", "seg"))
    shape = dict(mesh.shape)

    def run(records, pairs, observed, lag_mask):
        args = (records, pairs, observed, lag_mask)
        if not fits_fused(shape, records, pairs):
            return jax.shard_map(
                on_device, mesh=mesh, in_specs=in_specs, out_specs=out_specs, check_vma=False
            )(*args)
        tables = [jnp.asarray(t) for t in window_tables(shape["fibre"] * shape["seg"])]

        def body(*blocks):
            return fused_on_device(shape, tables, *blocks)

        return jax.shard_map(
            body, mesh=mesh, in_specs=in_specs, out_specs=out_specs, check_vma=False
        )(*args)

    return run
```

```python
import functools

import jax
import jax.numpy as jnp
import numpy as np
from jax import lax
from jax.experimental import pallas as pl
from jax.experimental.pallas import tpu as pltpu
from jax.sharding import PartitionSpec as P

S = 2048
F = 1024
LAGS = 256
BLOCK = 32
CH_DEV = 64
VMEM_GRANT = 60899328


def forward_table():
    freq_index = jnp.arange(F, dtype=jnp.int32)
    time_index = jnp.arange(S, dtype=jnp.int32)
    phase = freq_index[:, None] * time_index[None, :] % S
    angles = phase.astype(jnp.float32) * (2.0 * jnp.pi / S)
    scale = 1.0 / jnp.sqrt(jnp.float32(S))
    return jnp.stack(
        [
            (jnp.cos(angles) * scale).astype(jnp.bfloat16),
            (-jnp.sin(angles) * scale).astype(jnp.bfloat16),
        ],
        axis=1,
    )


def lag_table():
    freq_index = jnp.arange(F, dtype=jnp.int32)
    shifts = (jnp.arange(LAGS, dtype=jnp.int32) - LAGS // 2) % S
    phase = freq_index[:, None] * shifts[None, :] % S
    angles = phase.astype(jnp.float32) * (2.0 * jnp.pi / S)
    scale = 1.0 / jnp.sqrt(jnp.float32(F))
    return jnp.stack(
        [
            (jnp.cos(angles) * scale).astype(jnp.bfloat16),
            (-jnp.sin(angles) * scale).astype(jnp.bfloat16),
        ],
        axis=1,
    )


def synthesize(incoming, table):
    count = incoming.shape[-1]
    flat = incoming.reshape(2 * F, count)
    result = jnp.einsum(
        "qn,qt->tn", flat, table.reshape(2 * F, S), preferred_element_type=jnp.float32
    )
    return result.astype(jnp.bfloat16)


def on_device(records, pairs, observed, lag_mask):
    fibre_count = lax.axis_size("fibre")
    seg_count = lax.axis_size("seg")
    spread_count = fibre_count * seg_count
    freq_dev = F // spread_count
    blocks_dev = CH_DEV // BLOCK
    block_count = CH_DEV * spread_count // BLOCK
    pair_total = pairs.shape[0]
    pairs_dev = pair_total // spread_count
    table = forward_table()
    lags = lag_table()
    spans = records.reshape(1, S // fibre_count, fibre_count, CH_DEV)
    incoming = lax.all_to_all(spans, "fibre", split_axis=2, concat_axis=1, tiled=True)
    count = incoming.shape[3]
    signal = incoming.reshape(S, count)
    result = jnp.einsum(
        "qs,sn->qn", table.reshape(2 * F, S), signal, preferred_element_type=jnp.float32
    )
    spectra = result.reshape(F, 2, count).astype(jnp.bfloat16)
    widened = lax.all_to_all(spectra, ("fibre", "seg"), split_axis=0, concat_axis=2, tiled=True)
    seg_blocks = fibre_count * blocks_dev
    slot_ids = (
        pairs % seg_blocks // blocks_dev * seg_count + pairs // seg_blocks
    ) * blocks_dev + pairs % blocks_dev
    blocks_grid = widened.reshape(freq_dev, 2, block_count, BLOCK)
    first_side = jnp.take(blocks_grid, slot_ids[:, 0], axis=2).astype(jnp.float32)
    second_side = jnp.take(blocks_grid, slot_ids[:, 1], axis=2).astype(jnp.float32)
    first_re, first_im = (first_side[:, 0], first_side[:, 1])
    second_re, second_im = (second_side[:, 0], second_side[:, 1])
    cross_re = first_re * second_re + first_im * second_im
    cross_im = first_im * second_re - first_re * second_im
    cross_spec = jnp.stack([cross_re, cross_im], axis=1).astype(jnp.bfloat16)
    cross_spec = cross_spec.reshape(freq_dev, 2, spread_count, pairs_dev * BLOCK)
    owned_spec = lax.all_to_all(
        cross_spec, ("fibre", "seg"), split_axis=2, concat_axis=0, tiled=True
    )
    owned_spec = owned_spec.reshape(F, 2, pairs_dev * BLOCK)
    partial_corr = jnp.einsum("wpx,wpl->xl", owned_spec, lags, preferred_element_type=jnp.float32)
    synthetic = (
        lax.psum(partial_corr.astype(jnp.bfloat16), "rec")
        .astype(jnp.float32)
        .reshape(pairs_dev, BLOCK, LAGS)
    )
    weights = lag_mask[:, None, :].astype(jnp.float32) * jnp.tanh(synthetic - observed)
    weights_low = weights.astype(jnp.bfloat16).reshape(pairs_dev * BLOCK, LAGS)
    adjoint_spec = jnp.einsum("xl,wpl->wpx", weights_low, lags, preferred_element_type=jnp.float32)
    adjoint_spec = adjoint_spec.astype(jnp.bfloat16).reshape(F, 2, 1, pairs_dev * BLOCK)
    returned = lax.all_to_all(
        adjoint_spec, ("fibre", "seg"), split_axis=0, concat_axis=2, tiled=True
    )
    returned = returned.reshape(freq_dev, 2, pair_total, BLOCK).astype(jnp.float32)
    adjoint_re, adjoint_im = (returned[:, 0], returned[:, 1])
    grad_first = jnp.stack(
        [
            adjoint_re * second_re - adjoint_im * second_im,
            adjoint_re * second_im + adjoint_im * second_re,
        ],
        axis=1,
    )
    grad_second = jnp.stack(
        [
            adjoint_re * first_re + adjoint_im * first_im,
            adjoint_re * first_im - adjoint_im * first_re,
        ],
        axis=1,
    )
    contributions = jnp.concatenate([grad_first, grad_second], axis=2)
    endpoint_ids = jnp.concatenate([slot_ids[:, 0], slot_ids[:, 1]])
    summed = jax.ops.segment_sum(
        jnp.moveaxis(contributions, 2, 0), endpoint_ids, num_segments=block_count
    )
    block_adjoint = jnp.moveaxis(summed, 0, 2).astype(jnp.bfloat16)
    outgoing = block_adjoint.reshape(freq_dev, 2, spread_count, CH_DEV)
    sources = synthesize(
        lax.all_to_all(outgoing, ("fibre", "seg"), split_axis=2, concat_axis=0, tiled=True), table
    )
    regrouped = lax.all_to_all(sources, "fibre", split_axis=0, concat_axis=1, tiled=True)
    return regrouped[None]


def window_tables(bands):
    span, reach, n = S // bands, LAGS // 2, S // bands + LAGS
    half = n // 2
    freqs, places = np.arange(half), np.arange(n)
    shifts = np.arange(LAGS) - reach
    ends = np.where(freqs == 0, 1.0, 2.0) / (n * 2.0 * np.sqrt(F))

    def table(times, scale):
        angles = (freqs[None, :] * times[:, None] % n) * (2.0 * np.pi / n)
        real, imag = np.cos(angles), -np.sin(angles)
        imag[:, 0] = np.where(times % 2 == 0, 1.0, -1.0)
        return np.concatenate([real * scale, imag * scale], axis=1)

    whole = table(places, np.ones(half))
    lags = table(shifts, ends).T
    taps = table(shifts, np.ones(half))
    back = table(places[reach : reach + span], ends)
    lags = np.concatenate([lags, lags])
    return [t.astype(np.float32).astype(jnp.bfloat16) for t in (whole, lags, taps, back)]


def dot(left, right, left_dim=1, right_dim=0):
    return lax.dot_general(
        left,
        right,
        (((left_dim,), (right_dim,)), ((), ())),
        preferred_element_type=jnp.float32,
    )


def spectral_product(terms, sign, extra=None):
    both = sum(p1 * q1 for (_, p1), (_, q1) in terms)
    real = sum(p0 * q0 for (p0, _), (q0, _) in terms)
    imag = sum(p1 * q0 - sign * (p0 * q1) for (p0, p1), (q0, q1) in terms)
    whole = real + sign * both
    ends = lax.broadcasted_iota(jnp.int32, (both.shape[0], 128), 1) == 0
    return tuple(
        jnp.concatenate([jnp.where(ends, end, value[:, :128]), value[:, 128:]], axis=1)
        for end, value in ((real[:, :128], whole), (both[:, :128] if extra is None else both[:, :128] + extra, imag))
    )


def fused_kernel(
    sizes, x_hbm, pairs_hbm, observed_hbm, mask_hbm, whole_hbm, lags_hbm, taps_hbm, back_hbm,
    out, pairs, ext, observed, mask, whole, lags, taps, back,
    inbox_sum, stage_total, inbox_total, columns, core_spec, both_spec, left_spec,
    full_spec, select, cross, stage_core, inbox_core, stage3, inbox3, inbox4, grads,
    following, high, load_sem, send1, recv1, send_sum, recv_sum, total_sem, core_send, core_recv,
    relay_send, relay_recv, send3, recv3, send4, recv4,
):
    fibres, segs, recs = sizes
    bands = fibres * segs
    last = fibres - 1
    g, f, s, r = (lax.axis_index(name) for name in ("groups", "fibre", "seg", "rec"))
    o = 1 - s
    band = f * segs + s
    span, reach, width = S // bands, LAGS // 2, x_hbm.shape[1]
    n = span + LAGS
    half = n // 2
    blocks = width // BLOCK
    count = pairs.shape[1] * BLOCK
    low, full = jnp.bfloat16, jnp.float32

    def at(fibre, seg, rec):
        return (g, fibre, seg, rec)

    def at_band(index):
        return at(index // segs, index % segs, r)

    def remote(src, dst, send, recv, device):
        return pltpu.make_async_remote_copy(
            src_ref=src, dst_ref=dst, send_sem=send, recv_sem=recv,
            device_id=device, device_id_type=pl.DeviceIdType.MESH,
        )

    def push(src, dst, send, recv, device):
        copy = remote(src, dst, send, recv, device)
        copy.start()
        return copy

    def arrived(dst, recv):
        remote(dst, dst, recv, recv, at(f, s, 1 - r)).wait_recv()

    def signal(sem, device):
        pl.semaphore_signal(sem, inc=1, device_id=device, device_id_type=pl.DeviceIdType.MESH)

    def rows(start, size, unit):
        return pl.ds(pl.multiple_of(start, unit), size)

    def flipped(index, bits):
        result, bit = 0, 1
        while bit < bands:
            digit = index // bit % 2
            result += bit * (1 - digit if bits // bit % 2 else digit)
            bit *= 2
        return result

    partner = at(f, s, 1 - r)
    across = at(f, o, r)
    places = [(fi, si) for fi in range(fibres) for si in range(segs)]

    barrier = pltpu.get_barrier_semaphore()
    signal(barrier, partner)
    signal(barrier, across)
    for fi, si in places:

        @pl.when(fi > f)
        def _():
            signal(barrier, at(fi, si, r))

    loads = [
        pltpu.make_async_copy(src, dst, load_sem.at[i])
        for i, (src, dst) in enumerate(
            [
                (x_hbm, ext.at[s, pl.ds(reach, 2 * span)]), (pairs_hbm, pairs), (whole_hbm, whole), (lags_hbm, lags),
                (observed_hbm.at[r], observed), (mask_hbm, mask), (taps_hbm, taps), (back_hbm, back),
            ]
        )
    ]
    for load in loads:
        load.start()

    def give(first, size, place, send, recv, device):
        return remote(
            x_hbm.at[pl.ds(first, size)], ext.at[s, pl.ds(place, size)], send1.at[send], recv1.at[recv], device
        )

    needed = [
        [give(span, span, span + reach, 0, 0, across), give(reach, reach, 2 * reach, 1, 1, across)],
        [give(0, span, reach, 0, 0, across)],
    ]
    later = [give(0, reach, reach, 2, 2, across), give(span, span, reach + span, 2, 2, across)]
    upper, lower = (f + 1) % fibres, (f + last) % fibres
    up = give(2 * span - reach, reach, 0, 3, 3, at(upper, s, r))
    up_across = give(2 * span - reach, reach, 0, 4, 4, at(upper, 0, r))
    down = give(0, reach, reach + 2 * span, 5, 5, at(lower, s, r))
    edges = [pl.ds(0, reach), pl.ds(reach + 2 * span, reach)]
    passed = [
        remote(ext.at[s, edge], ext.at[s, edge], send1.at[6 + i], recv1.at[6 + i], across)
        for i, edge in enumerate(edges)
    ]

    def send_up():
        @pl.when(s == 0)
        def _():
            up.start()

        @pl.when(s == 1)
        def _():
            up_across.start()

    pl.semaphore_wait(barrier, segs * (f + 1))
    for si in range(segs):

        @pl.when(s == si)
        def _():
            for copy in needed[si]:
                copy.start()

    @pl.when(f == last)
    def _():
        send_up()

    for fi, si in places:

        @pl.when(fi == f - 1)
        def _():
            signal(following, at(fi, si, r))

        @pl.when(fi < f - 1)
        def _():
            signal(high, at(fi, si, r))

    loads[0].wait()
    folded = [
        ext[s, pl.ds(reach + span * w, span)].astype(full).reshape(-1, 8, width).sum(axis=0) for w in range(segs)
    ]
    odd = lax.broadcasted_iota(jnp.int32, (8, width), 0) % 2 == 1
    flat = jnp.sum(folded[0] + folded[1], axis=0, keepdims=True)
    turned = [jnp.sum(jnp.where(odd, -part, part), axis=0, keepdims=True) for part in folded]
    inbox_sum[band] = jnp.concatenate([flat] + turned + [jnp.zeros_like(flat)], axis=0)
    sends = [up, down]
    own_sum = inbox_sum.at[band]
    sum_sends = [
        remote(own_sum, own_sum, send_sum.at[fi * segs + si], recv_sum.at[band], at(fi, si, r)) for fi, si in places
    ]
    across_sum = push(own_sum, own_sum, send_sum.at[bands], recv_sum.at[band], across)
    sends.append(across_sum)
    for (fi, si), copy in zip(places, sum_sends):

        @pl.when(fi < f)
        def _():
            copy.start()

    loads[1].wait()
    cut = bands // 2
    near = band // cut
    groups = [(r, near), (r, 1 - near), (1 - r, near), (1 - r, 1 - near)]
    group = 2 * cut * BLOCK
    lane = lax.broadcasted_iota(jnp.int32, (1, 2 * count), 1)
    target = lane
    for p, (h, side) in enumerate(groups):
        for end in range(2):
            for i in range(cut):
                first = p * group + (end * cut + i) * BLOCK
                inside = (lane >= first) & (lane < first + BLOCK)
                target = jnp.where(inside, lane + (pairs[end, (side * cut + i) * recs + h] * BLOCK - first), target)
    line = lax.broadcasted_iota(jnp.int32, select.shape, 0) + s * width
    select[...] = jnp.where(line == target, 1.0, 0.0).astype(low)

    def put(spec, seg, value):
        spec[rows(seg * blocks, blocks, blocks)] = value.astype(spec.dtype).reshape(blocks, BLOCK, n)

    def core_part(seg):
        part = dot(ext[seg, rows(reach + span * s, span, reach)], whole[reach : reach + span], 0, 0)
        put(core_spec, seg, part)

    def left_part(seg):
        part = dot(ext[seg, rows(span * s, reach, reach)], whole[:reach], 0, 0)
        put(left_spec, seg, part)
        put(both_spec, seg, part + core_spec[rows(seg * blocks, blocks, blocks)].reshape(width, n))

    loads[2].wait()
    core_part(s)

    @pl.when(f < last)
    def _():
        pl.semaphore_wait(following, segs)
        send_up()

    for si in range(segs):

        @pl.when(s == 1 - si)
        def _():
            arrived(ext.at[si, pl.ds(reach + span * (1 - si), span)], recv1.at[0])

    core_part(o)

    @pl.when(f < last - 1)
    def _():
        pl.semaphore_wait(high, segs * (last - 1 - f))

    for (fi, si), copy in zip(places, sum_sends):

        @pl.when(fi > f)
        def _():
            copy.start()

    @pl.when(s == 1)
    def _():
        up.start()

    down.start()

    def send_later():
        for si in range(segs):

            @pl.when(s == si)
            def _():
                later[si].start()

    pl.when(f == 0)(send_later)

    @pl.when(s == 0)
    def _():
        arrived(ext.at[0, edges[0]], recv1.at[3])

    left_part(s)

    @pl.when(s == 0)
    def _():
        arrived(ext.at[1, edges[0]], recv1.at[4])

    @pl.when(s == 1)
    def _():
        arrived(ext.at[0, pl.ds(2 * reach, reach)], recv1.at[1])

    pl.when(f > 0)(send_later)
    left_part(o)

    def block(spec, index):
        value = spec[index].astype(full)
        return value[:, :half], value[:, half:]

    ordered = sorted(range(bands), key=lambda j: (-abs(2 * (j // segs) - last), -j))
    chunks = ordered[:cut], ordered[cut:]

    def correlate(place, h, chunk):
        for i, j in enumerate(chunk):
            pair = j * recs + h
            one, two = pairs[0, pair], pairs[1, pair]
            terms = [(block(core_spec, one), block(both_spec, two)), (block(left_spec, one), block(core_spec, two))]
            inner = terms[0][0][1][:, :128] * terms[1][1][1][:, :128]
            parts = spectral_product(terms, 1.0, inner * (-n / span))
            for q, part in enumerate(parts):
                high_part = part.astype(low)
                here = pl.ds(i * BLOCK, BLOCK)
                cross[place, here, pl.ds(q * half, half)] = high_part
                cross[place, here, pl.ds(n + q * half, half)] = (part - high_part.astype(full)).astype(low)
        return dot(cross[place], lags[...])

    loads[3].wait()
    for i, chunk in enumerate(chunks):
        stage_core[i] = correlate(i, 1 - r, chunk).astype(low)
        sends.append(push(stage_core.at[i], inbox_core.at[i], core_send.at[i], core_recv.at[i], partner))

    spread3 = [
        remote(stage3.at[j], inbox3.at[band], send3.at[j], recv3.at[band], at(j // segs, j % segs, r))
        for j in range(bands)
    ]
    for i, chunk in enumerate(chunks):
        partial = correlate(2 + i, r, chunk)
        arrived(inbox_core.at[i], core_recv.at[i])
        partial = (partial + inbox_core[i].astype(full)).astype(low)
        for place, j in enumerate(chunk):
            stage3[j] = partial[place * BLOCK : (place + 1) * BLOCK]

            @pl.when(band != j)
            def _():
                spread3[j].start()

    inbox3[band] = stage3[band]

    @pl.when(s == 0)
    def _():
        passed[0].start()

    @pl.when(s == 1)
    def _():
        arrived(ext.at[1, edges[0]], recv1.at[3])

    arrived(ext.at[s, edges[1]], recv1.at[5])
    passed[1].start()

    for d in range(1, bands):
        k = flipped(band, d)
        arrived(inbox_sum.at[k], recv_sum.at[k])
    for seg in range(segs):
        told = [inbox_sum[fi * segs + seg] for fi in range(fibres)]
        spans = jnp.concatenate([part[1:3] for part in told], axis=0)
        stage_total[seg] = jnp.concatenate(
            [
                sum(part[0:1] for part in told),
                jnp.sum(spans, axis=0, keepdims=True),
                spans,
                jnp.zeros((2 * bands - 2 - 2 * fibres, width), full),
            ],
            axis=0,
        )
    sends.append(push(stage_total, inbox_total, total_sem.at[0], total_sem.at[1], partner))
    arrived(inbox_total, total_sem.at[1])
    for seg in range(segs):
        total = jnp.concatenate([stage_total[seg], inbox_total[seg]], axis=0)
        columns[pl.ds(seg * blocks, blocks)] = total.T.reshape(blocks, BLOCK, 4 * bands)
    loads[4].wait()
    loads[5].wait()
    ends = columns[pairs[0, band * recs + r]] * columns[pairs[1, band * recs + r]] * (1.0 / (2.0 * F**0.5))
    kind = lax.broadcasted_iota(jnp.int32, ends.shape, 1) % (2 * bands)
    flat = jnp.sum(jnp.where(kind == 0, ends * (1.0 / S), 0.0), axis=1, keepdims=True)
    turned = jnp.where(kind == 1, ends * (-1.0 / S), ends * (1.0 / span))
    turned = jnp.sum(jnp.where(kind == 0, 0.0, turned), axis=1, keepdims=True)
    even = lax.broadcasted_iota(jnp.int32, (BLOCK, LAGS), 1) % 2 == reach % 2
    offset = flat + jnp.where(even, turned, -turned)
    for d in range(1, bands):
        k = flipped(band, d)
        arrived(inbox3.at[k], recv3.at[k])
    synthetic = offset + inbox3[0].astype(full)
    for k in range(1, bands):
        synthetic += inbox3[k].astype(full)
    window = mask[pl.ds(r, 1), :].astype(full)
    inbox4[r, band] = (window * jnp.tanh(synthetic - observed[...])).astype(low)
    own = inbox4.at[r, band]
    spread4 = [
        remote(own, own, send4.at[j], recv4.at[band], at(j // segs, j % segs, r)) for j in range(bands)
    ]
    for j in range(bands):

        @pl.when(band != j)
        def _():
            spread4[j].start()

    sends.append(push(own, own, relay_send.at[0], relay_recv.at[band], partner))

    for si in range(segs):

        @pl.when(s == 1 - si)
        def _():
            arrived(ext.at[si, pl.ds(reach + span * si, reach + (span - reach) * si)], recv1.at[2])

    @pl.when(s == 1)
    def _():
        arrived(ext.at[0, edges[0]], recv1.at[6])

    arrived(ext.at[o, edges[1]], recv1.at[7])
    head = lax.broadcasted_iota(jnp.int32, (1, half), 1) == 0
    for seg in range(segs):
        total = stage_total[seg].T * (n / S)
        for w in range(segs):
            value = dot(ext[seg, pl.ds(span * w, n)], whole[...], 0, 0)
            value = jnp.concatenate(
                [
                    value[:, :half] + jnp.where(head, total[:, 0:1], 0.0),
                    value[:, half:] - jnp.where(head, total[:, 1:2], 0.0),
                ],
                axis=1,
            )
            put(full_spec.at[w], seg, value)
    loads[6].wait()

    def gradients(p):
        h, side = groups[p]
        spread = dot(inbox4[h, pl.ds(side * cut, cut)].reshape(cut * BLOCK, LAGS), taps[...])
        for i in range(cut):
            pair = (side * cut + i) * recs + h
            filters = spread[i * BLOCK : (i + 1) * BLOCK]
            filters = filters[:, :half], filters[:, half:]
            base = p * group + i * BLOCK
            for w in range(segs):
                first = block(full_spec.at[w], pairs[0, pair])
                second = block(full_spec.at[w], pairs[1, pair])
                for start, parts in (
                    (base, spectral_product([(filters, second)], -1.0)),
                    (base + cut * BLOCK, spectral_product([(first, filters)], 1.0)),
                ):
                    for q in range(2):
                        grads[w, pl.ds(start, BLOCK), pl.ds(q * half, half)] = parts[q].astype(low)

    for d in range(1, bands):
        k = flipped(band, d)
        arrived(inbox4.at[r, k], recv4.at[k])
        got = inbox4.at[r, k]
        sends.append(push(got, got, relay_send.at[d], relay_recv.at[k], partner))
    for p, (first, stop) in enumerate(((0, 0), (0, 0), (0, cut), (cut, bands))):
        for d in range(first, stop):
            k = flipped(band, d)
            arrived(inbox4.at[1 - r, k], relay_recv.at[k])
        gradients(p)
    loads[7].wait()

    for w in range(segs):
        summed = dot(select[...], grads[w]).astype(low)
        out[pl.ds(span * w, span), :] = dot(back[...], summed, 1, 1).astype(low)
    for si in range(segs):

        @pl.when(s == si)
        def _():
            for copy in needed[si] + [later[si]] + passed[si:]:
                copy.wait_send()

    @pl.when(s == 1)
    def _():
        up_across.wait_send()

    for copy in sends:
        copy.wait_send()
    for j in range(bands):

        @pl.when(band != j)
        def _():
            spread3[j].wait_send()
            spread4[j].wait_send()

    for (fi, si), copy in zip(places, sum_sends):

        @pl.when(fi != f)
        def _():
            copy.wait_send()


def fused_on_device(mesh_shape, tables, records, pairs, observed, lag_mask):
    fibres, segs, recs = (mesh_shape[name] for name in ("fibre", "seg", "rec"))
    bands = fibres * segs
    _, extent, width = records.shape
    span, reach = S // bands, LAGS // 2
    n = span + LAGS
    count = pairs.shape[0] * BLOCK
    own = count // recs
    total = segs * width
    low, full = jnp.bfloat16, jnp.float32
    vmem = pl.BlockSpec(memory_space=pltpu.VMEM)
    hbm = pl.BlockSpec(memory_space=pltpu.HBM)
    corr = (BLOCK, LAGS)
    spec = (total // BLOCK, BLOCK, n)

    def sems(*sizes):
        return [pltpu.SemaphoreType.DMA((size,)) for size in sizes]

    result = pl.pallas_call(
        functools.partial(fused_kernel, (fibres, segs, recs)),
        out_shape=pltpu.VMEM((extent, width), low),
        in_specs=[hbm] * 8,
        out_specs=vmem,
        scratch_shapes=[
            pltpu.SMEM((2, pairs.shape[0]), jnp.int32),
            pltpu.VMEM((segs, 2 * span + 2 * reach, width), low),
            pltpu.VMEM(corr, full),
            pltpu.VMEM(lag_mask.shape, jnp.int32),
            pltpu.VMEM((n, n), low),
            pltpu.VMEM((2 * n, LAGS), low),
            pltpu.VMEM((LAGS, n), low),
            pltpu.VMEM((span, n), low),
            pltpu.VMEM((bands, 4, width), full),
            pltpu.VMEM((segs, 2 * bands, width), full),
            pltpu.VMEM((segs, 2 * bands, width), full),
            pltpu.VMEM((total // BLOCK, BLOCK, 4 * bands), full),
            pltpu.VMEM(spec, full),
            pltpu.VMEM(spec, full),
            pltpu.VMEM(spec, full),
            pltpu.VMEM((segs,) + spec, low),
            pltpu.VMEM((width, 2 * count), low),
            pltpu.VMEM((2 * recs, own // 2, 2 * n), low),
            pltpu.VMEM((2, own // 2, LAGS), low),
            pltpu.VMEM((2, own // 2, LAGS), low),
            pltpu.VMEM((bands,) + corr, low),
            pltpu.VMEM((bands,) + corr, low),
            pltpu.VMEM((recs, bands) + corr, low),
            pltpu.VMEM((segs, 2 * count, n), low),
            pltpu.SemaphoreType.REGULAR,
            pltpu.SemaphoreType.REGULAR,
            *sems(8, 8, 8, bands + 1, bands, 2, 2, 2, bands, bands, bands, bands, bands, bands),
        ],
        compiler_params=pltpu.CompilerParams(
            has_side_effects=True, collective_id=0, vmem_limit_bytes=VMEM_GRANT
        ),
        name="adjoint",
    )(records[0], pairs.T, observed, lag_mask, *tables)
    return result[None]


def fits_fused(shape, records, pairs):
    fibres, segs, recs = (shape[name] for name in ("fibre", "seg", "rec"))
    bands = fibres * segs
    width = records.shape[2] // (shape["groups"] * segs)
    return (
        fibres > 1
        and fibres & (fibres - 1) == 0
        and segs == 2
        and recs == 2
        and width % 128 == 0
        and width * segs <= 512
        and S // bands >= LAGS
        and pairs.shape[0] == bands * recs
    )


def solution(mesh):
    in_specs = (
        P("rec", "fibre", ("groups", "seg")),
        P(),
        P(("groups", "fibre", "seg"), None, None),
        P(("groups", "fibre", "seg"), None),
    )
    out_specs = P("rec", "fibre", ("groups", "seg"))
    shape = dict(mesh.shape)

    def run(records, pairs, observed, lag_mask):
        args = (records, pairs, observed, lag_mask)
        if not fits_fused(shape, records, pairs):
            return jax.shard_map(
                on_device, mesh=mesh, in_specs=in_specs, out_specs=out_specs, check_vma=False
            )(*args)
        tables = [jnp.asarray(t) for t in window_tables(shape["fibre"] * shape["seg"])]

        def body(*blocks):
            return fused_on_device(shape, tables, *blocks)

        return jax.shard_map(
            body, mesh=mesh, in_specs=in_specs, out_specs=out_specs, check_vma=False
        )(*args)

    return run
```

```python
import functools

import jax
import jax.numpy as jnp
import numpy as np
from jax import lax
from jax.experimental import pallas as pl
from jax.experimental.pallas import tpu as pltpu
from jax.sharding import PartitionSpec as P

S = 2048
F = 1024
LAGS = 256
BLOCK = 32
CH_DEV = 64
VMEM_GRANT = 60899328


def forward_table():
    freq_index = jnp.arange(F, dtype=jnp.int32)
    time_index = jnp.arange(S, dtype=jnp.int32)
    phase = freq_index[:, None] * time_index[None, :] % S
    angles = phase.astype(jnp.float32) * (2.0 * jnp.pi / S)
    scale = 1.0 / jnp.sqrt(jnp.float32(S))
    return jnp.stack(
        [
            (jnp.cos(angles) * scale).astype(jnp.bfloat16),
            (-jnp.sin(angles) * scale).astype(jnp.bfloat16),
        ],
        axis=1,
    )


def lag_table():
    freq_index = jnp.arange(F, dtype=jnp.int32)
    shifts = (jnp.arange(LAGS, dtype=jnp.int32) - LAGS // 2) % S
    phase = freq_index[:, None] * shifts[None, :] % S
    angles = phase.astype(jnp.float32) * (2.0 * jnp.pi / S)
    scale = 1.0 / jnp.sqrt(jnp.float32(F))
    return jnp.stack(
        [
            (jnp.cos(angles) * scale).astype(jnp.bfloat16),
            (-jnp.sin(angles) * scale).astype(jnp.bfloat16),
        ],
        axis=1,
    )


def synthesize(incoming, table):
    count = incoming.shape[-1]
    flat = incoming.reshape(2 * F, count)
    result = jnp.einsum(
        "qn,qt->tn", flat, table.reshape(2 * F, S), preferred_element_type=jnp.float32
    )
    return result.astype(jnp.bfloat16)


def on_device(records, pairs, observed, lag_mask):
    fibre_count = lax.axis_size("fibre")
    seg_count = lax.axis_size("seg")
    spread_count = fibre_count * seg_count
    freq_dev = F // spread_count
    blocks_dev = CH_DEV // BLOCK
    block_count = CH_DEV * spread_count // BLOCK
    pair_total = pairs.shape[0]
    pairs_dev = pair_total // spread_count
    table = forward_table()
    lags = lag_table()
    spans = records.reshape(1, S // fibre_count, fibre_count, CH_DEV)
    incoming = lax.all_to_all(spans, "fibre", split_axis=2, concat_axis=1, tiled=True)
    count = incoming.shape[3]
    signal = incoming.reshape(S, count)
    result = jnp.einsum(
        "qs,sn->qn", table.reshape(2 * F, S), signal, preferred_element_type=jnp.float32
    )
    spectra = result.reshape(F, 2, count).astype(jnp.bfloat16)
    widened = lax.all_to_all(spectra, ("fibre", "seg"), split_axis=0, concat_axis=2, tiled=True)
    seg_blocks = fibre_count * blocks_dev
    slot_ids = (
        pairs % seg_blocks // blocks_dev * seg_count + pairs // seg_blocks
    ) * blocks_dev + pairs % blocks_dev
    blocks_grid = widened.reshape(freq_dev, 2, block_count, BLOCK)
    first_side = jnp.take(blocks_grid, slot_ids[:, 0], axis=2).astype(jnp.float32)
    second_side = jnp.take(blocks_grid, slot_ids[:, 1], axis=2).astype(jnp.float32)
    first_re, first_im = (first_side[:, 0], first_side[:, 1])
    second_re, second_im = (second_side[:, 0], second_side[:, 1])
    cross_re = first_re * second_re + first_im * second_im
    cross_im = first_im * second_re - first_re * second_im
    cross_spec = jnp.stack([cross_re, cross_im], axis=1).astype(jnp.bfloat16)
    cross_spec = cross_spec.reshape(freq_dev, 2, spread_count, pairs_dev * BLOCK)
    owned_spec = lax.all_to_all(
        cross_spec, ("fibre", "seg"), split_axis=2, concat_axis=0, tiled=True
    )
    owned_spec = owned_spec.reshape(F, 2, pairs_dev * BLOCK)
    partial_corr = jnp.einsum("wpx,wpl->xl", owned_spec, lags, preferred_element_type=jnp.float32)
    synthetic = (
        lax.psum(partial_corr.astype(jnp.bfloat16), "rec")
        .astype(jnp.float32)
        .reshape(pairs_dev, BLOCK, LAGS)
    )
    weights = lag_mask[:, None, :].astype(jnp.float32) * jnp.tanh(synthetic - observed)
    weights_low = weights.astype(jnp.bfloat16).reshape(pairs_dev * BLOCK, LAGS)
    adjoint_spec = jnp.einsum("xl,wpl->wpx", weights_low, lags, preferred_element_type=jnp.float32)
    adjoint_spec = adjoint_spec.astype(jnp.bfloat16).reshape(F, 2, 1, pairs_dev * BLOCK)
    returned = lax.all_to_all(
        adjoint_spec, ("fibre", "seg"), split_axis=0, concat_axis=2, tiled=True
    )
    returned = returned.reshape(freq_dev, 2, pair_total, BLOCK).astype(jnp.float32)
    adjoint_re, adjoint_im = (returned[:, 0], returned[:, 1])
    grad_first = jnp.stack(
        [
            adjoint_re * second_re - adjoint_im * second_im,
            adjoint_re * second_im + adjoint_im * second_re,
        ],
        axis=1,
    )
    grad_second = jnp.stack(
        [
            adjoint_re * first_re + adjoint_im * first_im,
            adjoint_re * first_im - adjoint_im * first_re,
        ],
        axis=1,
    )
    contributions = jnp.concatenate([grad_first, grad_second], axis=2)
    endpoint_ids = jnp.concatenate([slot_ids[:, 0], slot_ids[:, 1]])
    summed = jax.ops.segment_sum(
        jnp.moveaxis(contributions, 2, 0), endpoint_ids, num_segments=block_count
    )
    block_adjoint = jnp.moveaxis(summed, 0, 2).astype(jnp.bfloat16)
    outgoing = block_adjoint.reshape(freq_dev, 2, spread_count, CH_DEV)
    sources = synthesize(
        lax.all_to_all(outgoing, ("fibre", "seg"), split_axis=2, concat_axis=0, tiled=True), table
    )
    regrouped = lax.all_to_all(sources, "fibre", split_axis=0, concat_axis=1, tiled=True)
    return regrouped[None]


def window_tables(bands):
    span, reach, n = S // bands, LAGS // 2, S // bands + LAGS
    half = n // 2
    freqs, places = np.arange(half), np.arange(n)
    shifts = np.arange(LAGS) - reach
    ends = np.where(freqs == 0, 1.0, 2.0) / (n * 2.0 * np.sqrt(F))

    def table(times, scale):
        angles = (freqs[None, :] * times[:, None] % n) * (2.0 * np.pi / n)
        real, imag = np.cos(angles), -np.sin(angles)
        imag[:, 0] = np.where(times % 2 == 0, 1.0, -1.0)
        return np.concatenate([real * scale, imag * scale], axis=1)

    whole = table(places, np.ones(half))
    lags = table(shifts, ends).T
    taps = table(shifts, np.ones(half))
    back = table(places[reach : reach + span], ends)
    lags = np.concatenate([lags, lags])
    return [t.astype(np.float32).astype(jnp.bfloat16) for t in (whole, lags, taps, back)]


def dot(left, right, left_dim=1, right_dim=0):
    return lax.dot_general(
        left,
        right,
        (((left_dim,), (right_dim,)), ((), ())),
        preferred_element_type=jnp.float32,
    )


def spectral_product(terms, sign, extra=None):
    both = sum(p1 * q1 for (_, p1), (_, q1) in terms)
    real = sum(p0 * q0 for (p0, _), (q0, _) in terms)
    imag = sum(p1 * q0 - sign * (p0 * q1) for (p0, p1), (q0, q1) in terms)
    whole = real + sign * both
    ends = lax.broadcasted_iota(jnp.int32, (both.shape[0], 128), 1) == 0
    return tuple(
        jnp.concatenate([jnp.where(ends, end, value[:, :128]), value[:, 128:]], axis=1)
        for end, value in ((real[:, :128], whole), (both[:, :128] if extra is None else both[:, :128] + extra, imag))
    )


def fused_kernel(
    sizes, x_hbm, pairs_hbm, observed_hbm, mask_hbm, whole_hbm, lags_hbm, taps_hbm, back_hbm,
    out, pairs, ext, observed, mask, whole, lags, taps, back,
    inbox_sum, stage_total, inbox_total, columns, core_spec, both_spec, left_spec,
    full_spec, select, cross, stage_core, inbox_core, stage3, inbox3, inbox4, grads, held,
    following, high, load_sem, send1, recv1, send_sum, recv_sum, total_sem, core_send, core_recv,
    relay_send, relay_recv, send3, recv3, send4, recv4,
):
    fibres, segs, recs = sizes
    bands = fibres * segs
    last = fibres - 1
    g, f, s, r = (lax.axis_index(name) for name in ("groups", "fibre", "seg", "rec"))
    o = 1 - s
    band = f * segs + s
    span, reach, width = S // bands, LAGS // 2, x_hbm.shape[1]
    n = span + LAGS
    half = n // 2
    blocks = width // BLOCK
    count = pairs.shape[1] * BLOCK
    low, full = jnp.bfloat16, jnp.float32

    def at(fibre, seg, rec):
        return (g, fibre, seg, rec)

    def at_band(index):
        return at(index // segs, index % segs, r)

    def remote(src, dst, send, recv, device):
        return pltpu.make_async_remote_copy(
            src_ref=src, dst_ref=dst, send_sem=send, recv_sem=recv,
            device_id=device, device_id_type=pl.DeviceIdType.MESH,
        )

    def push(src, dst, send, recv, device):
        copy = remote(src, dst, send, recv, device)
        copy.start()
        return copy

    def arrived(dst, recv):
        remote(dst, dst, recv, recv, at(f, s, 1 - r)).wait_recv()

    def signal(sem, device):
        pl.semaphore_signal(sem, inc=1, device_id=device, device_id_type=pl.DeviceIdType.MESH)

    def rows(start, size, unit):
        return pl.ds(pl.multiple_of(start, unit), size)

    def flipped(index, bits):
        result, bit = 0, 1
        while bit < bands:
            digit = index // bit % 2
            result += bit * (1 - digit if bits // bit % 2 else digit)
            bit *= 2
        return result

    partner = at(f, s, 1 - r)
    across = at(f, o, r)
    places = [(fi, si) for fi in range(fibres) for si in range(segs)]

    barrier = pltpu.get_barrier_semaphore()
    signal(barrier, partner)
    signal(barrier, across)
    for fi, si in places:

        @pl.when(fi > f)
        def _():
            signal(barrier, at(fi, si, r))

    loads = [
        pltpu.make_async_copy(src, dst, load_sem.at[i])
        for i, (src, dst) in enumerate(
            [
                (x_hbm, ext.at[s, pl.ds(reach, 2 * span)]), (pairs_hbm, pairs), (whole_hbm, whole), (lags_hbm, lags),
                (observed_hbm.at[r], observed), (mask_hbm, mask), (taps_hbm, taps), (back_hbm, back),
            ]
        )
    ]
    for load in loads:
        load.start()

    def give(first, size, place, send, recv, device):
        return remote(
            x_hbm.at[pl.ds(first, size)], ext.at[s, pl.ds(place, size)], send1.at[send], recv1.at[recv], device
        )

    needed = [
        [give(span, span, span + reach, 0, 0, across), give(reach, reach, 2 * reach, 1, 1, across)],
        [give(0, span, reach, 0, 0, across)],
    ]
    later = [give(0, reach, reach, 2, 2, across), give(span, span, reach + span, 2, 2, across)]
    upper, lower = (f + 1) % fibres, (f + last) % fibres
    up = give(2 * span - reach, reach, 0, 3, 3, at(upper, s, r))
    up_across = give(2 * span - reach, reach, 0, 4, 4, at(upper, 0, r))
    down = give(0, reach, reach + 2 * span, 5, 5, at(lower, s, r))
    edges = [pl.ds(0, reach), pl.ds(reach + 2 * span, reach)]
    passed = [
        remote(ext.at[s, edge], ext.at[s, edge], send1.at[6 + i], recv1.at[6 + i], across)
        for i, edge in enumerate(edges)
    ]

    def send_up():
        @pl.when(s == 0)
        def _():
            up.start()

        @pl.when(s == 1)
        def _():
            up_across.start()

    pl.semaphore_wait(barrier, segs * (f + 1))
    for si in range(segs):

        @pl.when(s == si)
        def _():
            for copy in needed[si]:
                copy.start()

    @pl.when(f == last)
    def _():
        send_up()

    for fi, si in places:

        @pl.when(fi == f - 1)
        def _():
            signal(following, at(fi, si, r))

        @pl.when(fi < f - 1)
        def _():
            signal(high, at(fi, si, r))

    loads[0].wait()
    folded = [
        ext[s, pl.ds(reach + span * w, span)].astype(full).reshape(-1, 8, width).sum(axis=0) for w in range(segs)
    ]
    odd = lax.broadcasted_iota(jnp.int32, (8, width), 0) % 2 == 1
    flat = jnp.sum(folded[0] + folded[1], axis=0, keepdims=True)
    turned = [jnp.sum(jnp.where(odd, -part, part), axis=0, keepdims=True) for part in folded]
    inbox_sum[band] = jnp.concatenate([flat] + turned + [jnp.zeros_like(flat)], axis=0)
    sends = [up, down]
    own_sum = inbox_sum.at[band]
    sum_sends = [
        remote(own_sum, own_sum, send_sum.at[fi * segs + si], recv_sum.at[band], at(fi, si, r)) for fi, si in places
    ]
    across_sum = push(own_sum, own_sum, send_sum.at[bands], recv_sum.at[band], across)
    sends.append(across_sum)
    for (fi, si), copy in zip(places, sum_sends):

        @pl.when(fi < f)
        def _():
            copy.start()

    loads[1].wait()
    cut = bands // 2
    others = [flipped(band, k * segs) // segs for k in range(1, fibres)]
    entries = [(r, f), (1 - r, f)] + [(r, fibre) for fibre in others] + [(1 - r, fibre) for fibre in others]
    group = 2 * segs * BLOCK
    lane = lax.broadcasted_iota(jnp.int32, (1, 2 * count), 1)
    target = lane
    for p, (h, fibre) in enumerate(entries):
        for end in range(2):
            for i in range(segs):
                first = p * group + (end * segs + i) * BLOCK
                inside = (lane >= first) & (lane < first + BLOCK)
                target = jnp.where(inside, lane + (pairs[end, (fibre * segs + i) * recs + h] * BLOCK - first), target)
    line = lax.broadcasted_iota(jnp.int32, select.shape, 0) + s * width
    select[...] = jnp.where(line == target, 1.0, 0.0).astype(low)

    def put(spec, seg, value):
        spec[rows(seg * blocks, blocks, blocks)] = value.astype(spec.dtype).reshape(blocks, BLOCK, n)

    def core_part(seg):
        part = dot(ext[seg, rows(reach + span * s, span, reach)], whole[reach : reach + span], 0, 0)
        put(core_spec, seg, part)

    def left_part(seg):
        part = dot(ext[seg, rows(span * s, reach, reach)], whole[:reach], 0, 0)
        put(left_spec, seg, part)
        put(both_spec, seg, part + core_spec[rows(seg * blocks, blocks, blocks)].reshape(width, n))

    loads[2].wait()
    core_part(s)

    @pl.when(f < last)
    def _():
        pl.semaphore_wait(following, segs)
        send_up()

    for si in range(segs):

        @pl.when(s == 1 - si)
        def _():
            arrived(ext.at[si, pl.ds(reach + span * (1 - si), span)], recv1.at[0])

    core_part(o)

    @pl.when(f < last - 1)
    def _():
        pl.semaphore_wait(high, segs * (last - 1 - f))

    for (fi, si), copy in zip(places, sum_sends):

        @pl.when(fi > f)
        def _():
            copy.start()

    @pl.when(s == 1)
    def _():
        up.start()

    down.start()

    def send_later():
        for si in range(segs):

            @pl.when(s == si)
            def _():
                later[si].start()

    pl.when(f == 0)(send_later)

    @pl.when(s == 0)
    def _():
        arrived(ext.at[0, edges[0]], recv1.at[3])

    left_part(s)

    @pl.when(s == 0)
    def _():
        arrived(ext.at[1, edges[0]], recv1.at[4])

    @pl.when(s == 1)
    def _():
        arrived(ext.at[0, pl.ds(2 * reach, reach)], recv1.at[1])

    pl.when(f > 0)(send_later)
    left_part(o)

    def block(spec, index):
        value = spec[index].astype(full)
        return value[:, :half], value[:, half:]

    ordered = sorted(range(bands), key=lambda j: (-abs(2 * (j // segs) - last), -j))
    chunks = ordered[:cut], ordered[cut:]

    def correlate(place, h, chunk):
        for i, j in enumerate(chunk):
            pair = j * recs + h
            one, two = pairs[0, pair], pairs[1, pair]
            terms = [(block(core_spec, one), block(both_spec, two)), (block(left_spec, one), block(core_spec, two))]
            inner = terms[0][0][1][:, :128] * terms[1][1][1][:, :128]
            parts = spectral_product(terms, 1.0, inner * (-n / span))
            for q, part in enumerate(parts):
                high_part = part.astype(low)
                here = pl.ds(i * BLOCK, BLOCK)
                cross[place, here, pl.ds(q * half, half)] = high_part
                cross[place, here, pl.ds(n + q * half, half)] = (part - high_part.astype(full)).astype(low)
        return dot(cross[place], lags[...])

    loads[3].wait()
    for i, chunk in enumerate(chunks):
        stage_core[i] = correlate(i, 1 - r, chunk).astype(low)
        sends.append(push(stage_core.at[i], inbox_core.at[i], core_send.at[i], core_recv.at[i], partner))

    spread3 = [
        remote(stage3.at[j], inbox3.at[band], send3.at[j], recv3.at[band], at(j // segs, j % segs, r))
        for j in range(bands)
    ]
    for i, chunk in enumerate(chunks):
        partial = correlate(2 + i, r, chunk)
        arrived(inbox_core.at[i], core_recv.at[i])
        partial = (partial + inbox_core[i].astype(full)).astype(low)
        for place, j in enumerate(chunk):
            stage3[j] = partial[place * BLOCK : (place + 1) * BLOCK]

            @pl.when(band != j)
            def _():
                spread3[j].start()

    inbox3[band] = stage3[band]

    @pl.when(s == 0)
    def _():
        passed[0].start()

    @pl.when(s == 1)
    def _():
        arrived(ext.at[1, edges[0]], recv1.at[3])

    arrived(ext.at[s, edges[1]], recv1.at[5])
    passed[1].start()

    for d in range(1, bands):
        k = flipped(band, d)
        arrived(inbox_sum.at[k], recv_sum.at[k])
    for seg in range(segs):
        told = [inbox_sum[fi * segs + seg] for fi in range(fibres)]
        spans = jnp.concatenate([part[1:3] for part in told], axis=0)
        stage_total[seg] = jnp.concatenate(
            [
                sum(part[0:1] for part in told),
                jnp.sum(spans, axis=0, keepdims=True),
                spans,
                jnp.zeros((2 * bands - 2 - 2 * fibres, width), full),
            ],
            axis=0,
        )
    sends.append(push(stage_total, inbox_total, total_sem.at[0], total_sem.at[1], partner))
    arrived(inbox_total, total_sem.at[1])
    for seg in range(segs):
        total = jnp.concatenate([stage_total[seg], inbox_total[seg]], axis=0)
        columns[pl.ds(seg * blocks, blocks)] = total.T.reshape(blocks, BLOCK, 4 * bands)
    loads[4].wait()
    loads[5].wait()
    ends = columns[pairs[0, band * recs + r]] * columns[pairs[1, band * recs + r]] * (1.0 / (2.0 * F**0.5))
    kind = lax.broadcasted_iota(jnp.int32, ends.shape, 1) % (2 * bands)
    flat = jnp.sum(jnp.where(kind == 0, ends * (1.0 / S), 0.0), axis=1, keepdims=True)
    turned = jnp.where(kind == 1, ends * (-1.0 / S), ends * (1.0 / span))
    turned = jnp.sum(jnp.where(kind == 0, 0.0, turned), axis=1, keepdims=True)
    even = lax.broadcasted_iota(jnp.int32, (BLOCK, LAGS), 1) % 2 == reach % 2
    offset = flat + jnp.where(even, turned, -turned)
    for d in range(1, bands):
        k = flipped(band, d)
        arrived(inbox3.at[k], recv3.at[k])
    synthetic = offset + inbox3[0].astype(full)
    for k in range(1, bands):
        synthetic += inbox3[k].astype(full)
    window = mask[pl.ds(r, 1), :].astype(full)
    inbox4[r, band] = (window * jnp.tanh(synthetic - observed[...])).astype(low)
    own = inbox4.at[r, band]
    spread4 = [
        remote(own, own, send4.at[j], recv4.at[band], at(j // segs, j % segs, r)) for j in range(bands)
    ]
    for j in range(bands):

        @pl.when(band != j)
        def _():
            spread4[j].start()

    sends.append(push(own, own, relay_send.at[0], relay_recv.at[band], partner))

    for si in range(segs):

        @pl.when(s == 1 - si)
        def _():
            arrived(ext.at[si, pl.ds(reach + span * si, reach + (span - reach) * si)], recv1.at[2])

    @pl.when(s == 1)
    def _():
        arrived(ext.at[0, edges[0]], recv1.at[6])

    arrived(ext.at[o, edges[1]], recv1.at[7])
    head = lax.broadcasted_iota(jnp.int32, (1, half), 1) == 0
    for seg in range(segs):
        total = stage_total[seg].T * (n / S)
        for w in range(segs):
            value = dot(ext[seg, pl.ds(span * w, n)], whole[...], 0, 0)
            value = jnp.concatenate(
                [
                    value[:, :half] + jnp.where(head, total[:, 0:1], 0.0),
                    value[:, half:] - jnp.where(head, total[:, 1:2], 0.0),
                ],
                axis=1,
            )
            put(full_spec.at[w], seg, value)
    loads[6].wait()

    def gradients(first, stop):
        given = [inbox4[h, pl.ds(fibre * segs, segs)].reshape(segs * BLOCK, LAGS) for h, fibre in entries[first:stop]]
        spread = dot(jnp.concatenate(given, axis=0), taps[...])
        for p in range(first, stop):
            h, fibre = entries[p]
            for i in range(segs):
                pair = (fibre * segs + i) * recs + h
                start = ((p - first) * segs + i) * BLOCK
                filters = spread[start : start + BLOCK]
                filters = filters[:, :half], filters[:, half:]
                base = p * group + i * BLOCK
                for w in range(segs):
                    one = block(full_spec.at[w], pairs[0, pair])
                    two = block(full_spec.at[w], pairs[1, pair])
                    for place, parts in (
                        (base, spectral_product([(filters, two)], -1.0)),
                        (base + segs * BLOCK, spectral_product([(one, filters)], 1.0)),
                    ):
                        for q in range(2):
                            grads[w, pl.ds(place, BLOCK), pl.ds(q * half, half)] = parts[q].astype(low)

    turns = [flipped(band, d) for d in range(bands)]
    relays = [
        remote(inbox4.at[r, k], inbox4.at[r, k], relay_send.at[d], relay_recv.at[k], partner)
        for d, k in enumerate(turns)
    ]
    sends += relays[1:]

    def take(d):
        arrived(inbox4.at[r, turns[d]], recv4.at[turns[d]])
        relays[d].start()

    def relayed(d):
        arrived(inbox4.at[1 - r, turns[d]], relay_recv.at[turns[d]])

    def fibre_first():
        for d in range(segs):
            relayed(d)
        gradients(0, recs)

    def gather(first, stop):
        cut_at = slice(first * group, stop * group)
        return [dot(select[:, cut_at], grads[w, cut_at]) for w in range(segs)]

    direct = recs + fibres - 1
    for d in range(1, segs):
        take(d)

    @pl.when(r == 0)
    def _():
        fibre_first()
        for w, part in enumerate(gather(0, recs)):
            held[w] = part

    for d in range(segs, bands):
        take(d)

    @pl.when(r == 1)
    def _():
        fibre_first()
        gradients(recs, direct)
        for w, part in enumerate(gather(0, direct)):
            held[w] = part

    @pl.when(r == 0)
    def _():
        gradients(recs, direct)

    for d in range(segs, bands):
        relayed(d)
    gradients(direct, recs * fibres)
    loads[7].wait()

    for core, first in enumerate((recs, direct)):

        @pl.when(r == core)
        def _():
            for w, part in enumerate(gather(first, recs * fibres)):
                summed = (held[w] + part).astype(low)
                out[pl.ds(span * w, span), :] = dot(back[...], summed, 1, 1).astype(low)

    for si in range(segs):

        @pl.when(s == si)
        def _():
            for copy in needed[si] + [later[si]] + passed[si:]:
                copy.wait_send()

    @pl.when(s == 1)
    def _():
        up_across.wait_send()

    for copy in sends:
        copy.wait_send()
    for j in range(bands):

        @pl.when(band != j)
        def _():
            spread3[j].wait_send()
            spread4[j].wait_send()

    for (fi, si), copy in zip(places, sum_sends):

        @pl.when(fi != f)
        def _():
            copy.wait_send()


def fused_on_device(mesh_shape, tables, records, pairs, observed, lag_mask):
    fibres, segs, recs = (mesh_shape[name] for name in ("fibre", "seg", "rec"))
    bands = fibres * segs
    _, extent, width = records.shape
    span, reach = S // bands, LAGS // 2
    n = span + LAGS
    count = pairs.shape[0] * BLOCK
    own = count // recs
    total = segs * width
    low, full = jnp.bfloat16, jnp.float32
    vmem = pl.BlockSpec(memory_space=pltpu.VMEM)
    hbm = pl.BlockSpec(memory_space=pltpu.HBM)
    corr = (BLOCK, LAGS)
    spec = (total // BLOCK, BLOCK, n)

    def sems(*sizes):
        return [pltpu.SemaphoreType.DMA((size,)) for size in sizes]

    result = pl.pallas_call(
        functools.partial(fused_kernel, (fibres, segs, recs)),
        out_shape=pltpu.VMEM((extent, width), low),
        in_specs=[hbm] * 8,
        out_specs=vmem,
        scratch_shapes=[
            pltpu.SMEM((2, pairs.shape[0]), jnp.int32),
            pltpu.VMEM((segs, 2 * span + 2 * reach, width), low),
            pltpu.VMEM(corr, full),
            pltpu.VMEM(lag_mask.shape, jnp.int32),
            pltpu.VMEM((n, n), low),
            pltpu.VMEM((2 * n, LAGS), low),
            pltpu.VMEM((LAGS, n), low),
            pltpu.VMEM((span, n), low),
            pltpu.VMEM((bands, 4, width), full),
            pltpu.VMEM((segs, 2 * bands, width), full),
            pltpu.VMEM((segs, 2 * bands, width), full),
            pltpu.VMEM((total // BLOCK, BLOCK, 4 * bands), full),
            pltpu.VMEM(spec, full),
            pltpu.VMEM(spec, full),
            pltpu.VMEM(spec, full),
            pltpu.VMEM((segs,) + spec, low),
            pltpu.VMEM((width, 2 * count), low),
            pltpu.VMEM((2 * recs, own // 2, 2 * n), low),
            pltpu.VMEM((2, own // 2, LAGS), low),
            pltpu.VMEM((2, own // 2, LAGS), low),
            pltpu.VMEM((bands,) + corr, low),
            pltpu.VMEM((bands,) + corr, low),
            pltpu.VMEM((recs, bands) + corr, low),
            pltpu.VMEM((segs, 2 * count, n), low),
            pltpu.VMEM((segs, width, n), full),
            pltpu.SemaphoreType.REGULAR,
            pltpu.SemaphoreType.REGULAR,
            *sems(8, 8, 8, bands + 1, bands, 2, 2, 2, bands, bands, bands, bands, bands, bands),
        ],
        compiler_params=pltpu.CompilerParams(
            has_side_effects=True, collective_id=0, vmem_limit_bytes=VMEM_GRANT
        ),
        name="adjoint",
    )(records[0], pairs.T, observed, lag_mask, *tables)
    return result[None]


def fits_fused(shape, records, pairs):
    fibres, segs, recs = (shape[name] for name in ("fibre", "seg", "rec"))
    bands = fibres * segs
    width = records.shape[2] // (shape["groups"] * segs)
    return (
        fibres > 1
        and fibres & (fibres - 1) == 0
        and segs == 2
        and recs == 2
        and width % 128 == 0
        and width * segs <= 512
        and S // bands >= LAGS
        and pairs.shape[0] == bands * recs
    )


def solution(mesh):
    in_specs = (
        P("rec", "fibre", ("groups", "seg")),
        P(),
        P(("groups", "fibre", "seg"), None, None),
        P(("groups", "fibre", "seg"), None),
    )
    out_specs = P("rec", "fibre", ("groups", "seg"))
    shape = dict(mesh.shape)

    def run(records, pairs, observed, lag_mask):
        args = (records, pairs, observed, lag_mask)
        if not fits_fused(shape, records, pairs):
            return jax.shard_map(
                on_device, mesh=mesh, in_specs=in_specs, out_specs=out_specs, check_vma=False
            )(*args)
        tables = [jnp.asarray(t) for t in window_tables(shape["fibre"] * shape["seg"])]

        def body(*blocks):
            return fused_on_device(shape, tables, *blocks)

        return jax.shard_map(
            body, mesh=mesh, in_specs=in_specs, out_specs=out_specs, check_vma=False
        )(*args)

    return run
```

```python
import functools

import jax
import jax.numpy as jnp
import numpy as np
from jax import lax
from jax.experimental import pallas as pl
from jax.experimental.pallas import tpu as pltpu
from jax.sharding import PartitionSpec as P

S = 2048
F = 1024
LAGS = 256
BLOCK = 32
CH_DEV = 64
VMEM_GRANT = 60899328


def forward_table():
    freq_index = jnp.arange(F, dtype=jnp.int32)
    time_index = jnp.arange(S, dtype=jnp.int32)
    phase = freq_index[:, None] * time_index[None, :] % S
    angles = phase.astype(jnp.float32) * (2.0 * jnp.pi / S)
    scale = 1.0 / jnp.sqrt(jnp.float32(S))
    return jnp.stack(
        [
            (jnp.cos(angles) * scale).astype(jnp.bfloat16),
            (-jnp.sin(angles) * scale).astype(jnp.bfloat16),
        ],
        axis=1,
    )


def lag_table():
    freq_index = jnp.arange(F, dtype=jnp.int32)
    shifts = (jnp.arange(LAGS, dtype=jnp.int32) - LAGS // 2) % S
    phase = freq_index[:, None] * shifts[None, :] % S
    angles = phase.astype(jnp.float32) * (2.0 * jnp.pi / S)
    scale = 1.0 / jnp.sqrt(jnp.float32(F))
    return jnp.stack(
        [
            (jnp.cos(angles) * scale).astype(jnp.bfloat16),
            (-jnp.sin(angles) * scale).astype(jnp.bfloat16),
        ],
        axis=1,
    )


def synthesize(incoming, table):
    count = incoming.shape[-1]
    flat = incoming.reshape(2 * F, count)
    result = jnp.einsum(
        "qn,qt->tn", flat, table.reshape(2 * F, S), preferred_element_type=jnp.float32
    )
    return result.astype(jnp.bfloat16)


def on_device(records, pairs, observed, lag_mask):
    fibre_count = lax.axis_size("fibre")
    seg_count = lax.axis_size("seg")
    spread_count = fibre_count * seg_count
    freq_dev = F // spread_count
    blocks_dev = CH_DEV // BLOCK
    block_count = CH_DEV * spread_count // BLOCK
    pair_total = pairs.shape[0]
    pairs_dev = pair_total // spread_count
    table = forward_table()
    lags = lag_table()
    spans = records.reshape(1, S // fibre_count, fibre_count, CH_DEV)
    incoming = lax.all_to_all(spans, "fibre", split_axis=2, concat_axis=1, tiled=True)
    count = incoming.shape[3]
    signal = incoming.reshape(S, count)
    result = jnp.einsum(
        "qs,sn->qn", table.reshape(2 * F, S), signal, preferred_element_type=jnp.float32
    )
    spectra = result.reshape(F, 2, count).astype(jnp.bfloat16)
    widened = lax.all_to_all(spectra, ("fibre", "seg"), split_axis=0, concat_axis=2, tiled=True)
    seg_blocks = fibre_count * blocks_dev
    slot_ids = (
        pairs % seg_blocks // blocks_dev * seg_count + pairs // seg_blocks
    ) * blocks_dev + pairs % blocks_dev
    blocks_grid = widened.reshape(freq_dev, 2, block_count, BLOCK)
    first_side = jnp.take(blocks_grid, slot_ids[:, 0], axis=2).astype(jnp.float32)
    second_side = jnp.take(blocks_grid, slot_ids[:, 1], axis=2).astype(jnp.float32)
    first_re, first_im = (first_side[:, 0], first_side[:, 1])
    second_re, second_im = (second_side[:, 0], second_side[:, 1])
    cross_re = first_re * second_re + first_im * second_im
    cross_im = first_im * second_re - first_re * second_im
    cross_spec = jnp.stack([cross_re, cross_im], axis=1).astype(jnp.bfloat16)
    cross_spec = cross_spec.reshape(freq_dev, 2, spread_count, pairs_dev * BLOCK)
    owned_spec = lax.all_to_all(
        cross_spec, ("fibre", "seg"), split_axis=2, concat_axis=0, tiled=True
    )
    owned_spec = owned_spec.reshape(F, 2, pairs_dev * BLOCK)
    partial_corr = jnp.einsum("wpx,wpl->xl", owned_spec, lags, preferred_element_type=jnp.float32)
    synthetic = (
        lax.psum(partial_corr.astype(jnp.bfloat16), "rec")
        .astype(jnp.float32)
        .reshape(pairs_dev, BLOCK, LAGS)
    )
    weights = lag_mask[:, None, :].astype(jnp.float32) * jnp.tanh(synthetic - observed)
    weights_low = weights.astype(jnp.bfloat16).reshape(pairs_dev * BLOCK, LAGS)
    adjoint_spec = jnp.einsum("xl,wpl->wpx", weights_low, lags, preferred_element_type=jnp.float32)
    adjoint_spec = adjoint_spec.astype(jnp.bfloat16).reshape(F, 2, 1, pairs_dev * BLOCK)
    returned = lax.all_to_all(
        adjoint_spec, ("fibre", "seg"), split_axis=0, concat_axis=2, tiled=True
    )
    returned = returned.reshape(freq_dev, 2, pair_total, BLOCK).astype(jnp.float32)
    adjoint_re, adjoint_im = (returned[:, 0], returned[:, 1])
    grad_first = jnp.stack(
        [
            adjoint_re * second_re - adjoint_im * second_im,
            adjoint_re * second_im + adjoint_im * second_re,
        ],
        axis=1,
    )
    grad_second = jnp.stack(
        [
            adjoint_re * first_re + adjoint_im * first_im,
            adjoint_re * first_im - adjoint_im * first_re,
        ],
        axis=1,
    )
    contributions = jnp.concatenate([grad_first, grad_second], axis=2)
    endpoint_ids = jnp.concatenate([slot_ids[:, 0], slot_ids[:, 1]])
    summed = jax.ops.segment_sum(
        jnp.moveaxis(contributions, 2, 0), endpoint_ids, num_segments=block_count
    )
    block_adjoint = jnp.moveaxis(summed, 0, 2).astype(jnp.bfloat16)
    outgoing = block_adjoint.reshape(freq_dev, 2, spread_count, CH_DEV)
    sources = synthesize(
        lax.all_to_all(outgoing, ("fibre", "seg"), split_axis=2, concat_axis=0, tiled=True), table
    )
    regrouped = lax.all_to_all(sources, "fibre", split_axis=0, concat_axis=1, tiled=True)
    return regrouped[None]


def window_tables(bands):
    span, reach, n = S // bands, LAGS // 2, S // bands + LAGS
    half = n // 2
    freqs, places = np.arange(half), np.arange(n)
    shifts = np.arange(LAGS) - reach
    ends = np.where(freqs == 0, 1.0, 2.0) / (n * 2.0 * np.sqrt(F))

    def table(times, scale):
        angles = (freqs[None, :] * times[:, None] % n) * (2.0 * np.pi / n)
        real, imag = np.cos(angles), -np.sin(angles)
        imag[:, 0] = np.where(times % 2 == 0, 1.0, -1.0)
        return np.concatenate([real * scale, imag * scale], axis=1)

    whole = table(places, np.ones(half))
    lags = table(shifts, ends).T
    taps = table(shifts, np.ones(half))
    back = table(places[reach : reach + span], ends)
    lags = np.concatenate([lags, lags])
    return [t.astype(np.float32).astype(jnp.bfloat16) for t in (whole, lags, taps, back)]


def dot(left, right, left_dim=1, right_dim=0):
    return lax.dot_general(
        left,
        right,
        (((left_dim,), (right_dim,)), ((), ())),
        preferred_element_type=jnp.float32,
    )


def spectral_product(terms, sign, extra=None):
    both = sum(p1 * q1 for (_, p1), (_, q1) in terms)
    real = sum(p0 * q0 for (p0, _), (q0, _) in terms)
    imag = sum(p1 * q0 - sign * (p0 * q1) for (p0, p1), (q0, q1) in terms)
    whole = real + sign * both
    ends = lax.broadcasted_iota(jnp.int32, (both.shape[0], 128), 1) == 0
    return tuple(
        jnp.concatenate([jnp.where(ends, end, value[:, :128]), value[:, 128:]], axis=1)
        for end, value in ((real[:, :128], whole), (both[:, :128] if extra is None else both[:, :128] + extra, imag))
    )


def fused_kernel(
    sizes, x_hbm, pairs_hbm, observed_hbm, mask_hbm, whole_hbm, lags_hbm, taps_hbm, back_hbm,
    out, pairs, ext, observed, mask, whole, lags, taps, back,
    inbox_sum, stage_total, inbox_total, columns, core_spec, both_spec, left_spec,
    full_spec, select, cross, stage_core, inbox_core, stage3, inbox3, inbox4, grads, held,
    following, high, load_sem, send1, recv1, send_sum, recv_sum, total_sem, core_send, core_recv,
    relay_send, relay_recv, send3, recv3, send4, recv4,
):
    fibres, segs, recs = sizes
    bands = fibres * segs
    last = fibres - 1
    g, f, s, r = (lax.axis_index(name) for name in ("groups", "fibre", "seg", "rec"))
    o = 1 - s
    band = f * segs + s
    span, reach, width = S // bands, LAGS // 2, x_hbm.shape[1]
    n = span + LAGS
    half = n // 2
    blocks = width // BLOCK
    count = pairs.shape[1] * BLOCK
    low, full = jnp.bfloat16, jnp.float32

    def at(fibre, seg, rec):
        return (g, fibre, seg, rec)

    def at_band(index):
        return at(index // segs, index % segs, r)

    def remote(src, dst, send, recv, device):
        return pltpu.make_async_remote_copy(
            src_ref=src, dst_ref=dst, send_sem=send, recv_sem=recv,
            device_id=device, device_id_type=pl.DeviceIdType.MESH,
        )

    def push(src, dst, send, recv, device):
        copy = remote(src, dst, send, recv, device)
        copy.start()
        return copy

    def arrived(dst, recv):
        remote(dst, dst, recv, recv, at(f, s, 1 - r)).wait_recv()

    def signal(sem, device):
        pl.semaphore_signal(sem, inc=1, device_id=device, device_id_type=pl.DeviceIdType.MESH)

    def rows(start, size, unit):
        return pl.ds(pl.multiple_of(start, unit), size)

    def flipped(index, bits):
        result, bit = 0, 1
        while bit < bands:
            digit = index // bit % 2
            result += bit * (1 - digit if bits // bit % 2 else digit)
            bit *= 2
        return result

    partner = at(f, s, 1 - r)
    across = at(f, o, r)
    places = [(fi, si) for fi in range(fibres) for si in range(segs)]

    barrier = pltpu.get_barrier_semaphore()
    signal(barrier, partner)
    signal(barrier, across)
    for fi, si in places:

        @pl.when(fi > f)
        def _():
            signal(barrier, at(fi, si, r))

    loads = [
        pltpu.make_async_copy(src, dst, load_sem.at[i])
        for i, (src, dst) in enumerate(
            [
                (x_hbm, ext.at[s, pl.ds(reach, 2 * span)]), (pairs_hbm, pairs), (whole_hbm, whole), (lags_hbm, lags),
                (observed_hbm.at[r], observed), (mask_hbm, mask), (taps_hbm, taps), (back_hbm, back),
            ]
        )
    ]
    for load in loads:
        load.start()

    def give(first, size, place, send, recv, device):
        return remote(
            x_hbm.at[pl.ds(first, size)], ext.at[s, pl.ds(place, size)], send1.at[send], recv1.at[recv], device
        )

    needed = [
        [give(span, span, span + reach, 0, 0, across), give(reach, reach, 2 * reach, 1, 1, across)],
        [give(0, span, reach, 0, 0, across)],
    ]
    later = [give(0, reach, reach, 2, 2, across), give(span, span, reach + span, 2, 2, across)]
    upper, lower = (f + 1) % fibres, (f + last) % fibres
    up = give(2 * span - reach, reach, 0, 3, 3, at(upper, s, r))
    up_across = give(2 * span - reach, reach, 0, 4, 4, at(upper, 0, r))
    down = give(0, reach, reach + 2 * span, 5, 5, at(lower, s, r))
    edges = [pl.ds(0, reach), pl.ds(reach + 2 * span, reach)]
    passed = [
        remote(ext.at[s, edge], ext.at[s, edge], send1.at[6 + i], recv1.at[6 + i], across)
        for i, edge in enumerate(edges)
    ]

    def send_up():
        @pl.when(s == 0)
        def _():
            up.start()

        @pl.when(s == 1)
        def _():
            up_across.start()

    pl.semaphore_wait(barrier, segs * (f + 1))
    for si in range(segs):

        @pl.when(s == si)
        def _():
            for copy in needed[si]:
                copy.start()

    @pl.when(f == last)
    def _():
        send_up()

    for fi, si in places:

        @pl.when(fi == f - 1)
        def _():
            signal(following, at(fi, si, r))

        @pl.when(fi < f - 1)
        def _():
            signal(high, at(fi, si, r))

    loads[0].wait()
    folded = [
        ext[s, pl.ds(reach + span * w, span)].astype(full).reshape(-1, 8, width).sum(axis=0) for w in range(segs)
    ]
    odd = lax.broadcasted_iota(jnp.int32, (8, width), 0) % 2 == 1
    flat = jnp.sum(folded[0] + folded[1], axis=0, keepdims=True)
    turned = [jnp.sum(jnp.where(odd, -part, part), axis=0, keepdims=True) for part in folded]
    inbox_sum[band] = jnp.concatenate([flat] + turned + [jnp.zeros_like(flat)], axis=0)
    sends = [up, down]
    own_sum = inbox_sum.at[band]
    sum_sends = [
        remote(own_sum, own_sum, send_sum.at[fi * segs + si], recv_sum.at[band], at(fi, si, r)) for fi, si in places
    ]
    across_sum = push(own_sum, own_sum, send_sum.at[bands], recv_sum.at[band], across)
    sends.append(across_sum)
    for (fi, si), copy in zip(places, sum_sends):

        @pl.when(fi < f)
        def _():
            copy.start()

    loads[1].wait()
    cut = bands // 2
    others = [flipped(band, k * segs) // segs for k in range(1, fibres)]
    entries = [(r, f), (1 - r, f)] + [(r, fibre) for fibre in others] + [(1 - r, fibre) for fibre in others]
    group = 2 * segs * BLOCK
    lane = lax.broadcasted_iota(jnp.int32, (1, 2 * count), 1)
    target = lane
    for p, (h, fibre) in enumerate(entries):
        for end in range(2):
            for i in range(segs):
                first = p * group + (end * segs + i) * BLOCK
                inside = (lane >= first) & (lane < first + BLOCK)
                target = jnp.where(inside, lane + (pairs[end, (fibre * segs + i) * recs + h] * BLOCK - first), target)
    line = lax.broadcasted_iota(jnp.int32, select.shape, 0) + s * width
    select[...] = jnp.where(line == target, 1.0, 0.0).astype(low)

    def put(spec, seg, value):
        spec[rows(seg * blocks, blocks, blocks)] = value.astype(spec.dtype).reshape(blocks, BLOCK, n)

    def core_part(seg):
        part = dot(ext[seg, rows(reach + span * s, span, reach)], whole[reach : reach + span], 0, 0)
        put(core_spec, seg, part)

    def left_part(seg):
        part = dot(ext[seg, rows(span * s, reach, reach)], whole[:reach], 0, 0)
        put(left_spec, seg, part)
        put(both_spec, seg, part + core_spec[rows(seg * blocks, blocks, blocks)].reshape(width, n))

    loads[2].wait()
    core_part(s)

    @pl.when(f < last)
    def _():
        pl.semaphore_wait(following, segs)
        send_up()

    for si in range(segs):

        @pl.when(s == 1 - si)
        def _():
            arrived(ext.at[si, pl.ds(reach + span * (1 - si), span)], recv1.at[0])

    core_part(o)

    @pl.when(f < last - 1)
    def _():
        pl.semaphore_wait(high, segs * (last - 1 - f))

    for (fi, si), copy in zip(places, sum_sends):

        @pl.when(fi > f)
        def _():
            copy.start()

    @pl.when(s == 1)
    def _():
        up.start()

    down.start()

    def send_later():
        for si in range(segs):

            @pl.when(s == si)
            def _():
                later[si].start()

    pl.when(f == 0)(send_later)

    @pl.when(s == 0)
    def _():
        arrived(ext.at[0, edges[0]], recv1.at[3])

    left_part(s)

    @pl.when(s == 0)
    def _():
        arrived(ext.at[1, edges[0]], recv1.at[4])

    @pl.when(s == 1)
    def _():
        arrived(ext.at[0, pl.ds(2 * reach, reach)], recv1.at[1])

    pl.when(f > 0)(send_later)
    left_part(o)

    def block(spec, index):
        value = spec[index].astype(full)
        return value[:, :half], value[:, half:]

    ordered = sorted(range(bands), key=lambda j: (-abs(2 * (j // segs) - last), -j))
    chunks = ordered[:cut], ordered[cut:]

    def correlate(place, h, chunk):
        for i, j in enumerate(chunk):
            pair = j * recs + h
            one, two = pairs[0, pair], pairs[1, pair]
            terms = [(block(core_spec, one), block(both_spec, two)), (block(left_spec, one), block(core_spec, two))]
            inner = terms[0][0][1][:, :128] * terms[1][1][1][:, :128]
            parts = spectral_product(terms, 1.0, inner * (-n / span))
            for q, part in enumerate(parts):
                high_part = part.astype(low)
                here = pl.ds(i * BLOCK, BLOCK)
                cross[place, here, pl.ds(q * half, half)] = high_part
                cross[place, here, pl.ds(n + q * half, half)] = (part - high_part.astype(full)).astype(low)
        return dot(cross[place], lags[...])

    loads[3].wait()
    for i, chunk in enumerate(chunks):
        stage_core[i] = correlate(i, 1 - r, chunk).astype(low)
        sends.append(push(stage_core.at[i], inbox_core.at[i], core_send.at[i], core_recv.at[i], partner))

    spread3 = [
        remote(stage3.at[j], inbox3.at[band], send3.at[j], recv3.at[band], at(j // segs, j % segs, r))
        for j in range(bands)
    ]
    for i, chunk in enumerate(chunks):
        partial = correlate(2 + i, r, chunk)
        arrived(inbox_core.at[i], core_recv.at[i])
        partial = (partial + inbox_core[i].astype(full)).astype(low)
        for place, j in enumerate(chunk):
            stage3[j] = partial[place * BLOCK : (place + 1) * BLOCK]

            @pl.when(band != j)
            def _():
                spread3[j].start()

    inbox3[band] = stage3[band]

    @pl.when(s == 0)
    def _():
        passed[0].start()

    @pl.when(s == 1)
    def _():
        arrived(ext.at[1, edges[0]], recv1.at[3])

    arrived(ext.at[s, edges[1]], recv1.at[5])
    passed[1].start()

    for d in range(1, bands):
        k = flipped(band, d)
        arrived(inbox_sum.at[k], recv_sum.at[k])
    for seg in range(segs):
        told = [inbox_sum[fi * segs + seg] for fi in range(fibres)]
        spans = jnp.concatenate([part[1:3] for part in told], axis=0)
        stage_total[seg] = jnp.concatenate(
            [
                sum(part[0:1] for part in told),
                jnp.sum(spans, axis=0, keepdims=True),
                spans,
                jnp.zeros((2 * bands - 2 - 2 * fibres, width), full),
            ],
            axis=0,
        )
    sends.append(push(stage_total, inbox_total, total_sem.at[0], total_sem.at[1], partner))
    arrived(inbox_total, total_sem.at[1])
    for seg in range(segs):
        total = jnp.concatenate([stage_total[seg], inbox_total[seg]], axis=0)
        columns[pl.ds(seg * blocks, blocks)] = total.T.reshape(blocks, BLOCK, 4 * bands)
    loads[4].wait()
    loads[5].wait()
    ends = columns[pairs[0, band * recs + r]] * columns[pairs[1, band * recs + r]] * (1.0 / (2.0 * F**0.5))
    kind = lax.broadcasted_iota(jnp.int32, ends.shape, 1) % (2 * bands)
    flat = jnp.sum(jnp.where(kind == 0, ends * (1.0 / S), 0.0), axis=1, keepdims=True)
    turned = jnp.where(kind == 1, ends * (-1.0 / S), ends * (1.0 / span))
    turned = jnp.sum(jnp.where(kind == 0, 0.0, turned), axis=1, keepdims=True)
    even = lax.broadcasted_iota(jnp.int32, (BLOCK, LAGS), 1) % 2 == reach % 2
    offset = flat + jnp.where(even, turned, -turned)
    for d in range(1, bands):
        k = flipped(band, d)
        arrived(inbox3.at[k], recv3.at[k])
    synthetic = offset + inbox3[0].astype(full)
    for k in range(1, bands):
        synthetic += inbox3[k].astype(full)
    window = mask[pl.ds(r, 1), :].astype(full)
    inbox4[r, band] = (window * jnp.tanh(synthetic - observed[...])).astype(low)
    own = inbox4.at[r, band]
    spread4 = [
        remote(own, own, send4.at[j], recv4.at[band], at(j // segs, j % segs, r)) for j in range(bands)
    ]
    sends.append(push(own, own, relay_send.at[0], relay_recv.at[band], partner))
    for j in range(bands):

        @pl.when(band != j)
        def _():
            spread4[j].start()


    for si in range(segs):

        @pl.when(s == 1 - si)
        def _():
            arrived(ext.at[si, pl.ds(reach + span * si, reach + (span - reach) * si)], recv1.at[2])

    @pl.when(s == 1)
    def _():
        arrived(ext.at[0, edges[0]], recv1.at[6])

    arrived(ext.at[o, edges[1]], recv1.at[7])
    head = lax.broadcasted_iota(jnp.int32, (1, half), 1) == 0
    for seg in range(segs):
        total = stage_total[seg].T * (n / S)
        for w in range(segs):
            value = dot(ext[seg, pl.ds(span * w, n)], whole[...], 0, 0)
            value = jnp.concatenate(
                [
                    value[:, :half] + jnp.where(head, total[:, 0:1], 0.0),
                    value[:, half:] - jnp.where(head, total[:, 1:2], 0.0),
                ],
                axis=1,
            )
            put(full_spec.at[w], seg, value)
    loads[6].wait()

    def gradients(first, stop):
        given = [inbox4[h, pl.ds(fibre * segs, segs)].reshape(segs * BLOCK, LAGS) for h, fibre in entries[first:stop]]
        spread = dot(jnp.concatenate(given, axis=0), taps[...])
        for p in range(first, stop):
            h, fibre = entries[p]
            for i in range(segs):
                pair = (fibre * segs + i) * recs + h
                start = ((p - first) * segs + i) * BLOCK
                filters = spread[start : start + BLOCK]
                filters = filters[:, :half], filters[:, half:]
                base = p * group + i * BLOCK
                for w in range(segs):
                    one = block(full_spec.at[w], pairs[0, pair])
                    two = block(full_spec.at[w], pairs[1, pair])
                    for place, parts in (
                        (base, spectral_product([(filters, two)], -1.0)),
                        (base + segs * BLOCK, spectral_product([(one, filters)], 1.0)),
                    ):
                        for q in range(2):
                            grads[w, pl.ds(place, BLOCK), pl.ds(q * half, half)] = parts[q].astype(low)

    turns = [flipped(band, d) for d in range(bands)]
    relays = [
        remote(inbox4.at[r, k], inbox4.at[r, k], relay_send.at[d], relay_recv.at[k], partner)
        for d, k in enumerate(turns)
    ]
    sends += relays[1:]

    def take(d):
        arrived(inbox4.at[r, turns[d]], recv4.at[turns[d]])
        relays[d].start()

    def relayed(d):
        arrived(inbox4.at[1 - r, turns[d]], relay_recv.at[turns[d]])

    def fibre_first():
        for d in range(segs):
            relayed(d)
        gradients(0, recs)

    def gather(first, stop):
        cut_at = slice(first * group, stop * group)
        return [dot(select[:, cut_at], grads[w, cut_at]) for w in range(segs)]

    direct = recs + fibres - 1
    for d in range(1, segs):
        take(d)

    @pl.when(r == 0)
    def _():
        fibre_first()
        for w, part in enumerate(gather(0, recs)):
            held[w] = part

    for d in range(segs, bands):
        take(d)

    @pl.when(r == 1)
    def _():
        fibre_first()
        gradients(recs, direct)
        for w, part in enumerate(gather(0, direct)):
            held[w] = part

    loads[7].wait()
    for d in range(segs, bands):
        relayed(d)
    for core, first in enumerate((recs, direct)):

        @pl.when(r == core)
        def _():
            gradients(first, recs * fibres)
            for w, part in enumerate(gather(first, recs * fibres)):
                summed = (held[w] + part).astype(low)
                out[pl.ds(span * w, span), :] = dot(back[...], summed, 1, 1).astype(low)

    for si in range(segs):

        @pl.when(s == si)
        def _():
            for copy in needed[si] + [later[si]] + passed[si:]:
                copy.wait_send()

    @pl.when(s == 1)
    def _():
        up_across.wait_send()

    for copy in sends:
        copy.wait_send()
    for j in range(bands):

        @pl.when(band != j)
        def _():
            spread3[j].wait_send()
            spread4[j].wait_send()

    for (fi, si), copy in zip(places, sum_sends):

        @pl.when(fi != f)
        def _():
            copy.wait_send()


def fused_on_device(mesh_shape, tables, records, pairs, observed, lag_mask):
    fibres, segs, recs = (mesh_shape[name] for name in ("fibre", "seg", "rec"))
    bands = fibres * segs
    _, extent, width = records.shape
    span, reach = S // bands, LAGS // 2
    n = span + LAGS
    count = pairs.shape[0] * BLOCK
    own = count // recs
    total = segs * width
    low, full = jnp.bfloat16, jnp.float32
    vmem = pl.BlockSpec(memory_space=pltpu.VMEM)
    hbm = pl.BlockSpec(memory_space=pltpu.HBM)
    corr = (BLOCK, LAGS)
    spec = (total // BLOCK, BLOCK, n)

    def sems(*sizes):
        return [pltpu.SemaphoreType.DMA((size,)) for size in sizes]

    result = pl.pallas_call(
        functools.partial(fused_kernel, (fibres, segs, recs)),
        out_shape=pltpu.VMEM((extent, width), low),
        in_specs=[hbm] * 8,
        out_specs=vmem,
        scratch_shapes=[
            pltpu.SMEM((2, pairs.shape[0]), jnp.int32),
            pltpu.VMEM((segs, 2 * span + 2 * reach, width), low),
            pltpu.VMEM(corr, full),
            pltpu.VMEM(lag_mask.shape, jnp.int32),
            pltpu.VMEM((n, n), low),
            pltpu.VMEM((2 * n, LAGS), low),
            pltpu.VMEM((LAGS, n), low),
            pltpu.VMEM((span, n), low),
            pltpu.VMEM((bands, 4, width), full),
            pltpu.VMEM((segs, 2 * bands, width), full),
            pltpu.VMEM((segs, 2 * bands, width), full),
            pltpu.VMEM((total // BLOCK, BLOCK, 4 * bands), full),
            pltpu.VMEM(spec, full),
            pltpu.VMEM(spec, full),
            pltpu.VMEM(spec, full),
            pltpu.VMEM((segs,) + spec, low),
            pltpu.VMEM((width, 2 * count), low),
            pltpu.VMEM((2 * recs, own // 2, 2 * n), low),
            pltpu.VMEM((2, own // 2, LAGS), low),
            pltpu.VMEM((2, own // 2, LAGS), low),
            pltpu.VMEM((bands,) + corr, low),
            pltpu.VMEM((bands,) + corr, low),
            pltpu.VMEM((recs, bands) + corr, low),
            pltpu.VMEM((segs, 2 * count, n), low),
            pltpu.VMEM((segs, width, n), full),
            pltpu.SemaphoreType.REGULAR,
            pltpu.SemaphoreType.REGULAR,
            *sems(8, 8, 8, bands + 1, bands, 2, 2, 2, bands, bands, bands, bands, bands, bands),
        ],
        compiler_params=pltpu.CompilerParams(
            has_side_effects=True, collective_id=0, vmem_limit_bytes=VMEM_GRANT
        ),
        name="adjoint",
    )(records[0], pairs.T, observed, lag_mask, *tables)
    return result[None]


def fits_fused(shape, records, pairs):
    fibres, segs, recs = (shape[name] for name in ("fibre", "seg", "rec"))
    bands = fibres * segs
    width = records.shape[2] // (shape["groups"] * segs)
    return (
        fibres > 1
        and fibres & (fibres - 1) == 0
        and segs == 2
        and recs == 2
        and width % 128 == 0
        and width * segs <= 512
        and S // bands >= LAGS
        and pairs.shape[0] == bands * recs
    )


def solution(mesh):
    in_specs = (
        P("rec", "fibre", ("groups", "seg")),
        P(),
        P(("groups", "fibre", "seg"), None, None),
        P(("groups", "fibre", "seg"), None),
    )
    out_specs = P("rec", "fibre", ("groups", "seg"))
    shape = dict(mesh.shape)

    def run(records, pairs, observed, lag_mask):
        args = (records, pairs, observed, lag_mask)
        if not fits_fused(shape, records, pairs):
            return jax.shard_map(
                on_device, mesh=mesh, in_specs=in_specs, out_specs=out_specs, check_vma=False
            )(*args)
        tables = [jnp.asarray(t) for t in window_tables(shape["fibre"] * shape["seg"])]

        def body(*blocks):
            return fused_on_device(shape, tables, *blocks)

        return jax.shard_map(
            body, mesh=mesh, in_specs=in_specs, out_specs=out_specs, check_vma=False
        )(*args)

    return run
```
